256 devices in a mesh: section: 8 (over y, x_hi), dp: 32 (over z, x_lo, core).
Axes of the slice: x: 4 (x_hi: 2, x_lo: 2; x = x_hi * 2 + x_lo), y: 4, z: 8, core: 2. Of those that a mesh axis runs over, the one named last changes fastest.
Arguments:
- block_inputs: bfloat16 [8, 4, 2048, 2048], P('section', None, 'dp'), may hold values from -6 to 6
- mixed_inputs: bfloat16 [8, 4, 2048, 2048], P('section', None, 'dp'), may hold values from -6 to 6
- token_ids: int32 [4, 2048], P(None, 'dp'), may hold values from 0 to 2047
- target_ids: int32 [4, 2048], P(None, 'dp'), may hold values from 0 to 2047
- final_gain: float32 [2048], replicated, may hold values from 0.5 to 1.5
- out_weight: bfloat16 [8, 2048, 2048], P('section'), may hold values from -0.046875 to 0.046875
- head_weight: bfloat16 [2048, 2048], P('section'), may hold values from -0.375 to 0.375
- out_master: float32 [8, 2048, 2048], P('section', 'dp'), may hold values from -0.125 to 0.125
- out_first: float32 [8, 2048, 2048], P('section', 'dp'), may hold values from -2.5 to 2.5
- out_second: float32 [8, 2048, 2048], P('section', 'dp'), may hold values from 4 to 80
- head_master: float32 [2048, 2048], P(('section', 'dp')), may hold values from -0.125 to 0.125
- head_first: float32 [2048, 2048], P(('section', 'dp')), may hold values from -1.5 to 1.5
- head_second: float32 [2048, 2048], P(('section', 'dp')), may hold values from 1.2 to 24
- embed_master: float32 [2048, 2048], P(('section', 'dp')), may hold values from -0.125 to 0.125
- embed_first: float32 [2048, 2048], P(('section', 'dp')), may hold values from -0.125 to 0.125
- embed_second: float32 [2048, 2048], P(('section', 'dp')), may hold values from 0.009765625 to 0.1953125
Outputs:
- out_master_next: float32 [8, 2048, 2048], P('section', 'dp')
- out_first_next: float32 [8, 2048, 2048], P('section', 'dp')
- out_second_next: float32 [8, 2048, 2048], P('section', 'dp')
- head_master_next: float32 [2048, 2048], P(('section', 'dp'))
- head_first_next: float32 [2048, 2048], P(('section', 'dp'))
- head_second_next: float32 [2048, 2048], P(('section', 'dp'))
- embed_master_next: float32 [2048, 2048], P(('section', 'dp'))
- embed_first_next: float32 [2048, 2048], P(('section', 'dp'))
- embed_second_next: float32 [2048, 2048], P(('section', 'dp'))
The draws below stay inside these ranges and needn't reach their ends.
Inputs may be any that keep to these rules, and one draw needn't show every extreme that they name: `token_ids`: every token id lies in 0 to 2047. `target_ids`: every target id lies in 0 to 2047.
All inputs are finite; a program needn't handle non-finite values.
Results may differ from the reference program's by a relative error of at most 0.00155.
Values may be sent and summed in bfloat16 or wider, within the bound.
A program may use at most 128 MiB of HBM per device.

```python
import math
import jax
import jax.numpy as jnp
import numpy as np
from jax import lax

D = 2048
VOCAB = 2048
MICRO = 4
TOKENS_MB = 2048
N_SECTION = 8


def with_ends(entries, key, least, largest):
    longest = entries.shape.index(max(entries.shape))
    spots = []
    for shift in (0, 1):
        where = [jax.random.randint(jax.random.fold_in(key, axis), (), 0, length) for axis, length in enumerate(entries.shape)]
        where[longest] = (where[longest] + shift) % entries.shape[longest]
        spots.append(tuple(where))
    return entries.at[spots[0]].set(least).at[spots[1]].set(largest)


def level_of(key, shape, shards, least, top_value):
    level = 1.0
    for position, shards_of in shards:
        steps = jax.random.uniform(jax.random.fold_in(jax.random.fold_in(key, 6), position), (shards_of,), jnp.float32, least / len(shards), top_value / len(shards))
        level = level * jnp.repeat(jnp.exp(steps), shape[position] // shards_of).reshape((-1,) + (1,) * (len(shape) - 1 - position))
    return level


def rank_table(amount, skew):
    portions = [(1 << 20) // math.isqrt(grade ** skew) + 1 for grade in range(1, amount + 1)]
    deviation = 1 + sum(portions) // (1 << 30)
    return np.cumsum(np.array([max(1, weight // deviation) for weight in portions]))


def ranked_ids(own_key, shape, number_of, slope):
    grid = rank_table(number_of, slope)
    ticket = jax.random.randint(jax.random.fold_in(own_key, 1), shape, 0, int(grid[number_of - 1]))
    rank = jnp.searchsorted(jnp.asarray(grid, jnp.int32), ticket, side="right")
    return jax.random.permutation(jax.random.fold_in(own_key, 2), number_of)[rank].astype(jnp.int32)


def centred(stream_key, shape, spread, bound, pieces=(), dtype=jnp.bfloat16):
    result = spread * jax.random.normal(stream_key, shape, jnp.float32)
    if pieces:
        result = result * level_of(stream_key, shape, pieces, -0.22, 0.18)
    return jnp.clip(result, -bound, bound).astype(dtype)


def setup_inputs(seed: int = 0) -> dict:
    arg_keys = jax.random.split(jax.random.key(seed), 17)
    return {
        "block_inputs": centred(arg_keys[0], (N_SECTION, MICRO, TOKENS_MB, D), 1.0, 6.0, ((0, 8), (2, 32))),
        "mixed_inputs": centred(arg_keys[1], (N_SECTION, MICRO, TOKENS_MB, D), 1.0, 6.0, ((0, 8), (2, 32))),
        "token_ids": with_ends(ranked_ids(arg_keys[2], (MICRO, TOKENS_MB), VOCAB, 2), jax.random.fold_in(arg_keys[2], 3), 0, VOCAB - 1).astype(jnp.int32),
        "target_ids": with_ends(ranked_ids(arg_keys[3], (MICRO, TOKENS_MB), VOCAB, 2), jax.random.fold_in(arg_keys[3], 3), 0, VOCAB - 1).astype(jnp.int32),
        "final_gain": jnp.clip(1.0 + 0.1 * jax.random.normal(arg_keys[4], (D,), jnp.float32), 0.5, 1.5),
        "out_weight": centred(arg_keys[5], (N_SECTION, D, D), (D * N_SECTION) ** -0.5, 0.046875, ((0, 8),)),
        "head_weight": centred(arg_keys[6], (VOCAB, D), (3 * D ** -0.5), 0.375, ((0, 8),)),
        "out_master": centred(arg_keys[7], (N_SECTION, D, D), D ** -0.5, 0.125, ((0, 8), (1, 32)), jnp.float32),
        "out_first": centred(arg_keys[8], (N_SECTION, D, D), (0.2 * (MICRO * TOKENS_MB) ** 0.5 * D ** -0.5), 2.5, ((0, 8), (1, 32)), jnp.float32),
        "out_second": jnp.clip(jnp.exp(math.log(80.0) - 2.9957323 * jax.random.uniform(arg_keys[9], (N_SECTION, D, D), jnp.float32) ** level_of(arg_keys[9], (N_SECTION, D, D), ((0, 8), (1, 32)), -0.2, 0.2)), 4.0, 80.0),
        "head_master": centred(arg_keys[10], (VOCAB, D), D ** -0.5, 0.125, ((0, 256),), jnp.float32),
        "head_first": centred(arg_keys[11], (VOCAB, D), (0.12 * (MICRO * TOKENS_MB) ** 0.5 * VOCAB ** -0.5), 1.5, ((0, 256),), jnp.float32),
        "head_second": jnp.clip(jnp.exp(math.log(24.0) - 2.9957322 * jax.random.uniform(arg_keys[12], (VOCAB, D), jnp.float32) ** level_of(arg_keys[12], (VOCAB, D), ((0, 256),), -0.2, 0.2)), 1.2, 24.0),
        "embed_master": centred(arg_keys[13], (VOCAB, D), D ** -0.5, 0.125, ((0, 256),), jnp.float32),
        "embed_first": centred(arg_keys[14], (VOCAB, D), (0.5 * (MICRO * TOKENS_MB) ** 0.5 * (VOCAB * D) ** -0.5), 0.125, ((0, 256),), jnp.float32),
        "embed_second": jnp.clip(jnp.exp(math.log(0.1953125) - 2.9957323 * jax.random.uniform(arg_keys[15], (VOCAB, D), jnp.float32) ** level_of(arg_keys[15], (VOCAB, D), ((0, 256),), -0.2, 0.2)), 0.009765625, 0.1953125),
    }


norm_eps = 1e-05
beta_first = 0.9
beta_second = 0.95
adam_eps = 1e-05
learning_rate = 0.0003
decay_rate = 0.1

def times_transposed(former, latter):
    return lax.dot_general(former, latter, (((1,), (1,)), ((), ())), preferred_element_type=jnp.float32)

def transposed_times(former, latter):
    return lax.dot_general(former, latter, (((0,), (0,)), ((), ())), preferred_element_type=jnp.float32)

def plain_times(former, latter):
    return jnp.dot(former, latter, preferred_element_type=jnp.float32)

def normalize(values, gain):
    inverse = lax.rsqrt(lax.optimization_barrier(jnp.mean(values * values, axis=-1, keepdims=True)) + norm_eps)
    return (inverse, values * inverse * gain)

def norm_backward(values, inverse, scaled_cotangent):
    unit = values * inverse
    return inverse * (scaled_cotangent - unit * lax.optimization_barrier(jnp.mean(scaled_cotangent * unit, axis=-1, keepdims=True)))

def adam_update(master, first, second, gradient):
    first_next = beta_first * first + (1.0 - beta_first) * gradient
    second_next = beta_second * second + (1.0 - beta_second) * gradient * gradient
    master_next = master - learning_rate * (first_next / (jnp.sqrt(second_next) + adam_eps) + decay_rate * master)
    return (master_next, first_next, second_next)

def reference(block_inputs, mixed_inputs, token_ids, target_ids, final_gain, out_weight, head_weight, out_master, out_first, out_second, head_master, head_first, head_second, embed_master, embed_first, embed_second):
    last = N_SECTION - 1
    count = MICRO * TOKENS_MB
    wide = block_inputs[last].reshape(count, D).astype(jnp.float32)
    final = wide + times_transposed(mixed_inputs[last].reshape(count, D), out_weight[last])
    final_inverse, final_scaled = normalize(final, final_gain)
    last_hidden = final_scaled.astype(jnp.bfloat16)
    logits = times_transposed(last_hidden, head_weight)
    predicted = jax.nn.softmax(logits, axis=-1)
    columns = lax.broadcasted_iota(jnp.int32, (1, VOCAB), 1)
    hits = (target_ids.reshape(-1)[:, None] == columns).astype(jnp.float32)
    logit_cotangent = (predicted - hits).astype(jnp.bfloat16)
    head_gradient = transposed_times(logit_cotangent, last_hidden)
    hidden_cotangent = plain_times(logit_cotangent, head_weight)
    cotangent = norm_backward(final, final_inverse, hidden_cotangent * final_gain).astype(jnp.bfloat16)
    parts = []
    for section in range(N_SECTION):
        parts.append(transposed_times(cotangent, mixed_inputs[section].reshape(count, D)))
    out_gradient = jnp.stack(parts)
    embed_gradient = jax.ops.segment_sum(cotangent.astype(jnp.float32), token_ids.reshape(-1), num_segments=VOCAB)
    out_out = adam_update(out_master, out_first, out_second, out_gradient)
    head_out = adam_update(head_master, head_first, head_second, head_gradient)
    embed_out = adam_update(embed_master, embed_first, embed_second, embed_gradient)
    return (out_out[0], out_out[1], out_out[2], head_out[0], head_out[1], head_out[2], embed_out[0], embed_out[1], embed_out[2])
```

```python
import functools
import jax
import jax.numpy as jnp
from jax import lax
from jax.experimental import pallas as pl
from jax.experimental.pallas import tpu as pltpu
from jax.sharding import PartitionSpec as P

norm_eps = 1e-05
beta_first = 0.9
beta_second = 0.95
adam_eps = 1e-05
learning_rate = 0.0003
decay_rate = 0.1

MESH = pl.DeviceIdType.MESH


def times_transposed(former, latter):
    return lax.dot_general(
        former, latter, (((1,), (1,)), ((), ())), preferred_element_type=jnp.float32
    )


def transposed_times(former, latter):
    return lax.dot_general(
        former, latter, (((0,), (0,)), ((), ())), preferred_element_type=jnp.float32
    )


def plain_times(former, latter):
    return jnp.dot(former, latter, preferred_element_type=jnp.float32)


def adam_update(master, first, second, gradient):
    first_next = beta_first * first + (1.0 - beta_first) * gradient
    second_next = beta_second * second + (1.0 - beta_second) * gradient * gradient
    master_next = master - learning_rate * (
        first_next / (jnp.sqrt(second_next) + adam_eps) + decay_rate * master
    )
    return (master_next, first_next, second_next)


def greet(axis, size, me):
    barrier = pltpu.get_barrier_semaphore()
    for step in range(1, size):
        partner = lax.rem(me + step, size)
        pl.semaphore_signal(barrier, inc=1, device_id={axis: partner}, device_id_type=MESH)
    pl.semaphore_wait(barrier, size - 1)


def exchange_kernel(axis, size, modes, *refs):
    count = len(modes)
    ins, outs = refs[:count], refs[count : 2 * count]
    send_sem, recv_sem = refs[2 * count :]
    me = lax.axis_index(axis)
    greet(axis, size, me)
    copies = []
    for step in range(1, size):
        partner = lax.rem(me + step, size)
        for k, mode in enumerate(modes):
            copy = pltpu.make_async_remote_copy(
                src_ref=ins[k] if mode == "share" else ins[k].at[partner],
                dst_ref=outs[k].at[step - 1 if mode == "others" else me],
                send_sem=send_sem.at[k, step - 1],
                recv_sem=recv_sem.at[k, step - 1],
                device_id={axis: partner},
                device_id_type=MESH,
            )
            copy.start()
            copies.append(copy)
    for k, mode in enumerate(modes):
        if mode != "others":
            outs[k][me] = ins[k][me] if mode == "swap" else ins[k][...]
    for copy in copies:
        copy.wait()


def exchange(arrays, modes, axis, collective_id):
    size = lax.axis_size(axis)
    lead = {"swap": (size,), "share": (size,), "others": (size - 1,)}
    shapes = [
        jax.ShapeDtypeStruct(lead[mode] + (a.shape if mode == "share" else a.shape[1:]), a.dtype)
        for a, mode in zip(arrays, modes)
    ]
    return pl.pallas_call(
        functools.partial(exchange_kernel, axis, size, tuple(modes)),
        out_shape=shapes,
        in_specs=[pl.BlockSpec(memory_space=pltpu.VMEM)] * len(arrays),
        out_specs=[pl.BlockSpec(memory_space=pltpu.VMEM)] * len(arrays),
        scratch_shapes=[
            pltpu.SemaphoreType.DMA((len(arrays), size - 1)),
            pltpu.SemaphoreType.DMA((len(arrays), size - 1)),
        ],
        compiler_params=pltpu.CompilerParams(collective_id=collective_id, has_side_effects=True),
    )(*arrays)


def remote(src, dst, send, recv, device):
    return pltpu.make_async_remote_copy(
        src_ref=src, dst_ref=dst, send_sem=send, recv_sem=recv, device_id=device, device_id_type=MESH
    )


def front_kernel(
    mixed, block, weight, head, gain, target,
    cot, logit_cot, hid, window,
    table, w_all, mixed_own, block_own, final, hid_all, inv_all, inv_in, logits,
    send_sem, recv_sem, spread_send, spread_recv, local_sem,
):
    s = lax.axis_index("section")
    r = lax.axis_index("dp")
    y, xh = s // 2, s % 2
    xl, c = (r // 2) % 2, r % 2
    z = r // 4
    zin = z % 2
    before, after = lax.rem(y + 3, 4), lax.rem(y + 1, 4)
    opposite = lax.rem(y + 2, 4)
    far = 1 - xh
    section_of = lambda yy, hh: yy * 2 + hh
    to_before = {"section": section_of(before, xh), "dp": r}
    to_after = {"section": section_of(after, xh), "dp": r}
    to_cross = {"section": section_of(y, far), "dp": z * 4 + (1 - xl) * 2 + c}
    to_sibling = {"section": s, "dp": z * 4 + xl * 2 + (1 - c)}
    to_x = {"section": s, "dp": z * 4 + (1 - xl) * 2 + c}
    to_z = {"section": s, "dp": (z + 1 - 2 * zin) * 4 + xl * 2 + c}
    last = 7
    share = hid.shape[0]

    table_load = pltpu.make_async_copy(head, table.at[pl.ds(s * 256, 256)], local_sem.at[0])
    table_load.start()
    mixed_load = pltpu.make_async_copy(mixed, mixed_own, local_sem.at[1])
    block_load = pltpu.make_async_copy(block, block_own, local_sem.at[2])
    weight_load = [
        pltpu.make_async_copy(weight.at[pl.ds(k * 256, 256)], w_all.at[pl.ds(k * 256, 256)], local_sem.at[3 + k])
        for k in range(8)
    ]

    @pl.when(s == last)
    def _():
        mixed_load.start()
        for k in range(8):
            weight_load[k].start()
        block_load.start()

    barrier = pltpu.get_barrier_semaphore()
    for step in range(1, 8):
        pl.semaphore_signal(
            barrier, inc=1, device_id={"section": lax.rem(s + step, 8), "dp": r}, device_id_type=MESH
        )
    for peer in (to_cross, to_sibling, to_x, to_z):
        pl.semaphore_signal(barrier, inc=1, device_id=peer, device_id_type=MESH)
    pl.semaphore_wait(barrier, 11)

    started = []

    def go(src, dst, number, device):
        copy = remote(src, dst, send_sem.at[len(started)], recv_sem.at[number], device)
        copy.start()
        started.append(copy)

    def arrived(dst, number):
        remote(dst, dst, send_sem.at[0], recv_sem.at[number], to_sibling).wait_recv()

    slot = zin * 4 + xl * 2 + c
    slot_x = zin * 4 + (1 - xl) * 2 + c
    slot_z = (1 - zin) * 4 + xl * 2 + c
    slot_xz = (1 - zin) * 4 + (1 - xl) * 2 + c
    go(mixed, window.at[slot], 31, to_x)
    go(mixed, window.at[slot], 32, to_z)
    go(mixed, window.at[slot], 35, to_sibling)

    def rows(yy, hh, p, half=None, core=None):
        start = section_of(yy, hh) * 256 + (c if core is None else core) * 128 + p * 64
        if half is None:
            return table.at[pl.ds(start, 64)]
        return table.at[pl.ds(start + half * 32, 32)]

    def pass_on(ref, number, device):
        go(ref, ref, number, device)

    table_load.wait()
    pass_on(rows(y, xh, 1), 6, to_before)
    pass_on(rows(y, xh, 1), 5, to_after)
    pass_on(rows(y, xh, 0), 0, to_cross)
    pass_on(rows(y, xh, 0), 8, to_before)
    pass_on(rows(y, xh, 0), 7, to_after)
    pass_on(rows(y, xh, 1), 1, to_cross)

    def piece(k):
        at = pl.ds(k * share, share)
        target_device = {"section": k, "dp": r}
        return (
            remote(hid_all.at[at], hid, spread_send.at[k], spread_recv.at[0], target_device),
            remote(inv_all.at[at], inv_in, spread_send.at[8 + k], spread_recv.at[1], target_device),
        )

    @pl.when(s == last)
    def _():
        mixed_load.wait()
        for k in range(8):
            weight_load[k].wait()
        block_load.wait()

        @pl.loop(0, 8)
        def _(k):
            at = pl.ds(pl.multiple_of(k * 256, 256), 256)
            final[:, at] = block_own[:, at].astype(jnp.float32) + times_transposed(mixed_own[...], w_all[at, :])

        for k in range(8):
            at = pl.ds(k * share, share)
            value = final[at, :]
            inverse = lax.rsqrt(jnp.mean(value * value, axis=-1, keepdims=True) + norm_eps)
            normed = (value * inverse * gain[...]).astype(jnp.bfloat16)
            wide_inverse = jnp.broadcast_to(inverse, (share, 128))
            if k < last:
                hid_all[at, :] = normed
                inv_all[at, :] = wide_inverse
                for copy in piece(k):
                    copy.start()
            else:
                hid[...] = normed
                inv_in[...] = wide_inverse

    sibling_numbers = []

    def share_chunk(yy, hh, p):
        number = 17 + len(sibling_numbers)
        sibling_numbers.append((yy, hh, p, number))
        pass_on(rows(yy, hh, p), number, to_sibling)

    arrived(rows(before, xh, 1), 5)
    pass_on(rows(before, xh, 1, 0), 11, to_after)
    pass_on(rows(before, xh, 1), 2, to_cross)
    share_chunk(before, xh, 1)
    arrived(rows(after, xh, 1), 6)
    pass_on(rows(after, xh, 1, 1), 12, to_before)
    pass_on(rows(after, xh, 1), 3, to_cross)
    share_chunk(after, xh, 1)
    arrived(rows(y, far, 0), 0)
    pass_on(rows(y, far, 0), 9, to_after)
    pass_on(rows(y, far, 0), 10, to_before)
    share_chunk(y, far, 0)
    arrived(rows(before, xh, 0), 7)
    pass_on(rows(before, xh, 0, 0), 13, to_after)
    share_chunk(before, xh, 0)
    arrived(rows(after, xh, 0), 8)
    pass_on(rows(after, xh, 0, 1), 14, to_before)
    share_chunk(after, xh, 0)
    arrived(rows(opposite, xh, 1, 0), 11)
    arrived(rows(opposite, xh, 1, 1), 12)
    pass_on(rows(opposite, xh, 1), 4, to_cross)
    share_chunk(opposite, xh, 1)
    arrived(rows(y, far, 1), 1)
    share_chunk(y, far, 1)
    arrived(rows(before, far, 0), 9)
    pass_on(rows(before, far, 0, 0), 15, to_after)
    share_chunk(before, far, 0)
    arrived(rows(after, far, 0), 10)
    pass_on(rows(after, far, 0, 1), 16, to_before)
    share_chunk(after, far, 0)

    half = mixed.shape[0] // 2
    arrived(window.at[slot_z], 32)
    go(window.at[slot_z, pl.ds(0, half)], window.at[slot_z, pl.ds(0, half)], 33, to_x)
    go(window.at[slot_z], window.at[slot_z], 37, to_sibling)
    arrived(window.at[slot_x], 31)
    go(window.at[slot_x, pl.ds(half, half)], window.at[slot_x, pl.ds(half, half)], 34, to_z)
    go(window.at[slot_x], window.at[slot_x], 36, to_sibling)

    arrived(rows(before, far, 1), 2)
    share_chunk(before, far, 1)
    arrived(rows(after, far, 1), 3)
    share_chunk(after, far, 1)
    arrived(rows(opposite, xh, 0, 0), 13)
    arrived(rows(opposite, xh, 0, 1), 14)
    share_chunk(opposite, xh, 0)
    arrived(rows(opposite, far, 0, 0), 15)
    arrived(rows(opposite, far, 0, 1), 16)
    share_chunk(opposite, far, 0)
    arrived(rows(opposite, far, 1), 4)
    share_chunk(opposite, far, 1)

    @pl.when(s != last)
    def _():
        for copy in piece(0):
            copy.wait_recv()

    for yy, hh, p, number in sibling_numbers:
        arrived(rows(yy, hh, p, core=1 - c), number)

    @pl.loop(0, 8)
    def _(k):
        at = pl.ds(pl.multiple_of(k * 256, 256), 256)
        logits[:, at] = times_transposed(hid[...], table[at, :])

    value = logits[...]
    weights = jnp.exp(value - jnp.max(value, axis=-1, keepdims=True))
    predicted = weights / jnp.sum(weights, axis=-1, keepdims=True)
    columns = lax.broadcasted_iota(jnp.int32, value.shape, 1)
    logit_cot[...] = jnp.where(columns == target[...], predicted - 1.0, predicted).astype(jnp.bfloat16)

    @pl.loop(0, 8)
    def _(k):
        at = pl.ds(pl.multiple_of(k * 256, 256), 256)
        logits[:, at] = plain_times(logit_cot[...], table[:, at]) * gain[:, at]

    scaled = logits[...]
    unit = hid[...].astype(jnp.float32) / gain[...]
    cot[...] = (
        inv_in[:, :1] * (scaled - unit * jnp.mean(scaled * unit, axis=-1, keepdims=True))
    ).astype(jnp.bfloat16)

    @pl.when(s == last)
    def _():
        for k in range(last):
            for copy in piece(k):
                copy.wait_send()

    arrived(window.at[slot_xz, pl.ds(0, half)], 33)
    arrived(window.at[slot_xz, pl.ds(half, half)], 34)
    go(window.at[slot_xz], window.at[slot_xz], 38, to_sibling)
    for number, at in ((35, slot), (36, slot_x), (37, slot_z), (38, slot_xz)):
        arrived(window.at[at + 1 - 2 * c], number)
    for copy in started:
        copy.wait_send()


def front(mixed, block, weight, head, gain, target):
    tokens, width = mixed.shape
    vmem = pl.BlockSpec(memory_space=pltpu.VMEM)
    anywhere = pl.BlockSpec(memory_space=pl.ANY)
    share = tokens // 8
    return pl.pallas_call(
        front_kernel,
        out_shape=[
            jax.ShapeDtypeStruct((share, width), jnp.bfloat16),
            jax.ShapeDtypeStruct((share, width), jnp.bfloat16),
            jax.ShapeDtypeStruct((share, width), jnp.bfloat16),
            jax.ShapeDtypeStruct((8, tokens, width), jnp.bfloat16),
        ],
        in_specs=[anywhere, anywhere, anywhere, anywhere, vmem, vmem],
        out_specs=[vmem, vmem, vmem, anywhere],
        scratch_shapes=[
            pltpu.VMEM((2048, width), jnp.bfloat16),
            pltpu.VMEM((width, width), jnp.bfloat16),
            pltpu.VMEM((tokens, width), jnp.bfloat16),
            pltpu.VMEM((tokens, width), jnp.bfloat16),
            pltpu.VMEM((tokens, width), jnp.float32),
            pltpu.VMEM((tokens, width), jnp.bfloat16),
            pltpu.VMEM((tokens, 128), jnp.float32),
            pltpu.VMEM((share, 128), jnp.float32),
            pltpu.VMEM((share, 2048), jnp.float32),
            pltpu.SemaphoreType.DMA((48,)),
            pltpu.SemaphoreType.DMA((39,)),
            pltpu.SemaphoreType.DMA((16,)),
            pltpu.SemaphoreType.DMA((2,)),
            pltpu.SemaphoreType.DMA((11,)),
        ],
        compiler_params=pltpu.CompilerParams(collective_id=0, has_side_effects=True),
        name="front",
    )(mixed, block, weight, head, gain, target)


def local(
    block_inputs,
    mixed_inputs,
    token_ids,
    target_ids,
    final_gain,
    out_weight,
    head_weight,
    out_master,
    out_first,
    out_second,
    head_master,
    head_first,
    head_second,
    embed_master,
    embed_first,
    embed_second,
):
    sections = lax.axis_size("section")
    replicas = lax.axis_size("dp")
    section = lax.axis_index("section")
    batches, rows, width = mixed_inputs[0].shape
    tokens = batches * rows
    share = tokens // sections
    columns_own = width // replicas
    flat_mixed = mixed_inputs[0].reshape(tokens, width)
    slice_rows = head_weight.shape[0]
    columns = section * slice_rows + lax.broadcasted_iota(jnp.int32, (1, slice_rows), 1)
    target = lax.dynamic_slice_in_dim(target_ids.reshape(-1), section * share, share)[:, None]
    cotangent, own_logit_cotangent, own_hidden, _ = front(
        flat_mixed,
        block_inputs[0].reshape(tokens, width),
        out_weight[0],
        head_weight,
        final_gain.reshape(1, width),
        target,
    )
    all_mixed = lax.all_gather(flat_mixed, "dp", tiled=True)
    logit_pieces = own_logit_cotangent.reshape(share, sections, slice_rows).transpose(1, 0, 2)
    logit_cotangent, hidden = exchange([logit_pieces, own_hidden], ["swap", "share"], "section", 1)
    head_part = transposed_times(
        logit_cotangent.reshape(tokens, slice_rows), hidden.reshape(tokens, width)
    )
    head_gradient = lax.psum_scatter(
        head_part, "dp", scatter_dimension=0, tiled=True
    )
    pieces = cotangent.reshape(share, replicas, columns_own).transpose(1, 0, 2)
    own_columns, all_tokens = exchange(
        [pieces, token_ids.reshape(1, tokens)], ["swap", "share"], "dp", 3
    )
    (all_columns,) = exchange([own_columns], ["share"], "section", 4)
    cotangent_columns = all_columns.transpose(1, 0, 2, 3).reshape(replicas * tokens, columns_own)
    marks = (all_tokens.reshape(-1, 1) == columns).astype(jnp.bfloat16)
    embed_columns = transposed_times(marks, cotangent_columns)
    (embed_parts,) = exchange(
        [embed_columns.reshape(replicas, slice_rows // replicas, columns_own)], ["swap"], "dp", 5
    )
    embed_gradient = (
        embed_parts.astype(jnp.float32).transpose(1, 0, 2).reshape(slice_rows // replicas, width)
    )
    out_gradient = transposed_times(cotangent_columns, all_mixed)
    out_out = adam_update(out_master, out_first, out_second, out_gradient.reshape(out_master.shape))
    head_out = adam_update(head_master, head_first, head_second, head_gradient)
    embed_out = adam_update(embed_master, embed_first, embed_second, embed_gradient)
    return out_out + head_out + embed_out


def solution(mesh):
    return jax.shard_map(
        local,
        mesh=mesh,
        in_specs=(
            P("section", None, "dp", None),
            P("section", None, "dp", None),
            P(None, "dp"),
            P(None, "dp"),
            P(),
            P("section", None, None),
            P("section", None),
            P("section", "dp", None),
            P("section", "dp", None),
            P("section", "dp", None),
            P(("section", "dp"), None),
            P(("section", "dp"), None),
            P(("section", "dp"), None),
            P(("section", "dp"), None),
            P(("section", "dp"), None),
            P(("section", "dp"), None),
        ),
        out_specs=(
            P("section", "dp", None),
            P("section", "dp", None),
            P("section", "dp", None),
            P(("section", "dp"), None),
            P(("section", "dp"), None),
            P(("section", "dp"), None),
            P(("section", "dp"), None),
            P(("section", "dp"), None),
            P(("section", "dp"), None),
        ),
        check_vma=False,
    )
```

```python
import jax
import jax.numpy as jnp
from jax import lax
from jax.experimental import pallas as pl
from jax.experimental.pallas import tpu as pltpu
from jax.sharding import PartitionSpec as P

norm_eps = 1e-05
beta_first = 0.9
beta_second = 0.95
adam_eps = 1e-05
learning_rate = 0.0003
decay_rate = 0.1

MESH = pl.DeviceIdType.MESH


def times_transposed(former, latter):
    return lax.dot_general(
        former, latter, (((1,), (1,)), ((), ())), preferred_element_type=jnp.float32
    )


def transposed_times(former, latter):
    return lax.dot_general(
        former, latter, (((0,), (0,)), ((), ())), preferred_element_type=jnp.float32
    )


def plain_times(former, latter):
    return jnp.dot(former, latter, preferred_element_type=jnp.float32)


def adam_update(master, first, second, gradient):
    first_next = beta_first * first + (1.0 - beta_first) * gradient
    second_next = beta_second * second + (1.0 - beta_second) * gradient * gradient
    master_next = master - learning_rate * (
        first_next / (jnp.sqrt(second_next) + adam_eps) + decay_rate * master
    )
    return (master_next, first_next, second_next)


def remote(src, dst, send, recv, device):
    return pltpu.make_async_remote_copy(
        src_ref=src, dst_ref=dst, send_sem=send, recv_sem=recv, device_id=device, device_id_type=MESH
    )


def front_kernel(
    mixed, block, weight, head, gain, target, ids,
    cot, logit_cot, hid, window, id_window,
    table, w_all, mixed_own, block_own, final, hid_all, inv_all, inv_in, logits,
    send_sem, recv_sem, spread_send, spread_recv, local_sem,
):
    s = lax.axis_index("section")
    r = lax.axis_index("dp")
    y, xh = s // 2, s % 2
    xl, c = (r // 2) % 2, r % 2
    z = r // 4
    zin = z % 2
    before, after = lax.rem(y + 3, 4), lax.rem(y + 1, 4)
    opposite = lax.rem(y + 2, 4)
    far = 1 - xh
    section_of = lambda yy, hh: yy * 2 + hh
    to_before = {"section": section_of(before, xh), "dp": r}
    to_after = {"section": section_of(after, xh), "dp": r}
    to_cross = {"section": section_of(y, far), "dp": z * 4 + (1 - xl) * 2 + c}
    to_sibling = {"section": s, "dp": z * 4 + xl * 2 + (1 - c)}
    to_x = {"section": s, "dp": z * 4 + (1 - xl) * 2 + c}
    to_z = {"section": s, "dp": (z + 1 - 2 * zin) * 4 + xl * 2 + c}
    last = 7
    share = hid.shape[0]

    def near(k):
        other_z, other_x, other_c = (zin + k // 4) % 2, (xl + (k // 2) % 2) % 2, (c + k % 2) % 2
        device = {"section": s, "dp": (z - zin + other_z) * 4 + other_x * 2 + other_c}
        return other_z * 4 + other_x * 2 + other_c, device

    table_load = pltpu.make_async_copy(head, table.at[pl.ds(s * 256, 256)], local_sem.at[0])
    table_load.start()
    mixed_load = pltpu.make_async_copy(mixed, mixed_own, local_sem.at[1])
    block_load = pltpu.make_async_copy(block, block_own, local_sem.at[2])
    weight_load = [
        pltpu.make_async_copy(weight.at[pl.ds(k * 256, 256)], w_all.at[pl.ds(k * 256, 256)], local_sem.at[3 + k])
        for k in range(8)
    ]

    @pl.when(s == last)
    def _():
        mixed_load.start()
        for k in range(8):
            weight_load[k].start()
        block_load.start()

    barrier = pltpu.get_barrier_semaphore()
    for step in range(1, 8):
        pl.semaphore_signal(
            barrier, inc=1, device_id={"section": lax.rem(s + step, 8), "dp": r}, device_id_type=MESH
        )
    pl.semaphore_signal(barrier, inc=1, device_id=to_cross, device_id_type=MESH)
    for k in range(1, 8):
        pl.semaphore_signal(barrier, inc=1, device_id=near(k)[1], device_id_type=MESH)
    pl.semaphore_wait(barrier, 15)

    started = []

    def go(src, dst, number, device):
        copy = remote(src, dst, send_sem.at[len(started)], recv_sem.at[number], device)
        copy.start()
        started.append(copy)

    def arrived(dst, number):
        remote(dst, dst, send_sem.at[0], recv_sem.at[number], to_sibling).wait_recv()

    slot = zin * 4 + xl * 2 + c
    slot_x = zin * 4 + (1 - xl) * 2 + c
    slot_z = (1 - zin) * 4 + xl * 2 + c
    slot_xz = (1 - zin) * 4 + (1 - xl) * 2 + c
    go(mixed, window.at[slot], 31, to_x)
    go(mixed, window.at[slot], 32, to_z)
    go(mixed, window.at[slot], 35, to_sibling)

    for k in range(1, 8):
        go(ids, id_window.at[slot], 39 + k - 1, near(k)[1])
    id_window[slot] = ids[...]

    def rows(yy, hh, p, half=None, core=None):
        start = section_of(yy, hh) * 256 + (c if core is None else core) * 128 + p * 64
        if half is None:
            return table.at[pl.ds(start, 64)]
        return table.at[pl.ds(start + half * 32, 32)]

    def pass_on(ref, number, device):
        go(ref, ref, number, device)

    table_load.wait()
    pass_on(rows(y, xh, 1), 6, to_before)
    pass_on(rows(y, xh, 1), 5, to_after)
    pass_on(rows(y, xh, 0), 0, to_cross)
    pass_on(rows(y, xh, 0), 8, to_before)
    pass_on(rows(y, xh, 0), 7, to_after)
    pass_on(rows(y, xh, 1), 1, to_cross)

    def piece(k, number):
        at = pl.ds(k * share, share)
        target_device = {"section": k, "dp": r}
        return (
            remote(hid_all.at[at], hid, spread_send.at[k], spread_recv.at[0], target_device),
            remote(inv_all.at[at], inv_in, spread_send.at[8 + k], spread_recv.at[1], target_device),
        )

    @pl.when(s == last)
    def _():
        mixed_load.wait()
        for k in range(8):
            weight_load[k].wait()
        block_load.wait()

        @pl.loop(0, 8)
        def _(k):
            at = pl.ds(pl.multiple_of(k * 256, 256), 256)
            final[:, at] = block_own[:, at].astype(jnp.float32) + times_transposed(mixed_own[...], w_all[at, :])

        for k in range(8):
            at = pl.ds(k * share, share)
            value = final[at, :]
            inverse = lax.rsqrt(jnp.mean(value * value, axis=-1, keepdims=True) + norm_eps)
            normed = (value * inverse * gain[...]).astype(jnp.bfloat16)
            wide_inverse = jnp.broadcast_to(inverse, (share, 128))
            if k < last:
                hid_all[at, :] = normed
                inv_all[at, :] = wide_inverse
                for copy in piece(k, 0):
                    copy.start()
            else:
                hid[...] = normed
                inv_in[...] = wide_inverse

    sibling_numbers = []

    def share_chunk(yy, hh, p):
        number = 17 + len(sibling_numbers)
        sibling_numbers.append((yy, hh, p, number))
        pass_on(rows(yy, hh, p), number, to_sibling)

    arrived(rows(before, xh, 1), 5)
    pass_on(rows(before, xh, 1, 0), 11, to_after)
    pass_on(rows(before, xh, 1), 2, to_cross)
    share_chunk(before, xh, 1)
    arrived(rows(after, xh, 1), 6)
    pass_on(rows(after, xh, 1, 1), 12, to_before)
    pass_on(rows(after, xh, 1), 3, to_cross)
    share_chunk(after, xh, 1)
    arrived(rows(y, far, 0), 0)
    pass_on(rows(y, far, 0), 9, to_after)
    pass_on(rows(y, far, 0), 10, to_before)
    share_chunk(y, far, 0)
    arrived(rows(before, xh, 0), 7)
    pass_on(rows(before, xh, 0, 0), 13, to_after)
    share_chunk(before, xh, 0)
    arrived(rows(after, xh, 0), 8)
    pass_on(rows(after, xh, 0, 1), 14, to_before)
    share_chunk(after, xh, 0)
    arrived(rows(opposite, xh, 1, 0), 11)
    arrived(rows(opposite, xh, 1, 1), 12)
    pass_on(rows(opposite, xh, 1), 4, to_cross)
    share_chunk(opposite, xh, 1)
    arrived(rows(y, far, 1), 1)
    share_chunk(y, far, 1)
    arrived(rows(before, far, 0), 9)
    pass_on(rows(before, far, 0, 0), 15, to_after)
    share_chunk(before, far, 0)
    arrived(rows(after, far, 0), 10)
    pass_on(rows(after, far, 0, 1), 16, to_before)
    share_chunk(after, far, 0)

    half = mixed.shape[0] // 2
    arrived(window.at[slot_z], 32)
    go(window.at[slot_z, pl.ds(0, half)], window.at[slot_z, pl.ds(0, half)], 33, to_x)
    go(window.at[slot_z], window.at[slot_z], 37, to_sibling)
    arrived(window.at[slot_x], 31)
    go(window.at[slot_x, pl.ds(half, half)], window.at[slot_x, pl.ds(half, half)], 34, to_z)
    go(window.at[slot_x], window.at[slot_x], 36, to_sibling)

    arrived(rows(before, far, 1), 2)
    share_chunk(before, far, 1)
    arrived(rows(after, far, 1), 3)
    share_chunk(after, far, 1)
    arrived(rows(opposite, xh, 0, 0), 13)
    arrived(rows(opposite, xh, 0, 1), 14)
    share_chunk(opposite, xh, 0)
    arrived(rows(opposite, far, 0, 0), 15)
    arrived(rows(opposite, far, 0, 1), 16)
    share_chunk(opposite, far, 0)
    arrived(rows(opposite, far, 1), 4)
    share_chunk(opposite, far, 1)

    @pl.when(s != last)
    def _():
        for copy in piece(0, 0):
            copy.wait_recv()

    for yy, hh, p, number in sibling_numbers:
        arrived(rows(yy, hh, p, core=1 - c), number)

    @pl.loop(0, 8)
    def _(k):
        at = pl.ds(pl.multiple_of(k * 256, 256), 256)
        logits[:, at] = times_transposed(hid[...], table[at, :])

    value = logits[...]
    weights = jnp.exp(value - jnp.max(value, axis=-1, keepdims=True))
    predicted = weights / jnp.sum(weights, axis=-1, keepdims=True)
    columns = lax.broadcasted_iota(jnp.int32, value.shape, 1)
    logit_cot[...] = jnp.where(columns == target[...], predicted - 1.0, predicted).astype(jnp.bfloat16)

    @pl.loop(0, 8)
    def _(k):
        at = pl.ds(pl.multiple_of(k * 256, 256), 256)
        logits[:, at] = plain_times(logit_cot[...], table[:, at]) * gain[:, at]

    scaled = logits[...]
    unit = hid[...].astype(jnp.float32) / gain[...]
    cot[...] = (
        inv_in[:, :1] * (scaled - unit * jnp.mean(scaled * unit, axis=-1, keepdims=True))
    ).astype(jnp.bfloat16)

    @pl.when(s == last)
    def _():
        for k in range(last):
            for copy in piece(k, 0):
                copy.wait_send()

    arrived(window.at[slot_xz, pl.ds(0, half)], 33)
    arrived(window.at[slot_xz, pl.ds(half, half)], 34)
    go(window.at[slot_xz], window.at[slot_xz], 38, to_sibling)
    for number, at in ((35, slot), (36, slot_x), (37, slot_z), (38, slot_xz)):
        arrived(window.at[at + 1 - 2 * c], number)
    for k in range(1, 8):
        arrived(id_window.at[near(k)[0]], 39 + k - 1)
    for copy in started:
        copy.wait_send()


def front(mixed, block, weight, head, gain, target, ids):
    tokens, width = mixed.shape
    vmem = pl.BlockSpec(memory_space=pltpu.VMEM)
    anywhere = pl.BlockSpec(memory_space=pl.ANY)
    share = tokens // 8
    return pl.pallas_call(
        front_kernel,
        out_shape=[
            jax.ShapeDtypeStruct((share, width), jnp.bfloat16),
            jax.ShapeDtypeStruct((share, width), jnp.bfloat16),
            jax.ShapeDtypeStruct((share, width), jnp.bfloat16),
            jax.ShapeDtypeStruct((8, tokens, width), jnp.bfloat16),
            jax.ShapeDtypeStruct((8, 1, tokens), jnp.int32),
        ],
        in_specs=[anywhere, anywhere, anywhere, anywhere, vmem, vmem, vmem],
        out_specs=[vmem, vmem, vmem, anywhere, vmem],
        scratch_shapes=[
            pltpu.VMEM((2048, width), jnp.bfloat16),
            pltpu.VMEM((width, width), jnp.bfloat16),
            pltpu.VMEM((tokens, width), jnp.bfloat16),
            pltpu.VMEM((tokens, width), jnp.bfloat16),
            pltpu.VMEM((tokens, width), jnp.float32),
            pltpu.VMEM((tokens, width), jnp.bfloat16),
            pltpu.VMEM((tokens, 128), jnp.float32),
            pltpu.VMEM((share, 128), jnp.float32),
            pltpu.VMEM((share, 2048), jnp.float32),
            pltpu.SemaphoreType.DMA((48,)),
            pltpu.SemaphoreType.DMA((46,)),
            pltpu.SemaphoreType.DMA((16,)),
            pltpu.SemaphoreType.DMA((2,)),
            pltpu.SemaphoreType.DMA((11,)),
        ],
        compiler_params=pltpu.CompilerParams(collective_id=0, has_side_effects=True),
        name="front",
    )(mixed, block, weight, head, gain, target, ids)


def back_kernel(
    cot, logit_cot, hid, mixed, window, ids,
    out_grad, head_grad, embed_grad,
    mix, cot_all, hid_all, lc_all, cot_t, part, out_send, out_own, out_recv, rows_send, rows_recv,
    send_sem, recv_sem, swap_sem, rows_send_sem, rows_recv_sem, local_sem,
):
    s = lax.axis_index("section")
    r = lax.axis_index("dp")
    y, xh = s // 2, s % 2
    z, xl, c = r // 4, (r // 2) % 2, r % 2
    zin = z % 2
    pair = z // 2
    before, after = lax.rem(y + 3, 4), lax.rem(y + 1, 4)
    opposite = lax.rem(y + 2, 4)
    far = 1 - xh
    section_of = lambda yy, hh: yy * 2 + hh
    to_before = {"section": section_of(before, xh), "dp": r}
    to_after = {"section": section_of(after, xh), "dp": r}
    to_far = {"section": section_of(y, far), "dp": r}
    slot = zin * 4 + xl * 2 + c

    def near(k):
        other_z, other_x, other_c = (zin + k // 4) % 2, (xl + (k // 2) % 2) % 2, (c + k % 2) % 2
        return other_z, other_x, other_c

    def slot_of(k):
        other_z, other_x, other_c = near(k)
        return other_z * 4 + other_x * 2 + other_c

    def peer_of(k):
        other_z, other_x, other_c = near(k)
        return {"section": s, "dp": (pair * 2 + other_z) * 4 + other_x * 2 + other_c}

    def owner_z(zz, cc, b):
        distance = cc if b == 0 else 3 - cc
        return lax.rem(zz + 8 + (2 * (zz % 2) - 1) * distance, 8)

    def column_block(k, b):
        other_z, other_x, other_c = near(k)
        return owner_z(pair * 2 + other_z, other_c, b) * 2 + other_x

    loads = []
    for k in range(8):
        source = mixed if k == 0 else window.at[slot_of(k)]
        load = pltpu.make_async_copy(source, mix.at[:, slot_of(k)], local_sem.at[k])
        load.start()
        loads.append(load)

    barrier = pltpu.get_barrier_semaphore()

    @pl.loop(1, 8)
    def _(step):
        pl.semaphore_signal(
            barrier, inc=1, device_id={"section": lax.rem(s + step, 8), "dp": r}, device_id_type=MESH
        )

    @pl.loop(1, 32)
    def _(step):
        pl.semaphore_signal(
            barrier, inc=1, device_id={"section": s, "dp": lax.rem(r + step, 32)}, device_id_type=MESH
        )

    pl.semaphore_wait(barrier, 38)

    started = []

    def go(src, dst, recv, device):
        copy = remote(src, dst, send_sem.at[len(started)], recv, device)
        copy.start()
        started.append(copy)

    def arrived(dst, recv):
        remote(dst, dst, send_sem.at[0], recv, to_far).wait_recv()

    def swap_columns(array, spread, base):
        for k in range(1, 8):
            for b in range(2):
                columns = pl.ds(pl.multiple_of(column_block(k, b) * 128, 128), 128)
                go(array.at[:, columns], spread.at[b, s, slot], swap_sem.at[base + slot * 2 + b], peer_of(k))
        for b in range(2):
            columns = pl.ds(pl.multiple_of(column_block(0, b) * 128, 128), 128)
            spread[b, s, slot] = array[:, columns]

    def wait_columns(spread, base):
        for k in range(1, 8):
            for b in range(2):
                arrived(spread.at[b, s, slot_of(k)], swap_sem.at[base + slot_of(k) * 2 + b])

    def at_section(spread, section):
        return spread.at[:, section]

    def pass_on(ref, number, device):
        go(ref, ref, recv_sem.at[number], device)

    def gather_start(spread, base):
        own = at_section(spread, s)
        pass_on(own, base, to_far)
        pass_on(own, base + 2, to_before)
        pass_on(own, base + 1, to_after)

    def gather_near(spread, base):
        arrived(at_section(spread, section_of(before, xh)), recv_sem.at[base + 1])
        pass_on(spread.at[0, section_of(before, xh)], base + 5, to_after)
        arrived(at_section(spread, section_of(after, xh)), recv_sem.at[base + 2])
        pass_on(spread.at[1, section_of(after, xh)], base + 6, to_before)

    def gather_far(spread, base):
        block = at_section(spread, section_of(y, far))
        arrived(block, recv_sem.at[base])
        pass_on(block, base + 4, to_before)
        pass_on(block, base + 3, to_after)

    def gather_far_near(spread, base):
        arrived(at_section(spread, section_of(before, far)), recv_sem.at[base + 3])
        pass_on(spread.at[0, section_of(before, far)], base + 7, to_after)
        arrived(at_section(spread, section_of(after, far)), recv_sem.at[base + 4])
        pass_on(spread.at[1, section_of(after, far)], base + 8, to_before)

    def gather_end(spread, base):
        arrived(spread.at[0, section_of(opposite, xh)], recv_sem.at[base + 5])
        arrived(spread.at[1, section_of(opposite, xh)], recv_sem.at[base + 6])
        arrived(spread.at[0, section_of(opposite, far)], recv_sem.at[base + 7])
        arrived(spread.at[1, section_of(opposite, far)], recv_sem.at[base + 8])

    swap_columns(cot, cot_all, 0)
    swap_columns(hid, hid_all, 16)
    for step in range(1, 8):
        target = lax.rem(s + step, 8)
        columns = pl.ds(pl.multiple_of(target * 256, 256), 256)
        go(logit_cot.at[:, columns], lc_all.at[s, slot], swap_sem.at[32 + s], {"section": target, "dp": r})
    lc_all[s, slot] = logit_cot[:, pl.ds(pl.multiple_of(s * 256, 256), 256)]

    wait_columns(cot_all, 0)
    gather_start(cot_all, 0)
    wait_columns(hid_all, 16)
    gather_start(hid_all, 9)
    for step in range(1, 8):
        source = lax.rem(s + step, 8)
        arrived(lc_all.at[source, slot], swap_sem.at[32 + source])
    lc_own = lc_all.at[:, slot]
    for k in (2, 4, 6, 1):
        pass_on(lc_own, 18 + k, peer_of(k))

    gather_near(cot_all, 0)
    gather_far(cot_all, 0)
    gather_near(hid_all, 9)
    for k in (2, 4, 6):
        block = lc_all.at[:, slot_of(k)]
        arrived(block, recv_sem.at[18 + k])
        pass_on(block, 18 + k + 1, peer_of(1))
    gather_far_near(cot_all, 0)
    gather_far(hid_all, 9)
    gather_end(cot_all, 0)
    gather_far_near(hid_all, 9)

    for b in range(2):
        cot_t[pl.ds(b * 128, 128), :] = cot_all[b].reshape(2048, 128).T
    for load in loads:
        load.wait()

    @pl.loop(0, 8)
    def _(k):
        at = pl.ds(pl.multiple_of(k * 256, 256), 256)
        product = plain_times(cot_t[...], mix[:, :, :, at].reshape(2048, 256))
        part[:, at] = product[:128]
        out_send[:, :, at] = product.reshape(4, 64, 256).astype(jnp.bfloat16)

    sign = 2 * zin - 1

    def owner(distance, core):
        return {"section": s, "dp": lax.rem(z + 8 + sign * distance, 8) * 4 + xl * 2 + core}

    def far_rows(number, b, core, distance):
        return remote(
            out_send.at[2 * b + core],
            out_recv.at[distance - 1],
            rows_send_sem.at[64 + number],
            rows_recv_sem.at[63 + distance],
            owner(distance, core),
        )

    def sibling_rows():
        return remote(
            part.at[pl.ds(64, 64)], out_own, rows_send_sem.at[64], rows_recv_sem.at[67], owner(0, 1)
        )

    def even_core():
        return [sibling_rows(), far_rows(1, 1, 0, 3), far_rows(2, 1, 1, 3)]

    def odd_core():
        return [far_rows(2 * b + core, b, core, 1 + b) for b in (1, 0) for core in range(2)]

    @pl.when(c == 0)
    def _():
        for copy in even_core():
            copy.start()

    @pl.when(c == 1)
    def _():
        for copy in odd_core():
            copy.start()

    vocabulary = s * 256 + lax.broadcasted_iota(jnp.int32, (256, 256), 0)
    for b in range(2):
        total = jnp.zeros((256, 128), jnp.float32)
        for k in range(8):
            marks = jnp.where(vocabulary == ids[k], 1.0, 0.0).astype(jnp.bfloat16)
            total = total + plain_times(marks, cot_all[b, :, k].reshape(256, 128))
        rows_send[b, :, 8:16, :] = total.reshape(32, 8, 128)

    gather_end(hid_all, 9)
    for k in (1, 3, 5, 7):
        arrived(lc_all.at[:, slot_of(k)], recv_sem.at[18 + k])
    for b in range(2):
        product = transposed_times(lc_all[...].reshape(2048, 256), hid_all[b].reshape(2048, 128))
        rows_send[b, :, 0:8, :] = product.reshape(32, 8, 128)

    def row_copy(target, sender, b):
        columns = pl.ds(pl.multiple_of(column_block(0, b) * 128, 128), 128)
        return remote(
            rows_send.at[b, target],
            rows_recv.at[pair, :, columns],
            rows_send_sem.at[2 * target + b],
            rows_recv_sem.at[2 * sender + b],
            {"section": s, "dp": target},
        )

    for b in range(2):
        columns = pl.ds(pl.multiple_of(column_block(0, b) * 128, 128), 128)

        @pl.loop(1, 32)
        def _(step):
            row_copy(lax.rem(r + step, 32), r, b).start()

        rows_recv[pair, :, columns] = rows_send[b, r]

    @pl.when(c == 1)
    def _():
        remote(out_own, out_own, send_sem.at[0], rows_recv_sem.at[67], to_far).wait_recv()

    @pl.when(c == 0)
    def _():
        out_own[...] = part[:64, :]

    for distance in (1, 2, 3):
        arrived(out_recv.at[distance - 1], rows_recv_sem.at[63 + distance])
    total = out_own[...]
    for distance in (1, 2, 3):
        total = total + out_recv[distance - 1].astype(jnp.float32)
    out_grad[...] = total

    for b in range(2):

        @pl.loop(1, 32)
        def _(step):
            row_copy(r, lax.rem(r + step, 32), b).wait_recv()

    summed = rows_recv[0] + rows_recv[1] + rows_recv[2] + rows_recv[3]
    head_grad[...] = summed[:8]
    embed_grad[...] = summed[8:]

    for b in range(2):

        @pl.loop(1, 32)
        def _(step):
            row_copy(lax.rem(r + step, 32), r, b).wait_send()

    @pl.when(c == 0)
    def _():
        for copy in even_core():
            copy.wait_send()

    @pl.when(c == 1)
    def _():
        for copy in odd_core():
            copy.wait_send()

    for copy in started:
        copy.wait_send()


def back(cot, logit_cot, hid, mixed, window, ids):
    vmem = pl.BlockSpec(memory_space=pltpu.VMEM)
    anywhere = pl.BlockSpec(memory_space=pl.ANY)
    width = cot.shape[1]
    return pl.pallas_call(
        back_kernel,
        out_shape=[
            jax.ShapeDtypeStruct((64, width), jnp.float32),
            jax.ShapeDtypeStruct((8, width), jnp.float32),
            jax.ShapeDtypeStruct((8, width), jnp.float32),
        ],
        in_specs=[vmem, vmem, vmem, anywhere, anywhere, vmem],
        out_specs=[vmem, vmem, vmem],
        scratch_shapes=[
            pltpu.VMEM((8, 8, 32, width), jnp.bfloat16),
            pltpu.VMEM((2, 8, 8, 32, 128), jnp.bfloat16),
            pltpu.VMEM((2, 8, 8, 32, 128), jnp.bfloat16),
            pltpu.VMEM((8, 8, 32, 256), jnp.bfloat16),
            pltpu.VMEM((256, 2048), jnp.bfloat16),
            pltpu.VMEM((128, width), jnp.float32),
            pltpu.VMEM((4, 64, width), jnp.bfloat16),
            pltpu.VMEM((64, width), jnp.float32),
            pltpu.VMEM((3, 64, width), jnp.bfloat16),
            pltpu.VMEM((2, 32, 16, 128), jnp.float32),
            pltpu.VMEM((4, 16, width), jnp.float32),
            pltpu.SemaphoreType.DMA((64,)),
            pltpu.SemaphoreType.DMA((26,)),
            pltpu.SemaphoreType.DMA((40,)),
            pltpu.SemaphoreType.DMA((68,)),
            pltpu.SemaphoreType.DMA((68,)),
            pltpu.SemaphoreType.DMA((8,)),
        ],
        compiler_params=pltpu.CompilerParams(collective_id=1, has_side_effects=True),
        name="back",
    )(cot, logit_cot, hid, mixed, window, ids)


def local(
    block_inputs,
    mixed_inputs,
    token_ids,
    target_ids,
    final_gain,
    out_weight,
    head_weight,
    out_master,
    out_first,
    out_second,
    head_master,
    head_first,
    head_second,
    embed_master,
    embed_first,
    embed_second,
):
    sections = lax.axis_size("section")
    section = lax.axis_index("section")
    batches, rows, width = mixed_inputs[0].shape
    tokens = batches * rows
    share = tokens // sections
    flat_mixed = mixed_inputs[0].reshape(tokens, width)
    target = lax.dynamic_slice_in_dim(target_ids.reshape(-1), section * share, share)[:, None]
    cotangent, logit_cotangent, hidden, window, ids = front(
        flat_mixed,
        block_inputs[0].reshape(tokens, width),
        out_weight[0],
        head_weight,
        final_gain.reshape(1, width),
        target,
        token_ids.reshape(1, tokens),
    )
    out_gradient, head_gradient, embed_gradient = back(
        cotangent,
        logit_cotangent,
        hidden,
        flat_mixed.reshape(sections, share, width),
        window.reshape(8, sections, share, width),
        ids,
    )
    out_out = adam_update(out_master, out_first, out_second, out_gradient.reshape(out_master.shape))
    head_out = adam_update(head_master, head_first, head_second, head_gradient)
    embed_out = adam_update(embed_master, embed_first, embed_second, embed_gradient)
    return out_out + head_out + embed_out


def solution(mesh):
    step = jax.shard_map(
        local,
        mesh=mesh,
        in_specs=(
            P("section", None, "dp", None),
            P("section", None, "dp", None),
            P(None, "dp"),
            P(None, "dp"),
            P(),
            P("section", None, None),
            P("section", None),
            P("section", "dp", None),
            P("section", "dp", None),
            P("section", "dp", None),
            P(("section", "dp"), None),
            P(("section", "dp"), None),
            P(("section", "dp"), None),
            P(("section", "dp"), None),
            P(("section", "dp"), None),
            P(("section", "dp"), None),
        ),
        out_specs=(
            P("section", "dp", None),
            P("section", "dp", None),
            P("section", "dp", None),
            P(("section", "dp"), None),
            P(("section", "dp"), None),
            P(("section", "dp"), None),
            P(("section", "dp"), None),
            P(("section", "dp"), None),
            P(("section", "dp"), None),
        ),
        check_vma=False,
    )
    return step
```

```python
import jax
import jax.numpy as jnp
from jax import lax
from jax.experimental import pallas as pl
from jax.experimental.pallas import tpu as pltpu
from jax.sharding import PartitionSpec as P

norm_eps = 1e-05
beta_first = 0.9
beta_second = 0.95
adam_eps = 1e-05
learning_rate = 0.0003
decay_rate = 0.1

MESH = pl.DeviceIdType.MESH


def times_transposed(former, latter):
    return lax.dot_general(
        former, latter, (((1,), (1,)), ((), ())), preferred_element_type=jnp.float32
    )


def transposed_times(former, latter):
    return lax.dot_general(
        former, latter, (((0,), (0,)), ((), ())), preferred_element_type=jnp.float32
    )


def plain_times(former, latter):
    return jnp.dot(former, latter, preferred_element_type=jnp.float32)


def adam_update(master, first, second, gradient):
    first_next = beta_first * first + (1.0 - beta_first) * gradient
    second_next = beta_second * second + (1.0 - beta_second) * gradient * gradient
    master_next = master - learning_rate * (
        first_next / (jnp.sqrt(second_next) + adam_eps) + decay_rate * master
    )
    return (master_next, first_next, second_next)


def remote(src, dst, send, recv, device):
    return pltpu.make_async_remote_copy(
        src_ref=src, dst_ref=dst, send_sem=send, recv_sem=recv, device_id=device, device_id_type=MESH
    )


def step_kernel(
    mixed, block, weight, head, gain, target, ids,
    out_grad, head_grad, embed_grad,
    table, w_all, block_own, final, normed_all, inv_all, inv_in, hid_pass, inv_pass, logits, hid, logit_cot, cot,
    own_ids, id_all, mix, cot_all, hid_all, lc_all, cot_t, part, out_send, out_own, out_recv,
    head_send, embed_send, head_recv, embed_recv,
    send_sem, recv_sem, spread_send, spread_recv, far_send, far_recv, local_sem,
):
    s = lax.axis_index("section")
    r = lax.axis_index("dp")
    y, xh = s // 2, s % 2
    z, xl, c = r // 4, (r // 2) % 2, r % 2
    zin = z % 2
    even_z = lax.rem(z + 8 - 3 * zin, 8)
    pair = even_z // 2
    before, after = lax.rem(y + 3, 4), lax.rem(y + 1, 4)
    opposite = lax.rem(y + 2, 4)
    far = 1 - xh
    last = 7
    share = hid.shape[0]
    section_of = lambda yy, hh: yy * 2 + hh
    to_before = {"section": section_of(before, xh), "dp": r}
    to_after = {"section": section_of(after, xh), "dp": r}
    to_far = {"section": section_of(y, far), "dp": r}
    to_cross = {"section": section_of(y, far), "dp": z * 4 + (1 - xl) * 2 + c}

    def near(k):
        return (zin + k // 4) % 2, (xl + (k // 2) % 2) % 2, (c + k % 2) % 2

    def slot_of(k):
        other_z, other_x, other_c = near(k)
        return other_z * 4 + other_x * 2 + other_c

    def z_of(other_z):
        return lax.rem(even_z + 3 * other_z, 8)

    def peer_of(k):
        other_z, other_x, other_c = near(k)
        return {"section": s, "dp": z_of(other_z) * 4 + other_x * 2 + other_c}

    def owner_z(zz, cc, b):
        delta = cc if b == 0 else 2 - 3 * cc
        return lax.rem(zz + 8 + (2 * (zz % 2) - 1) * delta, 8)

    def column_block(k, b):
        other_z, other_x, other_c = near(k)
        return owner_z(z_of(other_z), other_c, b) * 2 + other_x

    def columns_of(k, b):
        return pl.ds(pl.multiple_of(column_block(k, b) * 128, 128), 128)

    slot = slot_of(0)
    to_sibling, to_x, to_z = peer_of(1), peer_of(2), peer_of(4)

    table_load = pltpu.make_async_copy(head, table.at[pl.ds(s * 256, 256)], local_sem.at[0])
    table_load.start()
    mixed_load = pltpu.make_async_copy(mixed, mix.at[:, slot], local_sem.at[1])
    mixed_load.start()
    block_load = pltpu.make_async_copy(block, block_own, local_sem.at[2])
    weight_load = [
        pltpu.make_async_copy(weight.at[pl.ds(k * 256, 256)], w_all.at[pl.ds(k * 256, 256)], local_sem.at[3 + k])
        for k in range(8)
    ]

    @pl.when(s == last)
    def _():
        for k in range(8):
            weight_load[k].start()
        block_load.start()

    barrier = pltpu.get_barrier_semaphore()
    pl.semaphore_signal(barrier, inc=1, device_id=to_cross, device_id_type=MESH)

    @pl.loop(1, 8)
    def _(step):
        pl.semaphore_signal(
            barrier, inc=1, device_id={"section": lax.rem(s + step, 8), "dp": r}, device_id_type=MESH
        )

    @pl.loop(1, 32)
    def _(step):
        pl.semaphore_signal(
            barrier, inc=1, device_id={"section": s, "dp": lax.rem(r + step, 32)}, device_id_type=MESH
        )

    for m in range(4):
        own_ids[0:1, m * 64 : (m + 1) * 64] = ids[m : m + 1, :]
    id_all[slot] = own_ids[...]
    table_load.wait()
    mixed_load.wait()
    pl.semaphore_wait(barrier, 39)

    table_out, mix_out, swap_out, cot_out, hid_out, lc_out, lc_swap_out, id_out = range(8)

    def arrived(dst, recv):
        remote(dst, dst, send_sem.at[0], recv, to_sibling).wait_recv()

    def sent(src, group):
        remote(src, src, send_sem.at[group], recv_sem.at[0], to_sibling).wait_send()

    def rows(yy, hh, p, half=None, core=None):
        start = section_of(yy, hh) * 256 + (c if core is None else core) * 128 + p * 64
        if half is None:
            return table.at[pl.ds(start, 64)]
        return table.at[pl.ds(start + half * 32, 32)]

    def make(ref, number, device, group=table_out):
        return remote(ref, ref, send_sem.at[group], recv_sem.at[number], device)

    def pass_on(ref, number, device, group=table_out):
        make(ref, number, device, group).start()

    pass_on(rows(y, xh, 1), 6, to_before)
    pass_on(rows(y, xh, 1), 5, to_after)
    pass_on(rows(y, xh, 0), 0, to_cross)
    pass_on(rows(y, xh, 0), 8, to_before)
    pass_on(rows(y, xh, 0), 7, to_after)
    for k in range(1, 8):
        remote(own_ids, id_all.at[slot], send_sem.at[id_out], recv_sem.at[39], peer_of(k)).start()

    own_mix = mix.at[:, slot]
    pass_on(own_mix, 35, to_sibling, mix_out)

    def pieces(direction, first, end, at):
        if direction == "z":
            return [make(mix.at[p, at], 40 + p // 2, to_z, mix_out) for p in range(first, end)]
        return [make(mix.at[p, at], 31 if at is slot else 33, to_x, mix_out) for p in range(first, end)]

    def feed(direction, first, end):
        for copy in pieces(direction, first, end, slot):
            copy.start()

    mix_x, mix_z, mix_xz = slot_of(2), slot_of(4), slot_of(6)

    def feed_corner(group):
        arrived(mix.at[pl.ds(2 * group, 2), mix_z], recv_sem.at[40 + group])
        for copy in pieces("x", 2 * group, 2 * group + 2, mix_z):
            copy.start()

    feed("z", 0, 3)
    bulk = [make(rows(y, xh, 1), 1, to_cross)] + pieces("x", 0, 3, slot)

    @pl.when(s != last)
    def _():
        for copy in bulk:
            copy.start()

    def piece(k):
        at = pl.ds(k * share, share)
        direct = k % 2 == 1 or k in (2, last - 1)
        target_device = {"section": k if direct else k + 1, "dp": r}
        return (
            remote(
                normed_all.at[at],
                hid if direct else hid_pass,
                spread_send.at[k],
                spread_recv.at[0 if direct else 2],
                target_device,
            ),
            remote(
                inv_all.at[at],
                inv_in if direct else inv_pass,
                spread_send.at[8 + k],
                spread_recv.at[1 if direct else 3],
                target_device,
            ),
        )

    def passed():
        return (
            remote(hid_pass, hid, spread_send.at[0], spread_recv.at[0], to_far),
            remote(inv_pass, inv_in, spread_send.at[8], spread_recv.at[1], to_far),
        )

    passes = jnp.logical_or(s == 1, s == 5)

    @pl.when(s == last)
    def _():
        for k in range(8):
            weight_load[k].wait()
        block_load.wait()

        @pl.loop(0, 8)
        def _(k):
            at = pl.ds(pl.multiple_of(k * 256, 256), 256)
            final[:, at] = block_own[:, at].astype(jnp.float32) + times_transposed(
                mix[:, slot].reshape(256, 2048), w_all[at, :]
            )

        for k in (0, 4, 2, 6, 3, 1, 5, 7):
            at = pl.ds(k * share, share)
            value = final[at, :]
            inverse = lax.rsqrt(jnp.mean(value * value, axis=-1, keepdims=True) + norm_eps)
            normed = (value * inverse * gain[...]).astype(jnp.bfloat16)
            wide_inverse = jnp.broadcast_to(inverse, (share, 128))
            if k < last:
                normed_all[at, :] = normed
                inv_all[at, :] = wide_inverse
                for copy in piece(k):
                    copy.start()
            else:
                hid[...] = normed
                inv_in[...] = wide_inverse
        for copy in bulk:
            copy.start()

    def swap_columns(array, spread, base):
        for k in range(1, 8):
            for b in range(2):
                remote(
                    array.at[:, columns_of(k, b)],
                    spread.at[b, s, slot],
                    send_sem.at[swap_out],
                    recv_sem.at[base],
                    peer_of(k),
                ).start()
        for b in range(2):
            spread[b, s, slot] = array[:, columns_of(0, b)]

    def wait_columns(spread, base):
        arrived(spread.at[:, 0, pl.ds(0, 7)], recv_sem.at[base])

    cot_base, hid_base, lc_base = 46, 55, 64

    def gather_start(spread, base):
        own = spread.at[:, s]
        pass_on(own, base, to_far, cot_out if base == cot_base else hid_out)
        pass_on(own, base + 2, to_before, cot_out if base == cot_base else hid_out)
        pass_on(own, base + 1, to_after, cot_out if base == cot_base else hid_out)

    def gather_near(spread, base):
        arrived(spread.at[:, section_of(before, xh)], recv_sem.at[base + 1])
        pass_on(spread.at[0, section_of(before, xh)], base + 5, to_after, cot_out if base == cot_base else hid_out)
        arrived(spread.at[:, section_of(after, xh)], recv_sem.at[base + 2])
        pass_on(spread.at[1, section_of(after, xh)], base + 6, to_before, cot_out if base == cot_base else hid_out)

    def gather_far(spread, base):
        other = spread.at[:, section_of(y, far)]
        arrived(other, recv_sem.at[base])
        pass_on(other, base + 4, to_before, cot_out if base == cot_base else hid_out)
        pass_on(other, base + 3, to_after, cot_out if base == cot_base else hid_out)

    def gather_far_near(spread, base):
        arrived(spread.at[:, section_of(before, far)], recv_sem.at[base + 3])
        pass_on(spread.at[0, section_of(before, far)], base + 7, to_after, cot_out if base == cot_base else hid_out)
        arrived(spread.at[:, section_of(after, far)], recv_sem.at[base + 4])
        pass_on(spread.at[1, section_of(after, far)], base + 8, to_before, cot_out if base == cot_base else hid_out)

    def gather_end(spread, base):
        arrived(spread.at[0, section_of(opposite, xh)], recv_sem.at[base + 5])
        arrived(spread.at[1, section_of(opposite, xh)], recv_sem.at[base + 6])
        arrived(spread.at[0, section_of(opposite, far)], recv_sem.at[base + 7])
        arrived(spread.at[1, section_of(opposite, far)], recv_sem.at[base + 8])

    def share_chunk(yy, hh, p):
        pass_on(rows(yy, hh, p), 17, to_sibling)

    def chunk_arrived(yy, hh, p, number, half=None):
        arrived(rows(yy, hh, p, half), recv_sem.at[number])

    chunk_arrived(before, xh, 1, 5)
    pass_on(rows(before, xh, 1, 0), 11, to_after)
    pass_on(rows(before, xh, 1), 2, to_cross)
    share_chunk(before, xh, 1)
    chunk_arrived(after, xh, 1, 6)
    pass_on(rows(after, xh, 1, 1), 12, to_before)
    pass_on(rows(after, xh, 1), 3, to_cross)
    share_chunk(after, xh, 1)
    feed("x", 3, 5)
    chunk_arrived(y, far, 0, 0)
    pass_on(rows(y, far, 0), 9, to_after)
    pass_on(rows(y, far, 0), 10, to_before)
    share_chunk(y, far, 0)
    chunk_arrived(before, xh, 0, 7)
    pass_on(rows(before, xh, 0, 0), 13, to_after)
    share_chunk(before, xh, 0)
    chunk_arrived(after, xh, 0, 8)
    pass_on(rows(after, xh, 0, 1), 14, to_before)
    share_chunk(after, xh, 0)
    feed("z", 3, 4)
    feed("x", 5, 8)
    chunk_arrived(opposite, xh, 1, 11, 0)
    chunk_arrived(opposite, xh, 1, 12, 1)
    pass_on(rows(opposite, xh, 1), 4, to_cross)
    share_chunk(opposite, xh, 1)
    chunk_arrived(y, far, 1, 1)
    share_chunk(y, far, 1)
    feed("z", 4, 5)
    feed_corner(0)
    @pl.when(passes)
    def _():
        for copy in piece(0):
            copy.wait_recv()
        for copy in passed():
            copy.start()

    chunk_arrived(before, far, 0, 9)
    pass_on(rows(before, far, 0, 0), 15, to_after)
    share_chunk(before, far, 0)
    chunk_arrived(after, far, 0, 10)
    pass_on(rows(after, far, 0, 1), 16, to_before)
    share_chunk(after, far, 0)

    feed("z", 5, 6)
    chunk_arrived(before, far, 1, 2)
    share_chunk(before, far, 1)
    chunk_arrived(after, far, 1, 3)
    share_chunk(after, far, 1)
    chunk_arrived(opposite, xh, 0, 13, 0)
    chunk_arrived(opposite, xh, 0, 14, 1)
    share_chunk(opposite, xh, 0)
    chunk_arrived(opposite, far, 0, 15, 0)
    chunk_arrived(opposite, far, 0, 16, 1)
    share_chunk(opposite, far, 0)
    @pl.when(s != last)
    def _():
        for copy in passed():
            copy.wait_recv()

    swap_columns(hid, hid_all, 36)
    feed("z", 6, 7)
    feed_corner(1)
    chunk_arrived(opposite, far, 1, 4)
    share_chunk(opposite, far, 1)
    arrived(table.at[pl.ds(0, 14 * 64)], recv_sem.at[17])

    @pl.loop(0, 8)
    def _(k):
        at = pl.ds(pl.multiple_of(k * 256, 256), 256)
        logits[:, at] = times_transposed(hid[...], table[at, :])

    value = logits[...]
    weights = jnp.exp(value - jnp.max(value, axis=-1, keepdims=True))
    predicted = weights / jnp.sum(weights, axis=-1, keepdims=True)
    columns = lax.broadcasted_iota(jnp.int32, value.shape, 1)
    target_row = target[pl.ds(s // 2, 1), :]
    here = lax.broadcasted_iota(jnp.int32, (share, 64), 1) == share * (s % 2) + lax.broadcasted_iota(
        jnp.int32, (share, 64), 0
    )
    own_target = jnp.sum(jnp.where(here, target_row.astype(jnp.float32), 0.0), axis=1, keepdims=True)
    hit = columns == own_target.astype(jnp.int32)
    logit_cot[...] = jnp.where(hit, predicted - 1.0, predicted).astype(jnp.bfloat16)

    for step in range(1, 8):
        other = lax.rem(s + step, 8)
        at = pl.ds(pl.multiple_of(other * 256, 256), 256)
        remote(
            logit_cot.at[:, at],
            lc_all.at[s, slot],
            send_sem.at[lc_swap_out],
            recv_sem.at[38],
            {"section": other, "dp": r},
        ).start()
    lc_all[s, slot] = logit_cot[:, pl.ds(pl.multiple_of(s * 256, 256), 256)]

    wait_columns(hid_all, 36)
    gather_start(hid_all, hid_base)
    @pl.loop(0, 8)
    def _(k):
        at = pl.ds(pl.multiple_of(k * 256, 256), 256)
        logits[:, at] = plain_times(logit_cot[...], table[:, at]) * gain[:, at]

    scaled = logits[...]
    unit = hid[...].astype(jnp.float32) / gain[...]
    cot[...] = (
        inv_in[:, :1] * (scaled - unit * jnp.mean(scaled * unit, axis=-1, keepdims=True))
    ).astype(jnp.bfloat16)
    swap_columns(cot, cot_all, 37)

    feed("z", 7, 8)
    wait_columns(cot_all, 37)
    gather_start(cot_all, cot_base)
    feed_corner(2)
    gather_near(hid_all, hid_base)
    arrived(lc_all.at[0, pl.ds(0, 7)], recv_sem.at[38])
    for k in (2, 4, 6, 1):
        pass_on(lc_all.at[:, slot], lc_base + k, peer_of(k), lc_out)
    gather_near(cot_all, cot_base)
    gather_far(cot_all, cot_base)
    gather_far(hid_all, hid_base)
    arrived(mix.at[:, mix_x], recv_sem.at[31])
    pass_on(mix.at[:, mix_x], 32, to_sibling, mix_out)
    feed_corner(3)
    pass_on(mix.at[:, mix_z], 34, to_sibling, mix_out)
    gather_far_near(cot_all, cot_base)
    gather_far_near(hid_all, hid_base)
    for k in (2, 4, 6):
        other = lc_all.at[:, slot_of(k)]
        arrived(other, recv_sem.at[lc_base + k])
        pass_on(other, lc_base + k + 1, to_sibling, lc_out)
    def row_copy(send, recv, send_at, recv_at, target_dp):
        return remote(
            send.at[target_dp], recv.at[pair, slot], send_at, recv_at, {"section": s, "dp": target_dp}
        )

    head_rows = (head_send, head_recv, send_sem.at[8], recv_sem.at[18])
    embed_rows = (embed_send, embed_recv, send_sem.at[9], recv_sem.at[19])

    def rows_start(refs):
        @pl.loop(1, 32)
        def _(step):
            row_copy(*refs, lax.rem(r + step, 32)).start()

        refs[1][pair, slot] = refs[0][r]

    def rows_wait(refs):
        arrived(refs[0].at[pl.ds(0, 31)], refs[3])

    def rows_end(refs):
        everything = refs[0].at[pl.ds(0, 31)]
        remote(everything, everything, refs[2], refs[3], to_sibling).wait_send()

    def rows_sum(recv, grad):
        sources = {}
        for w in range(4):
            for j in range(8):
                sender_z = (2 * w + 3 * (j // 4)) % 8
                for b in range(2):
                    delta = j % 2 if b == 0 else 2 - 3 * (j % 2)
                    owner_of = (sender_z + 8 + (2 * (sender_z % 2) - 1) * delta) % 8
                    sources.setdefault(owner_of * 2 + (j // 2) % 2, []).append((w, j, b))
        for column, senders in sources.items():
            total = 0.0
            for w, j, b in senders:
                total = total + recv[w, j, 8 * b : 8 * b + 8, :]
            grad[:, column * 128 : column * 128 + 128] = total

    gather_end(cot_all, cot_base)

    arrived(id_all.at[pl.ds(0, 7)], recv_sem.at[39])
    vocabulary = s * 256 + lax.broadcasted_iota(jnp.int32, (256, 256), 0)
    totals = [jnp.zeros((256, 128), jnp.float32)] * 2
    for k in range(8):
        marks = jnp.where(vocabulary == id_all[k], 1.0, 0.0).astype(jnp.bfloat16)
        for b in range(2):
            totals[b] = totals[b] + plain_times(marks, cot_all[b, :, k].reshape(256, 128))
    embed_send[...] = jnp.concatenate([total.reshape(32, 8, 128) for total in totals], axis=1)
    rows_start(embed_rows)
    gather_end(hid_all, hid_base)
    for k in (1, 3, 5, 7):
        arrived(lc_all.at[:, slot_of(k)], recv_sem.at[lc_base + k])
    products = [
        transposed_times(lc_all[...].reshape(2048, 256), hid_all[b].reshape(2048, 128)).reshape(32, 8, 128)
        for b in range(2)
    ]
    head_send[...] = jnp.concatenate(products, axis=1)
    rows_start(head_rows)
    arrived(mix.at[:, mix_xz], recv_sem.at[33])
    pass_on(mix.at[:, mix_xz], 44, to_sibling, mix_out)
    for number, k in ((35, 1), (32, 3), (34, 5), (44, 7)):
        arrived(mix.at[:, slot_of(k)], recv_sem.at[number])

    for b in range(2):
        cot_t[pl.ds(b * 128, 128), :] = cot_all[b].reshape(2048, 128).T

    sign = 2 * zin - 1

    def owner(delta, core):
        return {"section": s, "dp": lax.rem(z + 8 + sign * delta, 8) * 4 + xl * 2 + core}

    deltas = (0, 1, -1, 2)

    def far_rows(half, number, b, core, place):
        at = pl.ds(half * 1024, 1024)
        return remote(
            out_send.at[2 * b + core, :, at],
            out_recv.at[place - 1, :, at],
            far_send.at[half * 4 + number],
            far_recv.at[half * 4 + place],
            owner(deltas[place], core),
        )

    def sibling_rows(half):
        at = pl.ds(half * 1024, 1024)
        return remote(
            part.at[pl.ds(64, 64), at], out_own.at[:, at], far_send.at[half * 4], far_recv.at[half * 4], owner(0, 1)
        )

    def even_core(half):
        return [far_rows(half, 1, 1, 0, 3), far_rows(half, 2, 1, 1, 3), sibling_rows(half)]

    def odd_core(half):
        return [far_rows(half, 2 * b + core, b, core, 1 + b) for b in (1, 0) for core in range(2)]

    for half in range(2):

        @pl.loop(half * 4, half * 4 + 4)
        def _(k):
            at = pl.ds(pl.multiple_of(k * 256, 256), 256)
            product = plain_times(cot_t[...], mix[:, :, :, at].reshape(2048, 256))
            part[:, at] = product[:128]
            out_send[:, :, at] = product.reshape(4, 64, 256).astype(jnp.bfloat16)

        @pl.when(c == 0)
        def _():
            for copy in even_core(half):
                copy.start()

        @pl.when(c == 1)
        def _():
            for copy in odd_core(half):
                copy.start()

    for half in range(2):
        at = pl.ds(half * 1024, 1024)

        @pl.when(c == 1)
        def _():
            arrived(out_own.at[:, at], far_recv.at[half * 4])

        @pl.when(c == 0)
        def _():
            out_own[:, at] = part[:64, at]

        for place in (1, 2, 3):
            arrived(out_recv.at[place - 1, :, at], far_recv.at[half * 4 + place])
        total = out_own[:, at]
        for place in (1, 2, 3):
            total = total + out_recv[place - 1, :, at].astype(jnp.float32)
        out_grad[:, at] = total

    rows_wait(embed_rows)
    rows_sum(embed_recv, embed_grad)

    rows_wait(head_rows)
    rows_sum(head_recv, head_grad)
    rows_end(head_rows)
    rows_end(embed_rows)

    @pl.when(s == last)
    def _():
        for k in range(last):
            for copy in piece(k):
                copy.wait_send()

    @pl.when(passes)
    def _():
        for copy in passed():
            copy.wait_send()

    for half in range(2):

        @pl.when(c == 0)
        def _():
            for copy in even_core(half):
                copy.wait_send()

        @pl.when(c == 1)
        def _():
            for copy in odd_core(half):
                copy.wait_send()

    sent(table.at[pl.ds(0, 1792)], table_out)
    sent(mix.at[pl.ds(0, 7)], mix_out)
    sent(cot_all.at[0, pl.ds(0, 7), pl.ds(0, 4)], swap_out)
    sent(cot_all.at[:, pl.ds(0, 7)], cot_out)
    sent(hid_all.at[:, pl.ds(0, 7)], hid_out)
    sent(lc_all.at[pl.ds(0, 7)], lc_out)
    sent(lc_all.at[0, pl.ds(0, 7)], lc_swap_out)
    sent(id_all.at[pl.ds(0, 7)], id_out)


def gradients(mixed, block, weight, head, gain, target, ids):
    sections, share, width = mixed.shape
    tokens = sections * share
    vmem = pl.BlockSpec(memory_space=pltpu.VMEM)
    anywhere = pl.BlockSpec(memory_space=pl.ANY)
    bf16, f32 = jnp.bfloat16, jnp.float32
    dma = pltpu.SemaphoreType.DMA
    return pl.pallas_call(
        step_kernel,
        out_shape=[
            jax.ShapeDtypeStruct((64, width), f32),
            jax.ShapeDtypeStruct((8, width), f32),
            jax.ShapeDtypeStruct((8, width), f32),
        ],
        in_specs=[anywhere, anywhere, anywhere, anywhere, vmem, vmem, vmem],
        out_specs=[vmem, vmem, vmem],
        scratch_shapes=[
            pltpu.VMEM((2048, width), bf16),
            pltpu.VMEM((width, width), bf16),
            pltpu.VMEM((tokens, width), bf16),
            pltpu.VMEM((tokens, width), f32),
            pltpu.VMEM((tokens, width), bf16),
            pltpu.VMEM((tokens, 128), f32),
            pltpu.VMEM((share, 128), f32),
            pltpu.VMEM((share, width), bf16),
            pltpu.VMEM((share, 128), f32),
            pltpu.VMEM((share, 2048), f32),
            pltpu.VMEM((share, width), bf16),
            pltpu.VMEM((share, 2048), bf16),
            pltpu.VMEM((share, width), bf16),
            pltpu.VMEM((1, tokens), jnp.int32),
            pltpu.VMEM((8, 1, tokens), jnp.int32),
            pltpu.VMEM((8, 8, share, width), bf16),
            pltpu.VMEM((2, 8, 8, share, 128), bf16),
            pltpu.VMEM((2, 8, 8, share, 128), bf16),
            pltpu.VMEM((8, 8, share, 256), bf16),
            pltpu.VMEM((256, 2048), bf16),
            pltpu.VMEM((128, width), f32),
            pltpu.VMEM((4, 64, width), bf16),
            pltpu.VMEM((64, width), f32),
            pltpu.VMEM((3, 64, width), bf16),
            pltpu.VMEM((32, 16, 128), f32),
            pltpu.VMEM((32, 16, 128), f32),
            pltpu.VMEM((4, 8, 16, 128), f32),
            pltpu.VMEM((4, 8, 16, 128), f32),
            dma((10,)),
            dma((72,)),
            dma((16,)),
            dma((4,)),
            dma((8,)),
            dma((8,)),
            dma((11,)),
        ],
        compiler_params=pltpu.CompilerParams(collective_id=0, has_side_effects=True, vmem_limit_bytes=53 * 2**20),
        name="gradients",
    )(mixed, block, weight, head, gain, target, ids)


def local(
    block_inputs,
    mixed_inputs,
    token_ids,
    target_ids,
    final_gain,
    out_weight,
    head_weight,
    out_master,
    out_first,
    out_second,
    head_master,
    head_first,
    head_second,
    embed_master,
    embed_first,
    embed_second,
):
    sections = lax.axis_size("section")
    batches, rows, width = mixed_inputs[0].shape
    tokens = batches * rows
    out_gradient, head_gradient, embed_gradient = gradients(
        mixed_inputs[0].reshape(sections, tokens // sections, width),
        block_inputs[0].reshape(tokens, width),
        out_weight[0],
        head_weight,
        final_gain.reshape(1, width),
        target_ids,
        token_ids,
    )
    out_out = adam_update(out_master, out_first, out_second, out_gradient.reshape(out_master.shape))
    head_out = adam_update(head_master, head_first, head_second, head_gradient)
    embed_out = adam_update(embed_master, embed_first, embed_second, embed_gradient)
    return out_out + head_out + embed_out


def solution(mesh):
    step = jax.shard_map(
        local,
        mesh=mesh,
        in_specs=(
            P("section", None, "dp", None),
            P("section", None, "dp", None),
            P(None, "dp"),
            P(None, "dp"),
            P(),
            P("section", None, None),
            P("section", None),
            P("section", "dp", None),
            P("section", "dp", None),
            P("section", "dp", None),
            P(("section", "dp"), None),
            P(("section", "dp"), None),
            P(("section", "dp"), None),
            P(("section", "dp"), None),
            P(("section", "dp"), None),
            P(("section", "dp"), None),
        ),
        out_specs=(
            P("section", "dp", None),
            P("section", "dp", None),
            P("section", "dp", None),
            P(("section", "dp"), None),
            P(("section", "dp"), None),
            P(("section", "dp"), None),
            P(("section", "dp"), None),
            P(("section", "dp"), None),
            P(("section", "dp"), None),
        ),
        check_vma=False,
    )
    return step
```

```python
import jax
import jax.numpy as jnp
from jax import lax
from jax.experimental import pallas as pl
from jax.experimental.pallas import tpu as pltpu
from jax.sharding import PartitionSpec as P

norm_eps = 1e-05
beta_first = 0.9
beta_second = 0.95
adam_eps = 1e-05
learning_rate = 0.0003
decay_rate = 0.1

MESH = pl.DeviceIdType.MESH


def times_transposed(former, latter):
    return lax.dot_general(
        former, latter, (((1,), (1,)), ((), ())), preferred_element_type=jnp.float32
    )


def transposed_times(former, latter):
    return lax.dot_general(
        former, latter, (((0,), (0,)), ((), ())), preferred_element_type=jnp.float32
    )


def plain_times(former, latter):
    return jnp.dot(former, latter, preferred_element_type=jnp.float32)


def adam_update(master, first, second, gradient):
    first_next = beta_first * first + (1.0 - beta_first) * gradient
    second_next = beta_second * second + (1.0 - beta_second) * gradient * gradient
    master_next = master - learning_rate * (
        first_next / (jnp.sqrt(second_next) + adam_eps) + decay_rate * master
    )
    return (master_next, first_next, second_next)


def remote(src, dst, send, recv, device):
    return pltpu.make_async_remote_copy(
        src_ref=src, dst_ref=dst, send_sem=send, recv_sem=recv, device_id=device, device_id_type=MESH
    )


def step_kernel(
    mixed, block, weight, head, gain, target, ids,
    out_grad, head_grad, embed_grad,
    table, w_all, block_own, final, normed_all, inv_all, inv_in, hid_pass, inv_pass, logits, hid, logit_cot, cot,
    own_ids, id_all, mix, cot_all, hid_all, lc_all, cot_t, part, out_send, out_own, out_recv,
    head_send, embed_send, head_recv, embed_recv,
    send_sem, recv_sem, spread_send, spread_recv, far_send, far_recv, local_sem,
):
    s = lax.axis_index("section")
    r = lax.axis_index("dp")
    y, xh = s // 2, s % 2
    z, xl, c = r // 4, (r // 2) % 2, r % 2
    zin = z % 2
    even_z = lax.rem(z + 8 - 3 * zin, 8)
    pair = even_z // 2
    before, after = lax.rem(y + 3, 4), lax.rem(y + 1, 4)
    opposite = lax.rem(y + 2, 4)
    far = 1 - xh
    last = 7
    share = hid.shape[0]
    section_of = lambda yy, hh: yy * 2 + hh
    to_before = {"section": section_of(before, xh), "dp": r}
    to_after = {"section": section_of(after, xh), "dp": r}
    to_far = {"section": section_of(y, far), "dp": r}
    to_cross = {"section": section_of(y, far), "dp": z * 4 + (1 - xl) * 2 + c}

    def near(k):
        return (zin + k // 4) % 2, (xl + (k // 2) % 2) % 2, (c + k % 2) % 2

    def slot_of(k):
        other_z, other_x, other_c = near(k)
        return other_z * 4 + other_x * 2 + other_c

    def z_of(other_z):
        return lax.rem(even_z + 3 * other_z, 8)

    def peer_of(k):
        other_z, other_x, other_c = near(k)
        return {"section": s, "dp": z_of(other_z) * 4 + other_x * 2 + other_c}

    def owner_z(zz, cc, b):
        delta = cc if b == 0 else 2 - 3 * cc
        return lax.rem(zz + 8 + (2 * (zz % 2) - 1) * delta, 8)

    def column_block(k, b):
        other_z, other_x, other_c = near(k)
        return owner_z(z_of(other_z), other_c, b) * 2 + other_x

    def columns_of(k, b):
        return pl.ds(pl.multiple_of(column_block(k, b) * 128, 128), 128)

    slot = slot_of(0)
    to_sibling, to_x, to_z = peer_of(1), peer_of(2), peer_of(4)

    table_load = pltpu.make_async_copy(head, table.at[pl.ds(s * 256, 256)], local_sem.at[0])
    table_load.start()
    mixed_load = pltpu.make_async_copy(mixed, mix.at[:, slot], local_sem.at[1])
    mixed_load.start()
    block_load = pltpu.make_async_copy(block, block_own, local_sem.at[2])
    weight_load = [
        pltpu.make_async_copy(weight.at[pl.ds(k * 256, 256)], w_all.at[pl.ds(k * 256, 256)], local_sem.at[3 + k])
        for k in range(8)
    ]

    @pl.when(s == last)
    def _():
        for k in range(8):
            weight_load[k].start()
        block_load.start()

    barrier = pltpu.get_barrier_semaphore()
    pl.semaphore_signal(barrier, inc=1, device_id=to_cross, device_id_type=MESH)

    @pl.loop(1, 8)
    def _(step):
        pl.semaphore_signal(
            barrier, inc=1, device_id={"section": lax.rem(s + step, 8), "dp": r}, device_id_type=MESH
        )

    @pl.loop(1, 32)
    def _(step):
        pl.semaphore_signal(
            barrier, inc=1, device_id={"section": s, "dp": lax.rem(r + step, 32)}, device_id_type=MESH
        )

    for m in range(4):
        own_ids[0:1, m * 64 : (m + 1) * 64] = ids[m : m + 1, :]
    id_all[slot] = own_ids[...]
    table_load.wait()
    mixed_load.wait()
    pl.semaphore_wait(barrier, 39)

    table_out, mix_out, swap_out, cot_out, hid_out, lc_out, lc_swap_out, id_out = range(8)

    def arrived(dst, recv):
        remote(dst, dst, send_sem.at[0], recv, to_sibling).wait_recv()

    def sent(src, group):
        remote(src, src, send_sem.at[group], recv_sem.at[0], to_sibling).wait_send()

    def rows(yy, hh, p, half=None, core=None):
        start = section_of(yy, hh) * 256 + (c if core is None else core) * 128 + p * 64
        if half is None:
            return table.at[pl.ds(start, 64)]
        return table.at[pl.ds(start + half * 32, 32)]

    def make(ref, number, device, group=table_out):
        return remote(ref, ref, send_sem.at[group], recv_sem.at[number], device)

    def pass_on(ref, number, device, group=table_out):
        make(ref, number, device, group).start()

    pass_on(rows(y, xh, 1), 6, to_before)
    pass_on(rows(y, xh, 1), 5, to_after)
    pass_on(rows(y, xh, 0), 0, to_cross)
    pass_on(rows(y, xh, 0), 8, to_before)
    pass_on(rows(y, xh, 0), 7, to_after)
    for k in range(1, 8):
        remote(own_ids, id_all.at[slot], send_sem.at[id_out], recv_sem.at[39], peer_of(k)).start()

    own_mix = mix.at[:, slot]
    pass_on(own_mix, 35, to_sibling, mix_out)

    def pieces(direction, first, end, at):
        if direction == "z":
            return [make(mix.at[p, at], 40 + p // 2, to_z, mix_out) for p in range(first, end)]
        return [make(mix.at[p, at], 31 if at is slot else 33, to_x, mix_out) for p in range(first, end)]

    def feed(direction, first, end):
        for copy in pieces(direction, first, end, slot):
            copy.start()

    mix_x, mix_z, mix_xz = slot_of(2), slot_of(4), slot_of(6)

    def feed_corner(group):
        arrived(mix.at[pl.ds(2 * group, 2), mix_z], recv_sem.at[40 + group])
        for copy in pieces("x", 2 * group, 2 * group + 2, mix_z):
            copy.start()

    feed("z", 0, 3)
    bulk = [make(rows(y, xh, 1), 1, to_cross)] + pieces("x", 0, 3, slot)

    @pl.when(s != last)
    def _():
        for copy in bulk:
            copy.start()

    def piece(k):
        at = pl.ds(k * share, share)
        direct = k % 2 == 1 or k in (2, last - 1)
        target_device = {"section": k if direct else k + 1, "dp": r}
        return (
            remote(
                normed_all.at[at],
                hid if direct else hid_pass,
                spread_send.at[k],
                spread_recv.at[0 if direct else 2],
                target_device,
            ),
            remote(
                inv_all.at[at],
                inv_in if direct else inv_pass,
                spread_send.at[8 + k],
                spread_recv.at[1 if direct else 3],
                target_device,
            ),
        )

    def passed():
        return (
            remote(hid_pass, hid, spread_send.at[0], spread_recv.at[0], to_far),
            remote(inv_pass, inv_in, spread_send.at[8], spread_recv.at[1], to_far),
        )

    passes = jnp.logical_or(s == 1, s == 5)

    @pl.when(s == last)
    def _():
        for k in range(8):
            weight_load[k].wait()
        block_load.wait()

        @pl.loop(0, 8)
        def _(k):
            at = pl.ds(pl.multiple_of(k * 256, 256), 256)
            final[:, at] = block_own[:, at].astype(jnp.float32) + times_transposed(
                mix[:, slot].reshape(256, 2048), w_all[at, :]
            )

        for k in (0, 4, 2, 6, 3, 1, 5, 7):
            at = pl.ds(k * share, share)
            value = final[at, :]
            inverse = lax.rsqrt(jnp.mean(value * value, axis=-1, keepdims=True) + norm_eps)
            normed = (value * inverse * gain[...]).astype(jnp.bfloat16)
            wide_inverse = jnp.broadcast_to(inverse, (share, 128))
            if k < last:
                normed_all[at, :] = normed
                inv_all[at, :] = wide_inverse
                for copy in piece(k):
                    copy.start()
            else:
                hid[...] = normed
                inv_in[...] = wide_inverse
        for copy in bulk:
            copy.start()

    def swap_columns(array, spread, base):
        for k in range(1, 8):
            for b in range(2):
                remote(
                    array.at[:, columns_of(k, b)],
                    spread.at[b, s, slot],
                    send_sem.at[swap_out],
                    recv_sem.at[base],
                    peer_of(k),
                ).start()
        for b in range(2):
            spread[b, s, slot] = array[:, columns_of(0, b)]

    def wait_columns(spread, base):
        arrived(spread.at[:, 0, pl.ds(0, 7)], recv_sem.at[base])

    cot_base, hid_base, lc_base = 46, 55, 64

    def gather_start(spread, base):
        own = spread.at[:, s]
        pass_on(own, base, to_far, cot_out if base == cot_base else hid_out)
        pass_on(own, base + 2, to_before, cot_out if base == cot_base else hid_out)
        pass_on(own, base + 1, to_after, cot_out if base == cot_base else hid_out)

    def gather_near(spread, base):
        arrived(spread.at[:, section_of(before, xh)], recv_sem.at[base + 1])
        pass_on(spread.at[0, section_of(before, xh)], base + 5, to_after, cot_out if base == cot_base else hid_out)
        arrived(spread.at[:, section_of(after, xh)], recv_sem.at[base + 2])
        pass_on(spread.at[1, section_of(after, xh)], base + 6, to_before, cot_out if base == cot_base else hid_out)

    def gather_far(spread, base):
        other = spread.at[:, section_of(y, far)]
        arrived(other, recv_sem.at[base])
        pass_on(other, base + 4, to_before, cot_out if base == cot_base else hid_out)
        pass_on(other, base + 3, to_after, cot_out if base == cot_base else hid_out)

    def gather_far_near(spread, base):
        arrived(spread.at[:, section_of(before, far)], recv_sem.at[base + 3])
        pass_on(spread.at[0, section_of(before, far)], base + 7, to_after, cot_out if base == cot_base else hid_out)
        arrived(spread.at[:, section_of(after, far)], recv_sem.at[base + 4])
        pass_on(spread.at[1, section_of(after, far)], base + 8, to_before, cot_out if base == cot_base else hid_out)

    def gather_end(spread, base):
        arrived(spread.at[0, section_of(opposite, xh)], recv_sem.at[base + 5])
        arrived(spread.at[1, section_of(opposite, xh)], recv_sem.at[base + 6])
        arrived(spread.at[0, section_of(opposite, far)], recv_sem.at[base + 7])
        arrived(spread.at[1, section_of(opposite, far)], recv_sem.at[base + 8])

    shared = []

    def share_chunk(yy, hh, p):
        shared.append((yy, hh, p))
        pass_on(rows(yy, hh, p), 17 if len(shared) <= 7 else 45, to_sibling)

    def chunk_arrived(yy, hh, p, number, half=None):
        arrived(rows(yy, hh, p, half), recv_sem.at[number])

    chunk_arrived(before, xh, 1, 5)
    pass_on(rows(before, xh, 1, 0), 11, to_after)
    pass_on(rows(before, xh, 1), 2, to_cross)
    share_chunk(before, xh, 1)
    chunk_arrived(after, xh, 1, 6)
    pass_on(rows(after, xh, 1, 1), 12, to_before)
    pass_on(rows(after, xh, 1), 3, to_cross)
    share_chunk(after, xh, 1)
    feed("x", 3, 5)
    chunk_arrived(y, far, 0, 0)
    pass_on(rows(y, far, 0), 9, to_after)
    pass_on(rows(y, far, 0), 10, to_before)
    share_chunk(y, far, 0)
    chunk_arrived(before, xh, 0, 7)
    pass_on(rows(before, xh, 0, 0), 13, to_after)
    share_chunk(before, xh, 0)
    chunk_arrived(after, xh, 0, 8)
    pass_on(rows(after, xh, 0, 1), 14, to_before)
    share_chunk(after, xh, 0)
    feed("z", 3, 4)
    feed("x", 5, 8)
    chunk_arrived(opposite, xh, 1, 11, 0)
    chunk_arrived(opposite, xh, 1, 12, 1)
    pass_on(rows(opposite, xh, 1), 4, to_cross)
    share_chunk(opposite, xh, 1)
    chunk_arrived(y, far, 1, 1)
    share_chunk(y, far, 1)
    feed("z", 4, 5)
    feed_corner(0)
    @pl.when(passes)
    def _():
        for copy in piece(0):
            copy.wait_recv()
        for copy in passed():
            copy.start()

    chunk_arrived(before, far, 0, 9)
    pass_on(rows(before, far, 0, 0), 15, to_after)
    share_chunk(before, far, 0)
    chunk_arrived(after, far, 0, 10)
    pass_on(rows(after, far, 0, 1), 16, to_before)
    share_chunk(after, far, 0)

    feed("z", 5, 6)
    chunk_arrived(before, far, 1, 2)
    share_chunk(before, far, 1)
    chunk_arrived(after, far, 1, 3)
    share_chunk(after, far, 1)
    chunk_arrived(opposite, xh, 0, 13, 0)
    chunk_arrived(opposite, xh, 0, 14, 1)
    share_chunk(opposite, xh, 0)
    chunk_arrived(opposite, far, 0, 15, 0)
    chunk_arrived(opposite, far, 0, 16, 1)
    share_chunk(opposite, far, 0)
    @pl.when(s != last)
    def _():
        for copy in passed():
            copy.wait_recv()

    swap_columns(hid, hid_all, 36)
    feed("z", 6, 7)
    feed_corner(1)
    chunk_arrived(opposite, far, 1, 4)
    share_chunk(opposite, far, 1)
    def score(sections):
        for section in sections:
            at = pl.ds(pl.multiple_of(section * 256, 256), 256)
            logits[:, at] = times_transposed(hid[...], table[at, :])

    arrived(table.at[pl.ds(0, 7 * 64)], recv_sem.at[17])
    score([s, section_of(before, xh), section_of(after, xh), section_of(y, far)])
    arrived(table.at[pl.ds(0, 7 * 64)], recv_sem.at[45])

    score([section_of(opposite, xh), section_of(before, far), section_of(after, far), section_of(opposite, far)])

    value = logits[...]
    weights = jnp.exp(value - jnp.max(value, axis=-1, keepdims=True))
    predicted = weights / jnp.sum(weights, axis=-1, keepdims=True)
    columns = lax.broadcasted_iota(jnp.int32, value.shape, 1)
    target_row = target[pl.ds(s // 2, 1), :]
    here = lax.broadcasted_iota(jnp.int32, (share, 64), 1) == share * (s % 2) + lax.broadcasted_iota(
        jnp.int32, (share, 64), 0
    )
    own_target = jnp.sum(jnp.where(here, target_row.astype(jnp.float32), 0.0), axis=1, keepdims=True)
    hit = columns == own_target.astype(jnp.int32)
    logit_cot[...] = jnp.where(hit, predicted - 1.0, predicted).astype(jnp.bfloat16)

    for step in range(1, 8):
        other = lax.rem(s + step, 8)
        at = pl.ds(pl.multiple_of(other * 256, 256), 256)
        remote(
            logit_cot.at[:, at],
            lc_all.at[s, slot],
            send_sem.at[lc_swap_out],
            recv_sem.at[38],
            {"section": other, "dp": r},
        ).start()
    lc_all[s, slot] = logit_cot[:, pl.ds(pl.multiple_of(s * 256, 256), 256)]

    @pl.loop(0, 8)
    def _(k):
        at = pl.ds(pl.multiple_of(k * 256, 256), 256)
        logits[:, at] = plain_times(logit_cot[...], table[:, at]) * gain[:, at]

    scaled = logits[...]
    unit = hid[...].astype(jnp.float32) / gain[...]
    cot[...] = (
        inv_in[:, :1] * (scaled - unit * jnp.mean(scaled * unit, axis=-1, keepdims=True))
    ).astype(jnp.bfloat16)
    swap_columns(cot, cot_all, 37)

    feed("z", 7, 8)
    wait_columns(hid_all, 36)
    gather_start(hid_all, hid_base)
    wait_columns(cot_all, 37)
    gather_start(cot_all, cot_base)
    feed_corner(2)
    gather_near(hid_all, hid_base)
    arrived(lc_all.at[0, pl.ds(0, 7)], recv_sem.at[38])
    for k in (2, 4, 6, 1):
        pass_on(lc_all.at[:, slot], lc_base + k, peer_of(k), lc_out)
    gather_near(cot_all, cot_base)
    gather_far(cot_all, cot_base)
    gather_far(hid_all, hid_base)
    arrived(mix.at[:, mix_x], recv_sem.at[31])
    pass_on(mix.at[:, mix_x], 32, to_sibling, mix_out)
    feed_corner(3)
    pass_on(mix.at[:, mix_z], 34, to_sibling, mix_out)
    gather_far_near(cot_all, cot_base)
    gather_far_near(hid_all, hid_base)
    for k in (2, 4, 6):
        other = lc_all.at[:, slot_of(k)]
        arrived(other, recv_sem.at[lc_base + k])
        pass_on(other, lc_base + k + 1, to_sibling, lc_out)
    def row_copy(send, recv, send_at, recv_at, target_dp):
        return remote(
            send.at[target_dp], recv.at[pair, slot], send_at, recv_at, {"section": s, "dp": target_dp}
        )

    head_rows = (head_send, head_recv, send_sem.at[8], recv_sem.at[18])
    embed_rows = (embed_send, embed_recv, send_sem.at[9], recv_sem.at[19])

    def rows_start(refs):
        @pl.loop(1, 32)
        def _(step):
            row_copy(*refs, lax.rem(r + step, 32)).start()

        refs[1][pair, slot] = refs[0][r]

    def rows_wait(refs):
        arrived(refs[0].at[pl.ds(0, 31)], refs[3])

    def rows_end(refs):
        everything = refs[0].at[pl.ds(0, 31)]
        remote(everything, everything, refs[2], refs[3], to_sibling).wait_send()

    def rows_sum(recv, grad):
        sources = {}
        for w in range(4):
            for j in range(8):
                sender_z = (2 * w + 3 * (j // 4)) % 8
                for b in range(2):
                    delta = j % 2 if b == 0 else 2 - 3 * (j % 2)
                    owner_of = (sender_z + 8 + (2 * (sender_z % 2) - 1) * delta) % 8
                    sources.setdefault(owner_of * 2 + (j // 2) % 2, []).append((w, j, b))
        for column, senders in sources.items():
            total = 0.0
            for w, j, b in senders:
                total = total + recv[w, j, 8 * b : 8 * b + 8, :]
            grad[:, column * 128 : column * 128 + 128] = total

    gather_end(cot_all, cot_base)

    arrived(id_all.at[pl.ds(0, 7)], recv_sem.at[39])
    vocabulary = s * 256 + lax.broadcasted_iota(jnp.int32, (256, 256), 0)
    totals = [jnp.zeros((256, 128), jnp.float32)] * 2
    for k in range(8):
        marks = jnp.where(vocabulary == id_all[k], 1.0, 0.0).astype(jnp.bfloat16)
        for b in range(2):
            totals[b] = totals[b] + plain_times(marks, cot_all[b, :, k].reshape(256, 128))
    embed_send[...] = jnp.concatenate([total.reshape(32, 8, 128) for total in totals], axis=1)
    rows_start(embed_rows)
    gather_end(hid_all, hid_base)
    for k in (1, 3, 5, 7):
        arrived(lc_all.at[:, slot_of(k)], recv_sem.at[lc_base + k])
    products = [
        transposed_times(lc_all[...].reshape(2048, 256), hid_all[b].reshape(2048, 128)).reshape(32, 8, 128)
        for b in range(2)
    ]
    head_send[...] = jnp.concatenate(products, axis=1)
    rows_start(head_rows)
    arrived(mix.at[:, mix_xz], recv_sem.at[33])
    pass_on(mix.at[:, mix_xz], 44, to_sibling, mix_out)
    for number, k in ((35, 1), (32, 3), (34, 5), (44, 7)):
        arrived(mix.at[:, slot_of(k)], recv_sem.at[number])

    for b in range(2):
        cot_t[pl.ds(b * 128, 128), :] = cot_all[b].reshape(2048, 128).T

    sign = 2 * zin - 1

    def owner(delta, core):
        return {"section": s, "dp": lax.rem(z + 8 + sign * delta, 8) * 4 + xl * 2 + core}

    deltas = (0, 1, -1, 2)

    def far_rows(half, number, b, core, place):
        at = pl.ds(half * 1024, 1024)
        return remote(
            out_send.at[2 * b + core, :, at],
            out_recv.at[place - 1, :, at],
            far_send.at[half * 4 + number],
            far_recv.at[half * 4 + place],
            owner(deltas[place], core),
        )

    def sibling_rows(half):
        at = pl.ds(half * 1024, 1024)
        return remote(
            part.at[pl.ds(64, 64), at], out_own.at[:, at], far_send.at[half * 4], far_recv.at[half * 4], owner(0, 1)
        )

    def even_core(half):
        return [far_rows(half, 1, 1, 0, 3), far_rows(half, 2, 1, 1, 3), sibling_rows(half)]

    def odd_core(half):
        return [far_rows(half, 2 * b + core, b, core, 1 + b) for b in (1, 0) for core in range(2)]

    for half in range(2):

        @pl.loop(half * 4, half * 4 + 4)
        def _(k):
            at = pl.ds(pl.multiple_of(k * 256, 256), 256)
            product = plain_times(cot_t[...], mix[:, :, :, at].reshape(2048, 256))
            part[:, at] = product[:128]
            out_send[:, :, at] = product.reshape(4, 64, 256).astype(jnp.bfloat16)

        @pl.when(c == 0)
        def _():
            for copy in even_core(half):
                copy.start()

        @pl.when(c == 1)
        def _():
            for copy in odd_core(half):
                copy.start()

    for half in range(2):
        at = pl.ds(half * 1024, 1024)

        @pl.when(c == 1)
        def _():
            arrived(out_own.at[:, at], far_recv.at[half * 4])

        @pl.when(c == 0)
        def _():
            out_own[:, at] = part[:64, at]

        for place in (1, 2, 3):
            arrived(out_recv.at[place - 1, :, at], far_recv.at[half * 4 + place])
        total = out_own[:, at]
        for place in (1, 2, 3):
            total = total + out_recv[place - 1, :, at].astype(jnp.float32)
        out_grad[:, at] = total

    rows_wait(embed_rows)
    rows_sum(embed_recv, embed_grad)

    rows_wait(head_rows)
    rows_sum(head_recv, head_grad)
    rows_end(head_rows)
    rows_end(embed_rows)

    @pl.when(s == last)
    def _():
        for k in range(last):
            for copy in piece(k):
                copy.wait_send()

    @pl.when(passes)
    def _():
        for copy in passed():
            copy.wait_send()

    for half in range(2):

        @pl.when(c == 0)
        def _():
            for copy in even_core(half):
                copy.wait_send()

        @pl.when(c == 1)
        def _():
            for copy in odd_core(half):
                copy.wait_send()

    sent(table.at[pl.ds(0, 1792)], table_out)
    sent(mix.at[pl.ds(0, 7)], mix_out)
    sent(cot_all.at[0, pl.ds(0, 7), pl.ds(0, 4)], swap_out)
    sent(cot_all.at[:, pl.ds(0, 7)], cot_out)
    sent(hid_all.at[:, pl.ds(0, 7)], hid_out)
    sent(lc_all.at[pl.ds(0, 7)], lc_out)
    sent(lc_all.at[0, pl.ds(0, 7)], lc_swap_out)
    sent(id_all.at[pl.ds(0, 7)], id_out)


def gradients(mixed, block, weight, head, gain, target, ids):
    sections, share, width = mixed.shape
    tokens = sections * share
    vmem = pl.BlockSpec(memory_space=pltpu.VMEM)
    anywhere = pl.BlockSpec(memory_space=pl.ANY)
    bf16, f32 = jnp.bfloat16, jnp.float32
    dma = pltpu.SemaphoreType.DMA
    return pl.pallas_call(
        step_kernel,
        out_shape=[
            jax.ShapeDtypeStruct((64, width), f32),
            jax.ShapeDtypeStruct((8, width), f32),
            jax.ShapeDtypeStruct((8, width), f32),
        ],
        in_specs=[anywhere, anywhere, anywhere, anywhere, vmem, vmem, vmem],
        out_specs=[vmem, vmem, vmem],
        scratch_shapes=[
            pltpu.VMEM((2048, width), bf16),
            pltpu.VMEM((width, width), bf16),
            pltpu.VMEM((tokens, width), bf16),
            pltpu.VMEM((tokens, width), f32),
            pltpu.VMEM((tokens, width), bf16),
            pltpu.VMEM((tokens, 128), f32),
            pltpu.VMEM((share, 128), f32),
            pltpu.VMEM((share, width), bf16),
            pltpu.VMEM((share, 128), f32),
            pltpu.VMEM((share, 2048), f32),
            pltpu.VMEM((share, width), bf16),
            pltpu.VMEM((share, 2048), bf16),
            pltpu.VMEM((share, width), bf16),
            pltpu.VMEM((1, tokens), jnp.int32),
            pltpu.VMEM((8, 1, tokens), jnp.int32),
            pltpu.VMEM((8, 8, share, width), bf16),
            pltpu.VMEM((2, 8, 8, share, 128), bf16),
            pltpu.VMEM((2, 8, 8, share, 128), bf16),
            pltpu.VMEM((8, 8, share, 256), bf16),
            pltpu.VMEM((256, 2048), bf16),
            pltpu.VMEM((128, width), f32),
            pltpu.VMEM((4, 64, width), bf16),
            pltpu.VMEM((64, width), f32),
            pltpu.VMEM((3, 64, width), bf16),
            pltpu.VMEM((32, 16, 128), f32),
            pltpu.VMEM((32, 16, 128), f32),
            pltpu.VMEM((4, 8, 16, 128), f32),
            pltpu.VMEM((4, 8, 16, 128), f32),
            dma((10,)),
            dma((72,)),
            dma((16,)),
            dma((4,)),
            dma((8,)),
            dma((8,)),
            dma((11,)),
        ],
        compiler_params=pltpu.CompilerParams(collective_id=0, has_side_effects=True, vmem_limit_bytes=53 * 2**20),
        name="gradients",
    )(mixed, block, weight, head, gain, target, ids)


def local(
    block_inputs,
    mixed_inputs,
    token_ids,
    target_ids,
    final_gain,
    out_weight,
    head_weight,
    out_master,
    out_first,
    out_second,
    head_master,
    head_first,
    head_second,
    embed_master,
    embed_first,
    embed_second,
):
    sections = lax.axis_size("section")
    batches, rows, width = mixed_inputs[0].shape
    tokens = batches * rows
    out_gradient, head_gradient, embed_gradient = gradients(
        mixed_inputs[0].reshape(sections, tokens // sections, width),
        block_inputs[0].reshape(tokens, width),
        out_weight[0],
        head_weight,
        final_gain.reshape(1, width),
        target_ids,
        token_ids,
    )
    out_out = adam_update(out_master, out_first, out_second, out_gradient.reshape(out_master.shape))
    head_out = adam_update(head_master, head_first, head_second, head_gradient)
    embed_out = adam_update(embed_master, embed_first, embed_second, embed_gradient)
    return out_out + head_out + embed_out


def solution(mesh):
    step = jax.shard_map(
        local,
        mesh=mesh,
        in_specs=(
            P("section", None, "dp", None),
            P("section", None, "dp", None),
            P(None, "dp"),
            P(None, "dp"),
            P(),
            P("section", None, None),
            P("section", None),
            P("section", "dp", None),
            P("section", "dp", None),
            P("section", "dp", None),
            P(("section", "dp"), None),
            P(("section", "dp"), None),
            P(("section", "dp"), None),
            P(("section", "dp"), None),
            P(("section", "dp"), None),
            P(("section", "dp"), None),
        ),
        out_specs=(
            P("section", "dp", None),
            P("section", "dp", None),
            P("section", "dp", None),
            P(("section", "dp"), None),
            P(("section", "dp"), None),
            P(("section", "dp"), None),
            P(("section", "dp"), None),
            P(("section", "dp"), None),
            P(("section", "dp"), None),
        ),
        check_vma=False,
    )
    return step
```

```python
import jax
import jax.numpy as jnp
from jax import lax
from jax.experimental import pallas as pl
from jax.experimental.pallas import tpu as pltpu
from jax.sharding import PartitionSpec as P

norm_eps = 1e-05
beta_first = 0.9
beta_second = 0.95
adam_eps = 1e-05
learning_rate = 0.0003
decay_rate = 0.1

MESH = pl.DeviceIdType.MESH


def times_transposed(former, latter):
    return lax.dot_general(
        former, latter, (((1,), (1,)), ((), ())), preferred_element_type=jnp.float32
    )


def transposed_times(former, latter):
    return lax.dot_general(
        former, latter, (((0,), (0,)), ((), ())), preferred_element_type=jnp.float32
    )


def plain_times(former, latter):
    return jnp.dot(former, latter, preferred_element_type=jnp.float32)


def adam_update(master, first, second, gradient):
    first_next = beta_first * first + (1.0 - beta_first) * gradient
    second_next = beta_second * second + (1.0 - beta_second) * gradient * gradient
    master_next = master - learning_rate * (
        first_next / (jnp.sqrt(second_next) + adam_eps) + decay_rate * master
    )
    return (master_next, first_next, second_next)


def remote(src, dst, send, recv, device):
    return pltpu.make_async_remote_copy(
        src_ref=src, dst_ref=dst, send_sem=send, recv_sem=recv, device_id=device, device_id_type=MESH
    )


def step_kernel(
    mixed, block, weight, head, small,
    out_grad, head_grad, embed_grad,
    table, w_all, block_own, final, normed_all, inv_all, inv_in, hid_pass, inv_pass, logits, hid, logit_cot, cot,
    gain, own_ids, id_all, mix, cot_all, hid_all, lc_all, cot_t, part, out_send, out_own, out_recv,
    head_send, embed_send, head_recv, embed_recv,
    send_sem, recv_sem, spread_send, spread_recv, far_send, far_recv, local_sem,
):
    s = lax.axis_index("section")
    r = lax.axis_index("dp")
    y, xh = s // 2, s % 2
    z, xl, c = r // 4, (r // 2) % 2, r % 2
    zin = z % 2
    even_z = lax.rem(z + 8 - 3 * zin, 8)
    pair = even_z // 2
    before, after = lax.rem(y + 3, 4), lax.rem(y + 1, 4)
    opposite = lax.rem(y + 2, 4)
    far = 1 - xh
    last = 7
    share = hid.shape[0]
    section_of = lambda yy, hh: yy * 2 + hh
    to_before = {"section": section_of(before, xh), "dp": r}
    to_after = {"section": section_of(after, xh), "dp": r}
    to_far = {"section": section_of(y, far), "dp": r}
    to_cross = {"section": section_of(y, far), "dp": z * 4 + (1 - xl) * 2 + c}

    def near(k):
        return (zin + k // 4) % 2, (xl + (k // 2) % 2) % 2, (c + k % 2) % 2

    def slot_of(k):
        other_z, other_x, other_c = near(k)
        return other_z * 4 + other_x * 2 + other_c

    def z_of(other_z):
        return lax.rem(even_z + 3 * other_z, 8)

    def peer_of(k):
        other_z, other_x, other_c = near(k)
        return {"section": s, "dp": z_of(other_z) * 4 + other_x * 2 + other_c}

    def owner_z(zz, cc, b):
        delta = cc if b == 0 else 2 - 3 * cc
        return lax.rem(zz + 8 + (2 * (zz % 2) - 1) * delta, 8)

    def column_block(k, b):
        other_z, other_x, other_c = near(k)
        return owner_z(z_of(other_z), other_c, b) * 2 + other_x

    def columns_of(k, b):
        return pl.ds(pl.multiple_of(column_block(k, b) * 128, 128), 128)

    slot = slot_of(0)
    to_sibling, to_x, to_z = peer_of(1), peer_of(2), peer_of(4)

    table_load = pltpu.make_async_copy(head, table.at[pl.ds(s * 256, 256)], local_sem.at[0])
    table_load.start()
    mixed_load = pltpu.make_async_copy(mixed, mix.at[:, slot], local_sem.at[1])
    mixed_load.start()
    block_load = pltpu.make_async_copy(block, block_own, local_sem.at[2])
    weight_load = [
        pltpu.make_async_copy(weight.at[pl.ds(k * 256, 256)], w_all.at[pl.ds(k * 256, 256)], local_sem.at[3 + k])
        for k in range(8)
    ]

    @pl.when(s == last)
    def _():
        for k in range(8):
            weight_load[k].start()
        block_load.start()

    barrier = pltpu.get_barrier_semaphore()
    pl.semaphore_signal(barrier, inc=1, device_id=to_cross, device_id_type=MESH)

    @pl.loop(1, 8)
    def _(step):
        pl.semaphore_signal(
            barrier, inc=1, device_id={"section": lax.rem(s + step, 8), "dp": r}, device_id_type=MESH
        )

    @pl.loop(1, 32)
    def _(step):
        pl.semaphore_signal(
            barrier, inc=1, device_id={"section": s, "dp": lax.rem(r + step, 32)}, device_id_type=MESH
        )

    for m in range(4):
        own_ids[0:1, m * 64 : (m + 1) * 64] = small[16 + m : 17 + m, 0:64].astype(jnp.int32)
    id_all[slot] = own_ids[...]
    for m in range(16):
        gain[0:1, m * 128 : (m + 1) * 128] = small[m : m + 1, :]
    table_load.wait()
    mixed_load.wait()
    pl.semaphore_wait(barrier, 39)

    table_out, mix_out, swap_out, cot_out, hid_out, lc_out, lc_swap_out, id_out = range(8)

    def arrived(dst, recv):
        remote(dst, dst, send_sem.at[0], recv, to_sibling).wait_recv()

    def sent(src, group):
        remote(src, src, send_sem.at[group], recv_sem.at[0], to_sibling).wait_send()

    def rows(yy, hh, p, half=None, core=None):
        start = section_of(yy, hh) * 256 + (c if core is None else core) * 128 + p * 64
        if half is None:
            return table.at[pl.ds(start, 64)]
        return table.at[pl.ds(start + half * 32, 32)]

    def make(ref, number, device, group=table_out):
        return remote(ref, ref, send_sem.at[group], recv_sem.at[number], device)

    def pass_on(ref, number, device, group=table_out):
        make(ref, number, device, group).start()

    pass_on(rows(y, xh, 1), 6, to_before)
    pass_on(rows(y, xh, 1), 5, to_after)
    pass_on(rows(y, xh, 0), 0, to_cross)
    pass_on(rows(y, xh, 0), 8, to_before)
    pass_on(rows(y, xh, 0), 7, to_after)
    for k in range(1, 8):
        remote(own_ids, id_all.at[slot], send_sem.at[id_out], recv_sem.at[39], peer_of(k)).start()

    own_mix = mix.at[:, slot]
    pass_on(own_mix, 35, to_sibling, mix_out)

    def pieces(direction, first, end, at):
        if direction == "z":
            return [make(mix.at[p, at], 40 + p // 2, to_z, mix_out) for p in range(first, end)]
        return [make(mix.at[p, at], 31 if at is slot else 33, to_x, mix_out) for p in range(first, end)]

    def feed(direction, first, end):
        for copy in pieces(direction, first, end, slot):
            copy.start()

    mix_x, mix_z, mix_xz = slot_of(2), slot_of(4), slot_of(6)

    def feed_corner(group):
        arrived(mix.at[pl.ds(2 * group, 2), mix_z], recv_sem.at[40 + group])
        for copy in pieces("x", 2 * group, 2 * group + 2, mix_z):
            copy.start()

    feed("z", 0, 3)
    bulk = [make(rows(y, xh, 1), 1, to_cross)] + pieces("x", 0, 3, slot)

    @pl.when(s != last)
    def _():
        for copy in bulk:
            copy.start()

    def piece(k):
        at = pl.ds(k * share, share)
        direct = k % 2 == 1 or k in (2, last - 1)
        target_device = {"section": k if direct else k + 1, "dp": r}
        return (
            remote(
                normed_all.at[at],
                hid if direct else hid_pass,
                spread_send.at[k],
                spread_recv.at[0 if direct else 2],
                target_device,
            ),
            remote(
                inv_all.at[at],
                inv_in if direct else inv_pass,
                spread_send.at[8 + k],
                spread_recv.at[1 if direct else 3],
                target_device,
            ),
        )

    def passed():
        return (
            remote(hid_pass, hid, spread_send.at[0], spread_recv.at[0], to_far),
            remote(inv_pass, inv_in, spread_send.at[8], spread_recv.at[1], to_far),
        )

    passes = jnp.logical_or(s == 1, s == 5)

    @pl.when(s == last)
    def _():
        for k in range(8):
            weight_load[k].wait()
        block_load.wait()

        @pl.loop(0, 8)
        def _(k):
            at = pl.ds(pl.multiple_of(k * 256, 256), 256)
            final[:, at] = block_own[:, at].astype(jnp.float32) + times_transposed(
                mix[:, slot].reshape(256, 2048), w_all[at, :]
            )

        for k in (0, 4, 2, 6, 3, 1, 5, 7):
            at = pl.ds(k * share, share)
            value = final[at, :]
            inverse = lax.rsqrt(jnp.mean(value * value, axis=-1, keepdims=True) + norm_eps)
            normed = (value * inverse * gain[...]).astype(jnp.bfloat16)
            wide_inverse = jnp.broadcast_to(inverse, (share, 128))
            if k < last:
                normed_all[at, :] = normed
                inv_all[at, :] = wide_inverse
                for copy in piece(k):
                    copy.start()
            else:
                hid[...] = normed
                inv_in[...] = wide_inverse
        for copy in bulk:
            copy.start()

    def swap_columns(array, spread, base):
        for k in range(1, 8):
            for b in range(2):
                remote(
                    array.at[:, columns_of(k, b)],
                    spread.at[b, s, slot],
                    send_sem.at[swap_out],
                    recv_sem.at[base],
                    peer_of(k),
                ).start()
        for b in range(2):
            spread[b, s, slot] = array[:, columns_of(0, b)]

    def wait_columns(spread, base):
        arrived(spread.at[:, 0, pl.ds(0, 7)], recv_sem.at[base])

    cot_base, hid_base, lc_base = 46, 55, 64

    def gather_start(spread, base):
        own = spread.at[:, s]
        pass_on(own, base, to_far, cot_out if base == cot_base else hid_out)
        pass_on(own, base + 2, to_before, cot_out if base == cot_base else hid_out)
        pass_on(own, base + 1, to_after, cot_out if base == cot_base else hid_out)

    def gather_near(spread, base):
        arrived(spread.at[:, section_of(before, xh)], recv_sem.at[base + 1])
        pass_on(spread.at[0, section_of(before, xh)], base + 5, to_after, cot_out if base == cot_base else hid_out)
        arrived(spread.at[:, section_of(after, xh)], recv_sem.at[base + 2])
        pass_on(spread.at[1, section_of(after, xh)], base + 6, to_before, cot_out if base == cot_base else hid_out)

    def gather_far(spread, base):
        other = spread.at[:, section_of(y, far)]
        arrived(other, recv_sem.at[base])
        pass_on(other, base + 4, to_before, cot_out if base == cot_base else hid_out)
        pass_on(other, base + 3, to_after, cot_out if base == cot_base else hid_out)

    def gather_far_near(spread, base):
        arrived(spread.at[:, section_of(before, far)], recv_sem.at[base + 3])
        pass_on(spread.at[0, section_of(before, far)], base + 7, to_after, cot_out if base == cot_base else hid_out)
        arrived(spread.at[:, section_of(after, far)], recv_sem.at[base + 4])
        pass_on(spread.at[1, section_of(after, far)], base + 8, to_before, cot_out if base == cot_base else hid_out)

    def gather_end(spread, base):
        arrived(spread.at[0, section_of(opposite, xh)], recv_sem.at[base + 5])
        arrived(spread.at[1, section_of(opposite, xh)], recv_sem.at[base + 6])
        arrived(spread.at[0, section_of(opposite, far)], recv_sem.at[base + 7])
        arrived(spread.at[1, section_of(opposite, far)], recv_sem.at[base + 8])

    shared = []

    def share_chunk(yy, hh, p):
        shared.append((yy, hh, p))
        pass_on(rows(yy, hh, p), 17 if len(shared) <= 7 else 45, to_sibling)

    def chunk_arrived(yy, hh, p, number, half=None):
        arrived(rows(yy, hh, p, half), recv_sem.at[number])

    chunk_arrived(before, xh, 1, 5)
    pass_on(rows(before, xh, 1, 0), 11, to_after)
    pass_on(rows(before, xh, 1), 2, to_cross)
    share_chunk(before, xh, 1)
    chunk_arrived(after, xh, 1, 6)
    pass_on(rows(after, xh, 1, 1), 12, to_before)
    pass_on(rows(after, xh, 1), 3, to_cross)
    share_chunk(after, xh, 1)
    feed("x", 3, 5)
    chunk_arrived(y, far, 0, 0)
    pass_on(rows(y, far, 0), 9, to_after)
    pass_on(rows(y, far, 0), 10, to_before)
    share_chunk(y, far, 0)
    chunk_arrived(before, xh, 0, 7)
    pass_on(rows(before, xh, 0, 0), 13, to_after)
    share_chunk(before, xh, 0)
    chunk_arrived(after, xh, 0, 8)
    pass_on(rows(after, xh, 0, 1), 14, to_before)
    share_chunk(after, xh, 0)
    feed("z", 3, 4)
    feed("x", 5, 8)
    chunk_arrived(opposite, xh, 1, 11, 0)
    chunk_arrived(opposite, xh, 1, 12, 1)
    pass_on(rows(opposite, xh, 1), 4, to_cross)
    share_chunk(opposite, xh, 1)
    chunk_arrived(y, far, 1, 1)
    share_chunk(y, far, 1)
    feed("z", 4, 5)
    feed_corner(0)
    @pl.when(passes)
    def _():
        for copy in piece(0):
            copy.wait_recv()
        for copy in passed():
            copy.start()

    chunk_arrived(before, far, 0, 9)
    pass_on(rows(before, far, 0, 0), 15, to_after)
    share_chunk(before, far, 0)
    chunk_arrived(after, far, 0, 10)
    pass_on(rows(after, far, 0, 1), 16, to_before)
    share_chunk(after, far, 0)

    feed("z", 5, 6)
    chunk_arrived(before, far, 1, 2)
    share_chunk(before, far, 1)
    chunk_arrived(after, far, 1, 3)
    share_chunk(after, far, 1)
    chunk_arrived(opposite, xh, 0, 13, 0)
    chunk_arrived(opposite, xh, 0, 14, 1)
    share_chunk(opposite, xh, 0)
    chunk_arrived(opposite, far, 0, 15, 0)
    chunk_arrived(opposite, far, 0, 16, 1)
    share_chunk(opposite, far, 0)
    @pl.when(s != last)
    def _():
        for copy in passed():
            copy.wait_recv()

    swap_columns(hid, hid_all, 36)
    feed("z", 6, 7)
    feed_corner(1)
    chunk_arrived(opposite, far, 1, 4)
    share_chunk(opposite, far, 1)
    def score(sections):
        for section in sections:
            at = pl.ds(pl.multiple_of(section * 256, 256), 256)
            logits[:, at] = times_transposed(hid[...], table[at, :])

    arrived(table.at[pl.ds(0, 7 * 64)], recv_sem.at[17])
    score([s, section_of(before, xh), section_of(after, xh), section_of(y, far)])
    arrived(table.at[pl.ds(0, 7 * 64)], recv_sem.at[45])

    score([section_of(opposite, xh), section_of(before, far), section_of(after, far), section_of(opposite, far)])

    value = logits[...]
    weights = jnp.exp(value - jnp.max(value, axis=-1, keepdims=True))
    predicted = weights / jnp.sum(weights, axis=-1, keepdims=True)
    columns = lax.broadcasted_iota(jnp.int32, value.shape, 1)
    target_row = small[pl.ds(16 + s // 2, 1), 64:128]
    here = lax.broadcasted_iota(jnp.int32, (share, 64), 1) == share * (s % 2) + lax.broadcasted_iota(
        jnp.int32, (share, 64), 0
    )
    own_target = jnp.sum(jnp.where(here, target_row, 0.0), axis=1, keepdims=True)
    hit = columns == own_target.astype(jnp.int32)
    logit_cot[...] = jnp.where(hit, predicted - 1.0, predicted).astype(jnp.bfloat16)

    for step in range(1, 8):
        other = lax.rem(s + step, 8)
        at = pl.ds(pl.multiple_of(other * 256, 256), 256)
        remote(
            logit_cot.at[:, at],
            lc_all.at[s, slot],
            send_sem.at[lc_swap_out],
            recv_sem.at[38],
            {"section": other, "dp": r},
        ).start()
    lc_all[s, slot] = logit_cot[:, pl.ds(pl.multiple_of(s * 256, 256), 256)]

    @pl.loop(0, 8)
    def _(k):
        at = pl.ds(pl.multiple_of(k * 256, 256), 256)
        logits[:, at] = plain_times(logit_cot[...], table[:, at]) * gain[:, at]

    scaled = logits[...]
    unit = hid[...].astype(jnp.float32) / gain[...]
    cot[...] = (
        inv_in[:, :1] * (scaled - unit * jnp.mean(scaled * unit, axis=-1, keepdims=True))
    ).astype(jnp.bfloat16)
    swap_columns(cot, cot_all, 37)

    feed("z", 7, 8)
    wait_columns(hid_all, 36)
    gather_start(hid_all, hid_base)
    wait_columns(cot_all, 37)
    gather_start(cot_all, cot_base)
    feed_corner(2)
    gather_near(hid_all, hid_base)
    arrived(lc_all.at[0, pl.ds(0, 7)], recv_sem.at[38])
    for k in (2, 4, 6, 1):
        pass_on(lc_all.at[:, slot], lc_base + k, peer_of(k), lc_out)
    gather_near(cot_all, cot_base)
    gather_far(cot_all, cot_base)
    gather_far(hid_all, hid_base)
    arrived(mix.at[:, mix_x], recv_sem.at[31])
    pass_on(mix.at[:, mix_x], 32, to_sibling, mix_out)
    feed_corner(3)
    pass_on(mix.at[:, mix_z], 34, to_sibling, mix_out)
    gather_far_near(cot_all, cot_base)
    gather_far_near(hid_all, hid_base)
    for k in (2, 4, 6):
        other = lc_all.at[:, slot_of(k)]
        arrived(other, recv_sem.at[lc_base + k])
        pass_on(other, lc_base + k + 1, to_sibling, lc_out)
    def row_copy(send, recv, send_at, recv_at, target_dp):
        return remote(
            send.at[target_dp], recv.at[pair, slot], send_at, recv_at, {"section": s, "dp": target_dp}
        )

    head_rows = (head_send, head_recv, send_sem.at[8], recv_sem.at[18])
    embed_rows = (embed_send, embed_recv, send_sem.at[9], recv_sem.at[19])

    def rows_start(refs):
        @pl.loop(1, 32)
        def _(step):
            row_copy(*refs, lax.rem(r + step, 32)).start()

        refs[1][pair, slot] = refs[0][r]

    def rows_wait(refs):
        arrived(refs[0].at[pl.ds(0, 31)], refs[3])

    def rows_end(refs):
        everything = refs[0].at[pl.ds(0, 31)]
        remote(everything, everything, refs[2], refs[3], to_sibling).wait_send()

    def rows_sum(recv, grad):
        sources = {}
        for w in range(4):
            for j in range(8):
                sender_z = (2 * w + 3 * (j // 4)) % 8
                for b in range(2):
                    delta = j % 2 if b == 0 else 2 - 3 * (j % 2)
                    owner_of = (sender_z + 8 + (2 * (sender_z % 2) - 1) * delta) % 8
                    sources.setdefault(owner_of * 2 + (j // 2) % 2, []).append((w, j, b))
        for column, senders in sources.items():
            total = 0.0
            for w, j, b in senders:
                total = total + recv[w, j, 8 * b : 8 * b + 8, :]
            grad[:, column * 128 : column * 128 + 128] = total

    gather_end(cot_all, cot_base)

    arrived(id_all.at[pl.ds(0, 7)], recv_sem.at[39])
    vocabulary = s * 256 + lax.broadcasted_iota(jnp.int32, (256, 256), 0)
    totals = [jnp.zeros((256, 128), jnp.float32)] * 2
    for k in range(8):
        marks = jnp.where(vocabulary == id_all[k], 1.0, 0.0).astype(jnp.bfloat16)
        for b in range(2):
            totals[b] = totals[b] + plain_times(marks, cot_all[b, :, k].reshape(256, 128))
    embed_send[...] = jnp.concatenate([total.reshape(32, 8, 128) for total in totals], axis=1)
    rows_start(embed_rows)
    gather_end(hid_all, hid_base)
    for k in (1, 3, 5, 7):
        arrived(lc_all.at[:, slot_of(k)], recv_sem.at[lc_base + k])
    products = [
        transposed_times(lc_all[...].reshape(2048, 256), hid_all[b].reshape(2048, 128)).reshape(32, 8, 128)
        for b in range(2)
    ]
    head_send[...] = jnp.concatenate(products, axis=1)
    rows_start(head_rows)
    arrived(mix.at[:, mix_xz], recv_sem.at[33])
    pass_on(mix.at[:, mix_xz], 44, to_sibling, mix_out)
    for number, k in ((35, 1), (32, 3), (34, 5), (44, 7)):
        arrived(mix.at[:, slot_of(k)], recv_sem.at[number])

    for b in range(2):
        cot_t[pl.ds(b * 128, 128), :] = cot_all[b].reshape(2048, 128).T

    sign = 2 * zin - 1

    def owner(delta, core):
        return {"section": s, "dp": lax.rem(z + 8 + sign * delta, 8) * 4 + xl * 2 + core}

    deltas = (0, 1, -1, 2)

    def far_rows(half, number, b, core, place):
        at = pl.ds(half * 1024, 1024)
        return remote(
            out_send.at[2 * b + core, :, at],
            out_recv.at[place - 1, :, at],
            far_send.at[half * 4 + number],
            far_recv.at[half * 4 + place],
            owner(deltas[place], core),
        )

    def sibling_rows(half):
        at = pl.ds(half * 1024, 1024)
        return remote(
            part.at[pl.ds(64, 64), at], out_own.at[:, at], far_send.at[half * 4], far_recv.at[half * 4], owner(0, 1)
        )

    def even_core(half):
        return [far_rows(half, 1, 1, 0, 3), far_rows(half, 2, 1, 1, 3), sibling_rows(half)]

    def odd_core(half):
        return [far_rows(half, 2 * b + core, b, core, 1 + b) for b in (1, 0) for core in range(2)]

    for half in range(2):

        @pl.loop(half * 4, half * 4 + 4)
        def _(k):
            at = pl.ds(pl.multiple_of(k * 256, 256), 256)
            product = plain_times(cot_t[...], mix[:, :, :, at].reshape(2048, 256))
            part[:, at] = product[:128]
            out_send[:, :, at] = product.reshape(4, 64, 256).astype(jnp.bfloat16)

        @pl.when(c == 0)
        def _():
            for copy in even_core(half):
                copy.start()

        @pl.when(c == 1)
        def _():
            for copy in odd_core(half):
                copy.start()

    for half in range(2):
        at = pl.ds(half * 1024, 1024)

        @pl.when(c == 1)
        def _():
            arrived(out_own.at[:, at], far_recv.at[half * 4])

        @pl.when(c == 0)
        def _():
            out_own[:, at] = part[:64, at]

        for place in (1, 2, 3):
            arrived(out_recv.at[place - 1, :, at], far_recv.at[half * 4 + place])
        total = out_own[:, at]
        for place in (1, 2, 3):
            total = total + out_recv[place - 1, :, at].astype(jnp.float32)
        out_grad[:, at] = total

    rows_wait(embed_rows)
    rows_sum(embed_recv, embed_grad)

    rows_wait(head_rows)
    rows_sum(head_recv, head_grad)
    rows_end(head_rows)
    rows_end(embed_rows)

    @pl.when(s == last)
    def _():
        for k in range(last):
            for copy in piece(k):
                copy.wait_send()

    @pl.when(passes)
    def _():
        for copy in passed():
            copy.wait_send()

    for half in range(2):

        @pl.when(c == 0)
        def _():
            for copy in even_core(half):
                copy.wait_send()

        @pl.when(c == 1)
        def _():
            for copy in odd_core(half):
                copy.wait_send()

    sent(table.at[pl.ds(0, 1792)], table_out)
    sent(mix.at[pl.ds(0, 7)], mix_out)
    sent(cot_all.at[0, pl.ds(0, 7), pl.ds(0, 4)], swap_out)
    sent(cot_all.at[:, pl.ds(0, 7)], cot_out)
    sent(hid_all.at[:, pl.ds(0, 7)], hid_out)
    sent(lc_all.at[pl.ds(0, 7)], lc_out)
    sent(lc_all.at[0, pl.ds(0, 7)], lc_swap_out)
    sent(id_all.at[pl.ds(0, 7)], id_out)


def gradients(mixed, block, weight, head, small):
    sections, share, width = mixed.shape
    tokens = sections * share
    vmem = pl.BlockSpec(memory_space=pltpu.VMEM)
    anywhere = pl.BlockSpec(memory_space=pl.ANY)
    bf16, f32 = jnp.bfloat16, jnp.float32
    dma = pltpu.SemaphoreType.DMA
    return pl.pallas_call(
        step_kernel,
        out_shape=[
            jax.ShapeDtypeStruct((64, width), f32),
            jax.ShapeDtypeStruct((8, width), f32),
            jax.ShapeDtypeStruct((8, width), f32),
        ],
        in_specs=[anywhere, anywhere, anywhere, anywhere, vmem],
        out_specs=[vmem, vmem, vmem],
        scratch_shapes=[
            pltpu.VMEM((2048, width), bf16),
            pltpu.VMEM((width, width), bf16),
            pltpu.VMEM((tokens, width), bf16),
            pltpu.VMEM((tokens, width), f32),
            pltpu.VMEM((tokens, width), bf16),
            pltpu.VMEM((tokens, 128), f32),
            pltpu.VMEM((share, 128), f32),
            pltpu.VMEM((share, width), bf16),
            pltpu.VMEM((share, 128), f32),
            pltpu.VMEM((share, 2048), f32),
            pltpu.VMEM((share, width), bf16),
            pltpu.VMEM((share, 2048), bf16),
            pltpu.VMEM((share, width), bf16),
            pltpu.VMEM((1, width), f32),
            pltpu.VMEM((1, tokens), jnp.int32),
            pltpu.VMEM((8, 1, tokens), jnp.int32),
            pltpu.VMEM((8, 8, share, width), bf16),
            pltpu.VMEM((2, 8, 8, share, 128), bf16),
            pltpu.VMEM((2, 8, 8, share, 128), bf16),
            pltpu.VMEM((8, 8, share, 256), bf16),
            pltpu.VMEM((256, 2048), bf16),
            pltpu.VMEM((128, width), f32),
            pltpu.VMEM((4, 64, width), bf16),
            pltpu.VMEM((64, width), f32),
            pltpu.VMEM((3, 64, width), bf16),
            pltpu.VMEM((32, 16, 128), f32),
            pltpu.VMEM((32, 16, 128), f32),
            pltpu.VMEM((4, 8, 16, 128), f32),
            pltpu.VMEM((4, 8, 16, 128), f32),
            dma((10,)),
            dma((72,)),
            dma((16,)),
            dma((4,)),
            dma((8,)),
            dma((8,)),
            dma((11,)),
        ],
        compiler_params=pltpu.CompilerParams(collective_id=0, has_side_effects=True, vmem_limit_bytes=53 * 2**20),
        name="gradients",
    )(mixed, block, weight, head, small)


def local(
    block_inputs,
    mixed_inputs,
    token_ids,
    target_ids,
    final_gain,
    out_weight,
    head_weight,
    out_master,
    out_first,
    out_second,
    head_master,
    head_first,
    head_second,
    embed_master,
    embed_first,
    embed_second,
):
    sections = lax.axis_size("section")
    batches, rows, width = mixed_inputs[0].shape
    tokens = batches * rows
    id_rows = jnp.concatenate([token_ids, target_ids], axis=1).astype(jnp.float32)
    small = jnp.concatenate([final_gain.reshape(width // 128, 128), id_rows])
    out_gradient, head_gradient, embed_gradient = gradients(
        mixed_inputs[0].reshape(sections, tokens // sections, width),
        block_inputs[0].reshape(tokens, width),
        out_weight[0],
        head_weight,
        small,
    )
    out_out = adam_update(out_master, out_first, out_second, out_gradient.reshape(out_master.shape))
    head_out = adam_update(head_master, head_first, head_second, head_gradient)
    embed_out = adam_update(embed_master, embed_first, embed_second, embed_gradient)
    return out_out + head_out + embed_out


def solution(mesh):
    step = jax.shard_map(
        local,
        mesh=mesh,
        in_specs=(
            P("section", None, "dp", None),
            P("section", None, "dp", None),
            P(None, "dp"),
            P(None, "dp"),
            P(),
            P("section", None, None),
            P("section", None),
            P("section", "dp", None),
            P("section", "dp", None),
            P("section", "dp", None),
            P(("section", "dp"), None),
            P(("section", "dp"), None),
            P(("section", "dp"), None),
            P(("section", "dp"), None),
            P(("section", "dp"), None),
            P(("section", "dp"), None),
        ),
        out_specs=(
            P("section", "dp", None),
            P("section", "dp", None),
            P("section", "dp", None),
            P(("section", "dp"), None),
            P(("section", "dp"), None),
            P(("section", "dp"), None),
            P(("section", "dp"), None),
            P(("section", "dp"), None),
            P(("section", "dp"), None),
        ),
        check_vma=False,
    )
    return step
```

```python
import jax
import jax.numpy as jnp
from jax import lax
from jax.experimental import pallas as pl
from jax.experimental.pallas import tpu as pltpu
from jax.sharding import PartitionSpec as P

norm_eps = 1e-05
beta_first = 0.9
beta_second = 0.95
adam_eps = 1e-05
learning_rate = 0.0003
decay_rate = 0.1

MESH = pl.DeviceIdType.MESH


def times_transposed(former, latter):
    return lax.dot_general(
        former, latter, (((1,), (1,)), ((), ())), preferred_element_type=jnp.float32
    )


def transposed_times(former, latter):
    return lax.dot_general(
        former, latter, (((0,), (0,)), ((), ())), preferred_element_type=jnp.float32
    )


def plain_times(former, latter):
    return jnp.dot(former, latter, preferred_element_type=jnp.float32)


def adam_update(master, first, second, gradient):
    first_next = beta_first * first + (1.0 - beta_first) * gradient
    second_next = beta_second * second + (1.0 - beta_second) * gradient * gradient
    master_next = master - learning_rate * (
        first_next / (jnp.sqrt(second_next) + adam_eps) + decay_rate * master
    )
    return (master_next, first_next, second_next)


def remote(src, dst, send, recv, device):
    return pltpu.make_async_remote_copy(
        src_ref=src, dst_ref=dst, send_sem=send, recv_sem=recv, device_id=device, device_id_type=MESH
    )


def step_kernel(
    mixed, block, weight, head, small,
    out_grad, head_grad, embed_grad,
    table, w_all, block_own, final, normed_all, inv_all, inv_in, hid_pass, inv_pass, logits, hid, logit_cot, cot,
    gain, own_ids, id_all, mix, cot_all, hid_all, lc_all, cot_t, part, out_send, out_own, out_recv,
    head_send, embed_send, head_recv, embed_recv,
    send_sem, recv_sem, spread_send, spread_recv, far_send, far_recv, local_sem,
):
    s = lax.axis_index("section")
    r = lax.axis_index("dp")
    y, xh = s // 2, s % 2
    z, xl, c = r // 4, (r // 2) % 2, r % 2
    zin = z % 2
    even_z = lax.rem(z + 8 - 3 * zin, 8)
    pair = even_z // 2
    before, after = lax.rem(y + 3, 4), lax.rem(y + 1, 4)
    opposite = lax.rem(y + 2, 4)
    far = 1 - xh
    last = 7
    share = hid.shape[0]
    section_of = lambda yy, hh: yy * 2 + hh
    to_before = {"section": section_of(before, xh), "dp": r}
    to_after = {"section": section_of(after, xh), "dp": r}
    to_far = {"section": section_of(y, far), "dp": r}
    to_cross = {"section": section_of(y, far), "dp": z * 4 + (1 - xl) * 2 + c}

    def near(k):
        return (zin + k // 4) % 2, (xl + (k // 2) % 2) % 2, (c + k % 2) % 2

    def slot_of(k):
        other_z, other_x, other_c = near(k)
        return other_z * 4 + other_x * 2 + other_c

    def z_of(other_z):
        return lax.rem(even_z + 3 * other_z, 8)

    def peer_of(k):
        other_z, other_x, other_c = near(k)
        return {"section": s, "dp": z_of(other_z) * 4 + other_x * 2 + other_c}

    def owner_z(zz, cc, b):
        delta = cc if b == 0 else 2 - 3 * cc
        return lax.rem(zz + 8 + (2 * (zz % 2) - 1) * delta, 8)

    def column_block(k, b):
        other_z, other_x, other_c = near(k)
        return owner_z(z_of(other_z), other_c, b) * 2 + other_x

    def columns_of(k, b):
        return pl.ds(pl.multiple_of(column_block(k, b) * 128, 128), 128)

    slot = slot_of(0)
    to_sibling, to_x, to_z = peer_of(1), peer_of(2), peer_of(4)

    table_load = pltpu.make_async_copy(head, table.at[pl.ds(s * 256, 256)], local_sem.at[0])
    table_load.start()
    mixed_load = pltpu.make_async_copy(mixed, mix.at[:, slot], local_sem.at[1])
    mixed_load.start()
    block_load = pltpu.make_async_copy(block, block_own, local_sem.at[2])
    weight_load = [
        pltpu.make_async_copy(weight.at[pl.ds(k * 256, 256)], w_all.at[pl.ds(k * 256, 256)], local_sem.at[3 + k])
        for k in range(8)
    ]

    @pl.when(s == last)
    def _():
        for k in range(8):
            weight_load[k].start()
        block_load.start()

    barrier = pltpu.get_barrier_semaphore()
    pl.semaphore_signal(barrier, inc=1, device_id=to_cross, device_id_type=MESH)

    @pl.loop(1, 8)
    def _(step):
        pl.semaphore_signal(
            barrier, inc=1, device_id={"section": lax.rem(s + step, 8), "dp": r}, device_id_type=MESH
        )

    @pl.loop(1, 32)
    def _(step):
        pl.semaphore_signal(
            barrier, inc=1, device_id={"section": s, "dp": lax.rem(r + step, 32)}, device_id_type=MESH
        )

    for m in range(4):
        own_ids[0:1, m * 64 : (m + 1) * 64] = small[16 + m : 17 + m, 0:64].astype(jnp.int32)
    id_all[slot] = own_ids[...]
    for m in range(16):
        gain[0:1, m * 128 : (m + 1) * 128] = small[m : m + 1, :]
    table_load.wait()
    mixed_load.wait()
    pl.semaphore_wait(barrier, 39)

    table_out, mix_out, swap_out, cot_out, hid_out, lc_out, lc_swap_out, id_out = range(8)

    def arrived(dst, recv):
        remote(dst, dst, send_sem.at[0], recv, to_sibling).wait_recv()

    def sent(src, group):
        remote(src, src, send_sem.at[group], recv_sem.at[0], to_sibling).wait_send()

    def rows(yy, hh, p, half=None, core=None):
        start = section_of(yy, hh) * 256 + (c if core is None else core) * 128 + p * 64
        if half is None:
            return table.at[pl.ds(start, 64)]
        return table.at[pl.ds(start + half * 32, 32)]

    def make(ref, number, device, group=table_out):
        return remote(ref, ref, send_sem.at[group], recv_sem.at[number], device)

    def pass_on(ref, number, device, group=table_out):
        make(ref, number, device, group).start()

    pass_on(rows(y, xh, 1), 6, to_before)
    pass_on(rows(y, xh, 1), 5, to_after)
    pass_on(rows(y, xh, 0), 0, to_cross)
    pass_on(rows(y, xh, 0), 8, to_before)
    pass_on(rows(y, xh, 0), 7, to_after)
    for k in range(1, 8):
        remote(own_ids, id_all.at[slot], send_sem.at[id_out], recv_sem.at[39], peer_of(k)).start()

    own_mix = mix.at[:, slot]
    pass_on(own_mix, 35, to_sibling, mix_out)

    def pieces(direction, first, end, at):
        if direction == "z":
            return [make(mix.at[p, at], 40 + p // 2, to_z, mix_out) for p in range(first, end)]
        return [make(mix.at[p, at], 31 if at is slot else 33, to_x, mix_out) for p in range(first, end)]

    def feed(direction, first, end):
        for copy in pieces(direction, first, end, slot):
            copy.start()

    mix_x, mix_z, mix_xz = slot_of(2), slot_of(4), slot_of(6)

    def feed_corner(group):
        arrived(mix.at[pl.ds(2 * group, 2), mix_z], recv_sem.at[40 + group])
        for copy in pieces("x", 2 * group, 2 * group + 2, mix_z):
            copy.start()

    feed("z", 0, 3)
    bulk = [make(rows(y, xh, 1), 1, to_cross)] + pieces("x", 0, 3, slot)

    @pl.when(s != last)
    def _():
        for copy in bulk:
            copy.start()

    def piece(k):
        at = pl.ds(k * share, share)
        direct = k % 2 == 1 or k in (2, last - 1)
        target_device = {"section": k if direct else k + 1, "dp": r}
        return (
            remote(
                normed_all.at[at],
                hid if direct else hid_pass,
                spread_send.at[k],
                spread_recv.at[0 if direct else 2],
                target_device,
            ),
            remote(
                inv_all.at[at],
                inv_in if direct else inv_pass,
                spread_send.at[8 + k],
                spread_recv.at[1 if direct else 3],
                target_device,
            ),
        )

    def passed():
        return (
            remote(hid_pass, hid, spread_send.at[0], spread_recv.at[0], to_far),
            remote(inv_pass, inv_in, spread_send.at[8], spread_recv.at[1], to_far),
        )

    passes = jnp.logical_or(s == 1, s == 5)

    @pl.when(s == last)
    def _():
        for k in range(8):
            weight_load[k].wait()
        block_load.wait()

        @pl.loop(0, 8)
        def _(k):
            at = pl.ds(pl.multiple_of(k * 256, 256), 256)
            final[:, at] = block_own[:, at].astype(jnp.float32) + times_transposed(
                mix[:, slot].reshape(256, 2048), w_all[at, :]
            )

        for k in (0, 4, 2, 6, 3, 1, 5, 7):
            at = pl.ds(k * share, share)
            value = final[at, :]
            inverse = lax.rsqrt(jnp.mean(value * value, axis=-1, keepdims=True) + norm_eps)
            normed = (value * inverse * gain[...]).astype(jnp.bfloat16)
            wide_inverse = jnp.broadcast_to(inverse, (share, 128))
            if k < last:
                normed_all[at, :] = normed
                inv_all[at, :] = wide_inverse
                for copy in piece(k):
                    copy.start()
            else:
                hid[...] = normed
                inv_in[...] = wide_inverse
        for copy in bulk:
            copy.start()

    def swap_columns(array, spread, base):
        for k in range(1, 8):
            for b in range(2):
                remote(
                    array.at[:, columns_of(k, b)],
                    spread.at[b, s, slot],
                    send_sem.at[swap_out],
                    recv_sem.at[base],
                    peer_of(k),
                ).start()
        for b in range(2):
            spread[b, s, slot] = array[:, columns_of(0, b)]

    def wait_columns(spread, base):
        arrived(spread.at[:, 0, pl.ds(0, 7)], recv_sem.at[base])

    cot_base, hid_base, lc_base = 46, 55, 64

    def gather_start(spread, base):
        own = spread.at[:, s]
        pass_on(own, base, to_far, cot_out if base == cot_base else hid_out)
        pass_on(own, base + 2, to_before, cot_out if base == cot_base else hid_out)
        pass_on(own, base + 1, to_after, cot_out if base == cot_base else hid_out)

    def gather_near(spread, base):
        arrived(spread.at[:, section_of(before, xh)], recv_sem.at[base + 1])
        pass_on(spread.at[0, section_of(before, xh)], base + 5, to_after, cot_out if base == cot_base else hid_out)
        arrived(spread.at[:, section_of(after, xh)], recv_sem.at[base + 2])
        pass_on(spread.at[1, section_of(after, xh)], base + 6, to_before, cot_out if base == cot_base else hid_out)

    def gather_far(spread, base):
        other = spread.at[:, section_of(y, far)]
        arrived(other, recv_sem.at[base])
        pass_on(other, base + 4, to_before, cot_out if base == cot_base else hid_out)
        pass_on(other, base + 3, to_after, cot_out if base == cot_base else hid_out)

    def gather_far_near(spread, base):
        arrived(spread.at[:, section_of(before, far)], recv_sem.at[base + 3])
        pass_on(spread.at[0, section_of(before, far)], base + 7, to_after, cot_out if base == cot_base else hid_out)
        arrived(spread.at[:, section_of(after, far)], recv_sem.at[base + 4])
        pass_on(spread.at[1, section_of(after, far)], base + 8, to_before, cot_out if base == cot_base else hid_out)

    def gather_end(spread, base):
        arrived(spread.at[0, section_of(opposite, xh)], recv_sem.at[base + 5])
        arrived(spread.at[1, section_of(opposite, xh)], recv_sem.at[base + 6])
        arrived(spread.at[0, section_of(opposite, far)], recv_sem.at[base + 7])
        arrived(spread.at[1, section_of(opposite, far)], recv_sem.at[base + 8])

    shared = []

    def share_chunk(yy, hh, p):
        shared.append((yy, hh, p))
        pass_on(rows(yy, hh, p), 17 if len(shared) <= 7 else 45, to_sibling)

    def chunk_arrived(yy, hh, p, number, half=None):
        arrived(rows(yy, hh, p, half), recv_sem.at[number])

    chunk_arrived(before, xh, 1, 5)
    pass_on(rows(before, xh, 1, 0), 11, to_after)
    pass_on(rows(before, xh, 1), 2, to_cross)
    share_chunk(before, xh, 1)
    chunk_arrived(after, xh, 1, 6)
    pass_on(rows(after, xh, 1, 1), 12, to_before)
    pass_on(rows(after, xh, 1), 3, to_cross)
    share_chunk(after, xh, 1)
    feed("x", 3, 5)
    chunk_arrived(y, far, 0, 0)
    pass_on(rows(y, far, 0), 9, to_after)
    pass_on(rows(y, far, 0), 10, to_before)
    share_chunk(y, far, 0)
    chunk_arrived(before, xh, 0, 7)
    pass_on(rows(before, xh, 0, 0), 13, to_after)
    share_chunk(before, xh, 0)
    chunk_arrived(after, xh, 0, 8)
    pass_on(rows(after, xh, 0, 1), 14, to_before)
    share_chunk(after, xh, 0)
    feed("z", 3, 4)
    feed("x", 5, 8)
    chunk_arrived(opposite, xh, 1, 11, 0)
    chunk_arrived(opposite, xh, 1, 12, 1)
    pass_on(rows(opposite, xh, 1), 4, to_cross)
    share_chunk(opposite, xh, 1)
    chunk_arrived(y, far, 1, 1)
    share_chunk(y, far, 1)
    feed("z", 4, 5)
    feed_corner(0)
    @pl.when(passes)
    def _():
        for copy in piece(0):
            copy.wait_recv()
        for copy in passed():
            copy.start()

    chunk_arrived(before, far, 0, 9)
    pass_on(rows(before, far, 0, 0), 15, to_after)
    share_chunk(before, far, 0)
    chunk_arrived(after, far, 0, 10)
    pass_on(rows(after, far, 0, 1), 16, to_before)
    share_chunk(after, far, 0)

    feed("z", 5, 6)
    chunk_arrived(before, far, 1, 2)
    share_chunk(before, far, 1)
    chunk_arrived(after, far, 1, 3)
    share_chunk(after, far, 1)
    chunk_arrived(opposite, xh, 0, 13, 0)
    chunk_arrived(opposite, xh, 0, 14, 1)
    share_chunk(opposite, xh, 0)
    chunk_arrived(opposite, far, 0, 15, 0)
    chunk_arrived(opposite, far, 0, 16, 1)
    share_chunk(opposite, far, 0)
    @pl.when(s != last)
    def _():
        for copy in passed():
            copy.wait_recv()

    swap_columns(hid, hid_all, 36)
    feed("z", 6, 7)
    feed_corner(1)
    chunk_arrived(opposite, far, 1, 4)
    share_chunk(opposite, far, 1)
    def score(sections):
        for section in sections:
            at = pl.ds(pl.multiple_of(section * 256, 256), 256)
            logits[:, at] = times_transposed(hid[...], table[at, :])

    arrived(table.at[pl.ds(0, 7 * 64)], recv_sem.at[17])
    score([s, section_of(before, xh), section_of(after, xh), section_of(y, far)])
    arrived(table.at[pl.ds(0, 7 * 64)], recv_sem.at[45])

    score([section_of(opposite, xh), section_of(before, far), section_of(after, far), section_of(opposite, far)])

    value = logits[...]
    weights = jnp.exp(value - jnp.max(value, axis=-1, keepdims=True))
    predicted = weights / jnp.sum(weights, axis=-1, keepdims=True)
    columns = lax.broadcasted_iota(jnp.int32, value.shape, 1)
    target_row = jnp.zeros((1, 64), jnp.float32)
    for m in range(4):
        target_row = jnp.where(s // 2 == m, small[16 + m : 17 + m, 64:128], target_row)
    here = lax.broadcasted_iota(jnp.int32, (share, 64), 1) == share * (s % 2) + lax.broadcasted_iota(
        jnp.int32, (share, 64), 0
    )
    own_target = jnp.sum(jnp.where(here, target_row, 0.0), axis=1, keepdims=True)
    hit = columns == own_target.astype(jnp.int32)
    logit_cot[...] = jnp.where(hit, predicted - 1.0, predicted).astype(jnp.bfloat16)

    for step in range(1, 8):
        other = lax.rem(s + step, 8)
        at = pl.ds(pl.multiple_of(other * 256, 256), 256)
        remote(
            logit_cot.at[:, at],
            lc_all.at[s, slot],
            send_sem.at[lc_swap_out],
            recv_sem.at[38],
            {"section": other, "dp": r},
        ).start()
    lc_all[s, slot] = logit_cot[:, pl.ds(pl.multiple_of(s * 256, 256), 256)]

    @pl.loop(0, 8)
    def _(k):
        at = pl.ds(pl.multiple_of(k * 256, 256), 256)
        logits[:, at] = plain_times(logit_cot[...], table[:, at]) * gain[:, at]

    scaled = logits[...]
    unit = hid[...].astype(jnp.float32) / gain[...]
    cot[...] = (
        inv_in[:, :1] * (scaled - unit * jnp.mean(scaled * unit, axis=-1, keepdims=True))
    ).astype(jnp.bfloat16)
    swap_columns(cot, cot_all, 37)

    feed("z", 7, 8)
    wait_columns(hid_all, 36)
    gather_start(hid_all, hid_base)
    wait_columns(cot_all, 37)
    gather_start(cot_all, cot_base)
    feed_corner(2)
    gather_near(hid_all, hid_base)
    arrived(lc_all.at[0, pl.ds(0, 7)], recv_sem.at[38])
    for k in (2, 4, 6, 1):
        pass_on(lc_all.at[:, slot], lc_base + k, peer_of(k), lc_out)
    gather_near(cot_all, cot_base)
    gather_far(cot_all, cot_base)
    gather_far(hid_all, hid_base)
    arrived(mix.at[:, mix_x], recv_sem.at[31])
    pass_on(mix.at[:, mix_x], 32, to_sibling, mix_out)
    feed_corner(3)
    pass_on(mix.at[:, mix_z], 34, to_sibling, mix_out)
    gather_far_near(cot_all, cot_base)
    gather_far_near(hid_all, hid_base)
    for k in (2, 4, 6):
        other = lc_all.at[:, slot_of(k)]
        arrived(other, recv_sem.at[lc_base + k])
        pass_on(other, lc_base + k + 1, to_sibling, lc_out)
    def row_copy(send, recv, send_at, recv_at, target_dp):
        return remote(
            send.at[target_dp], recv.at[pair, slot], send_at, recv_at, {"section": s, "dp": target_dp}
        )

    head_rows = (head_send, head_recv, send_sem.at[8], recv_sem.at[18])
    embed_rows = (embed_send, embed_recv, send_sem.at[9], recv_sem.at[19])

    def rows_start(refs):
        @pl.loop(1, 32)
        def _(step):
            row_copy(*refs, lax.rem(r + step, 32)).start()

        refs[1][pair, slot] = refs[0][r]

    def rows_wait(refs):
        arrived(refs[0].at[pl.ds(0, 31)], refs[3])

    def rows_end(refs):
        everything = refs[0].at[pl.ds(0, 31)]
        remote(everything, everything, refs[2], refs[3], to_sibling).wait_send()

    def rows_sum(recv, grad):
        sources = {}
        for w in range(4):
            for j in range(8):
                sender_z = (2 * w + 3 * (j // 4)) % 8
                for b in range(2):
                    delta = j % 2 if b == 0 else 2 - 3 * (j % 2)
                    owner_of = (sender_z + 8 + (2 * (sender_z % 2) - 1) * delta) % 8
                    sources.setdefault(owner_of * 2 + (j // 2) % 2, []).append((w, j, b))
        for column, senders in sources.items():
            total = 0.0
            for w, j, b in senders:
                total = total + recv[w, j, 8 * b : 8 * b + 8, :]
            grad[:, column * 128 : column * 128 + 128] = total

    gather_end(cot_all, cot_base)

    arrived(id_all.at[pl.ds(0, 7)], recv_sem.at[39])
    vocabulary = s * 256 + lax.broadcasted_iota(jnp.int32, (256, 256), 0)
    totals = [jnp.zeros((256, 128), jnp.float32)] * 2
    for k in range(8):
        marks = jnp.where(vocabulary == id_all[k], 1.0, 0.0).astype(jnp.bfloat16)
        for b in range(2):
            totals[b] = totals[b] + plain_times(marks, cot_all[b, :, k].reshape(256, 128))
    embed_send[...] = jnp.concatenate([total.reshape(32, 8, 128) for total in totals], axis=1)
    rows_start(embed_rows)
    gather_end(hid_all, hid_base)
    for k in (1, 3, 5, 7):
        arrived(lc_all.at[:, slot_of(k)], recv_sem.at[lc_base + k])
    products = [
        transposed_times(lc_all[...].reshape(2048, 256), hid_all[b].reshape(2048, 128)).reshape(32, 8, 128)
        for b in range(2)
    ]
    head_send[...] = jnp.concatenate(products, axis=1)
    rows_start(head_rows)
    arrived(mix.at[:, mix_xz], recv_sem.at[33])
    pass_on(mix.at[:, mix_xz], 44, to_sibling, mix_out)
    for number, k in ((35, 1), (32, 3), (34, 5), (44, 7)):
        arrived(mix.at[:, slot_of(k)], recv_sem.at[number])

    for b in range(2):
        cot_t[pl.ds(b * 128, 128), :] = cot_all[b].reshape(2048, 128).T

    sign = 2 * zin - 1

    def owner(delta, core):
        return {"section": s, "dp": lax.rem(z + 8 + sign * delta, 8) * 4 + xl * 2 + core}

    deltas = (0, 1, -1, 2)

    def far_rows(half, number, b, core, place):
        at = pl.ds(half * 1024, 1024)
        return remote(
            out_send.at[2 * b + core, :, at],
            out_recv.at[place - 1, :, at],
            far_send.at[half * 4 + number],
            far_recv.at[half * 4 + place],
            owner(deltas[place], core),
        )

    def sibling_rows(half):
        at = pl.ds(half * 1024, 1024)
        return remote(
            part.at[pl.ds(64, 64), at], out_own.at[:, at], far_send.at[half * 4], far_recv.at[half * 4], owner(0, 1)
        )

    def even_core(half):
        return [far_rows(half, 1, 1, 0, 3), far_rows(half, 2, 1, 1, 3), sibling_rows(half)]

    def odd_core(half):
        return [far_rows(half, 2 * b + core, b, core, 1 + b) for b in (1, 0) for core in range(2)]

    for half in range(2):

        @pl.loop(half * 4, half * 4 + 4)
        def _(k):
            at = pl.ds(pl.multiple_of(k * 256, 256), 256)
            product = plain_times(cot_t[...], mix[:, :, :, at].reshape(2048, 256))
            part[:, at] = product[:128]
            out_send[:, :, at] = product.reshape(4, 64, 256).astype(jnp.bfloat16)

        @pl.when(c == 0)
        def _():
            for copy in even_core(half):
                copy.start()

        @pl.when(c == 1)
        def _():
            for copy in odd_core(half):
                copy.start()

    for half in range(2):
        at = pl.ds(half * 1024, 1024)

        @pl.when(c == 1)
        def _():
            arrived(out_own.at[:, at], far_recv.at[half * 4])

        @pl.when(c == 0)
        def _():
            out_own[:, at] = part[:64, at]

        for place in (1, 2, 3):
            arrived(out_recv.at[place - 1, :, at], far_recv.at[half * 4 + place])
        total = out_own[:, at]
        for place in (1, 2, 3):
            total = total + out_recv[place - 1, :, at].astype(jnp.float32)
        out_grad[:, at] = total

    rows_wait(embed_rows)
    rows_sum(embed_recv, embed_grad)

    rows_wait(head_rows)
    rows_sum(head_recv, head_grad)
    rows_end(head_rows)
    rows_end(embed_rows)

    @pl.when(s == last)
    def _():
        for k in range(last):
            for copy in piece(k):
                copy.wait_send()

    @pl.when(passes)
    def _():
        for copy in passed():
            copy.wait_send()

    for half in range(2):

        @pl.when(c == 0)
        def _():
            for copy in even_core(half):
                copy.wait_send()

        @pl.when(c == 1)
        def _():
            for copy in odd_core(half):
                copy.wait_send()

    sent(table.at[pl.ds(0, 1792)], table_out)
    sent(mix.at[pl.ds(0, 7)], mix_out)
    sent(cot_all.at[0, pl.ds(0, 7), pl.ds(0, 4)], swap_out)
    sent(cot_all.at[:, pl.ds(0, 7)], cot_out)
    sent(hid_all.at[:, pl.ds(0, 7)], hid_out)
    sent(lc_all.at[pl.ds(0, 7)], lc_out)
    sent(lc_all.at[0, pl.ds(0, 7)], lc_swap_out)
    sent(id_all.at[pl.ds(0, 7)], id_out)


def gradients(mixed, block, weight, head, small):
    sections, share, width = mixed.shape
    tokens = sections * share
    vmem = pl.BlockSpec(memory_space=pltpu.VMEM)
    anywhere = pl.BlockSpec(memory_space=pl.ANY)
    bf16, f32 = jnp.bfloat16, jnp.float32
    dma = pltpu.SemaphoreType.DMA
    return pl.pallas_call(
        step_kernel,
        out_shape=[
            jax.ShapeDtypeStruct((64, width), f32),
            jax.ShapeDtypeStruct((8, width), f32),
            jax.ShapeDtypeStruct((8, width), f32),
        ],
        in_specs=[anywhere, anywhere, anywhere, anywhere, vmem],
        out_specs=[vmem, vmem, vmem],
        scratch_shapes=[
            pltpu.VMEM((2048, width), bf16),
            pltpu.VMEM((width, width), bf16),
            pltpu.VMEM((tokens, width), bf16),
            pltpu.VMEM((tokens, width), f32),
            pltpu.VMEM((tokens, width), bf16),
            pltpu.VMEM((tokens, 128), f32),
            pltpu.VMEM((share, 128), f32),
            pltpu.VMEM((share, width), bf16),
            pltpu.VMEM((share, 128), f32),
            pltpu.VMEM((share, 2048), f32),
            pltpu.VMEM((share, width), bf16),
            pltpu.VMEM((share, 2048), bf16),
            pltpu.VMEM((share, width), bf16),
            pltpu.VMEM((1, width), f32),
            pltpu.VMEM((1, tokens), jnp.int32),
            pltpu.VMEM((8, 1, tokens), jnp.int32),
            pltpu.VMEM((8, 8, share, width), bf16),
            pltpu.VMEM((2, 8, 8, share, 128), bf16),
            pltpu.VMEM((2, 8, 8, share, 128), bf16),
            pltpu.VMEM((8, 8, share, 256), bf16),
            pltpu.VMEM((256, 2048), bf16),
            pltpu.VMEM((128, width), f32),
            pltpu.VMEM((4, 64, width), bf16),
            pltpu.VMEM((64, width), f32),
            pltpu.VMEM((3, 64, width), bf16),
            pltpu.VMEM((32, 16, 128), f32),
            pltpu.VMEM((32, 16, 128), f32),
            pltpu.VMEM((4, 8, 16, 128), f32),
            pltpu.VMEM((4, 8, 16, 128), f32),
            dma((10,)),
            dma((72,)),
            dma((16,)),
            dma((4,)),
            dma((8,)),
            dma((8,)),
            dma((11,)),
        ],
        compiler_params=pltpu.CompilerParams(collective_id=0, has_side_effects=True, vmem_limit_bytes=53 * 2**20),
        name="gradients",
    )(mixed, block, weight, head, small)


def local(
    block_inputs,
    mixed_inputs,
    token_ids,
    target_ids,
    final_gain,
    out_weight,
    head_weight,
    out_master,
    out_first,
    out_second,
    head_master,
    head_first,
    head_second,
    embed_master,
    embed_first,
    embed_second,
):
    sections = lax.axis_size("section")
    batches, rows, width = mixed_inputs[0].shape
    tokens = batches * rows
    id_rows = jnp.concatenate([token_ids, target_ids], axis=1).astype(jnp.float32)
    small = jnp.concatenate([final_gain.reshape(width // 128, 128), id_rows])
    out_gradient, head_gradient, embed_gradient = gradients(
        mixed_inputs[0].reshape(sections, tokens // sections, width),
        block_inputs[0].reshape(tokens, width),
        out_weight[0],
        head_weight,
        small,
    )
    out_out = adam_update(out_master, out_first, out_second, out_gradient.reshape(out_master.shape))
    head_out = adam_update(head_master, head_first, head_second, head_gradient)
    embed_out = adam_update(embed_master, embed_first, embed_second, embed_gradient)
    return out_out + head_out + embed_out


def solution(mesh):
    step = jax.shard_map(
        local,
        mesh=mesh,
        in_specs=(
            P("section", None, "dp", None),
            P("section", None, "dp", None),
            P(None, "dp"),
            P(None, "dp"),
            P(),
            P("section", None, None),
            P("section", None),
            P("section", "dp", None),
            P("section", "dp", None),
            P("section", "dp", None),
            P(("section", "dp"), None),
            P(("section", "dp"), None),
            P(("section", "dp"), None),
            P(("section", "dp"), None),
            P(("section", "dp"), None),
            P(("section", "dp"), None),
        ),
        out_specs=(
            P("section", "dp", None),
            P("section", "dp", None),
            P("section", "dp", None),
            P(("section", "dp"), None),
            P(("section", "dp"), None),
            P(("section", "dp"), None),
            P(("section", "dp"), None),
            P(("section", "dp"), None),
            P(("section", "dp"), None),
        ),
        check_vma=False,
    )
    return step
```

```python
import jax
import jax.numpy as jnp
from jax import lax
from jax.experimental import pallas as pl
from jax.experimental.pallas import tpu as pltpu
from jax.sharding import PartitionSpec as P

norm_eps = 1e-05
beta_first = 0.9
beta_second = 0.95
adam_eps = 1e-05
learning_rate = 0.0003
decay_rate = 0.1

MESH = pl.DeviceIdType.MESH


def times_transposed(former, latter):
    return lax.dot_general(
        former, latter, (((1,), (1,)), ((), ())), preferred_element_type=jnp.float32
    )


def transposed_times(former, latter):
    return lax.dot_general(
        former, latter, (((0,), (0,)), ((), ())), preferred_element_type=jnp.float32
    )


def plain_times(former, latter):
    return jnp.dot(former, latter, preferred_element_type=jnp.float32)


def adam_update(master, first, second, gradient):
    first_next = beta_first * first + (1.0 - beta_first) * gradient
    second_next = beta_second * second + (1.0 - beta_second) * gradient * gradient
    master_next = master - learning_rate * (
        first_next / (jnp.sqrt(second_next) + adam_eps) + decay_rate * master
    )
    return (master_next, first_next, second_next)


def remote(src, dst, send, recv, device):
    return pltpu.make_async_remote_copy(
        src_ref=src, dst_ref=dst, send_sem=send, recv_sem=recv, device_id=device, device_id_type=MESH
    )


def step_kernel(
    mixed, block, weight, head, small,
    out_grad, head_grad, embed_grad,
    table, w_all, block_own, final, normed_all, inv_all, inv_in, hid_pass, inv_pass, logits, hid, logit_cot, cot,
    gain, own_ids, id_all, mix, cot_all, hid_all, lc_all, cot_t, part, out_send, out_own, out_recv,
    head_send, embed_send, head_recv, embed_recv,
    send_sem, recv_sem, spread_send, spread_recv, far_send, far_recv, local_sem,
):
    s = lax.axis_index("section")
    r = lax.axis_index("dp")
    y, xh = s // 2, s % 2
    z, xl, c = r // 4, (r // 2) % 2, r % 2
    zin = z % 2
    even_z = lax.rem(z + 8 - 3 * zin, 8)
    pair = even_z // 2
    before, after = lax.rem(y + 3, 4), lax.rem(y + 1, 4)
    opposite = lax.rem(y + 2, 4)
    far = 1 - xh
    last = 7
    share = hid.shape[0]
    section_of = lambda yy, hh: yy * 2 + hh
    to_before = {"section": section_of(before, xh), "dp": r}
    to_after = {"section": section_of(after, xh), "dp": r}
    to_far = {"section": section_of(y, far), "dp": r}
    to_cross = {"section": section_of(y, far), "dp": z * 4 + (1 - xl) * 2 + c}

    def near(k):
        return (zin + k // 4) % 2, (xl + (k // 2) % 2) % 2, (c + k % 2) % 2

    def slot_of(k):
        other_z, other_x, other_c = near(k)
        return other_z * 4 + other_x * 2 + other_c

    def z_of(other_z):
        return lax.rem(even_z + 3 * other_z, 8)

    def peer_of(k):
        other_z, other_x, other_c = near(k)
        return {"section": s, "dp": z_of(other_z) * 4 + other_x * 2 + other_c}

    def owner_z(zz, cc, b):
        delta = cc if b == 0 else 2 - 3 * cc
        return lax.rem(zz + 8 + (2 * (zz % 2) - 1) * delta, 8)

    def column_block(k, b):
        other_z, other_x, other_c = near(k)
        return owner_z(z_of(other_z), other_c, b) * 2 + other_x

    def columns_of(k, b):
        return pl.ds(pl.multiple_of(column_block(k, b) * 128, 128), 128)

    slot = slot_of(0)
    to_sibling, to_x, to_z = peer_of(1), peer_of(2), peer_of(4)

    table_load = pltpu.make_async_copy(head, table.at[pl.ds(s * 256, 256)], local_sem.at[0])
    table_load.start()
    mixed_load = pltpu.make_async_copy(mixed, mix.at[:, slot], local_sem.at[1])
    mixed_load.start()
    block_load = pltpu.make_async_copy(block, block_own, local_sem.at[2])
    weight_load = [
        pltpu.make_async_copy(weight.at[pl.ds(k * 256, 256)], w_all.at[pl.ds(k * 256, 256)], local_sem.at[3 + k])
        for k in range(8)
    ]

    @pl.when(s == last)
    def _():
        for k in range(8):
            weight_load[k].start()
        block_load.start()

    barrier = pltpu.get_barrier_semaphore()
    pl.semaphore_signal(barrier, inc=1, device_id=to_cross, device_id_type=MESH)

    @pl.loop(1, 8)
    def _(step):
        pl.semaphore_signal(
            barrier, inc=1, device_id={"section": lax.rem(s + step, 8), "dp": r}, device_id_type=MESH
        )

    @pl.loop(1, 32)
    def _(step):
        pl.semaphore_signal(
            barrier, inc=1, device_id={"section": s, "dp": lax.rem(r + step, 32)}, device_id_type=MESH
        )

    for m in range(4):
        own_ids[0:1, m * 64 : (m + 1) * 64] = small[16 + m : 17 + m, 0:64].astype(jnp.int32)
    id_all[slot] = own_ids[...]
    for m in range(16):
        gain[0:1, m * 128 : (m + 1) * 128] = small[m : m + 1, :]
    table_load.wait()
    mixed_load.wait()
    pl.semaphore_wait(barrier, 39)

    table_out, mix_out, swap_out, cot_out, hid_out, lc_out, lc_swap_out, id_out = range(8)

    def arrived(dst, recv):
        remote(dst, dst, send_sem.at[0], recv, to_sibling).wait_recv()

    def sent(src, group):
        remote(src, src, send_sem.at[group], recv_sem.at[0], to_sibling).wait_send()

    def rows(yy, hh, p, half=None, core=None):
        start = section_of(yy, hh) * 256 + (c if core is None else core) * 128 + p * 64
        if half is None:
            return table.at[pl.ds(start, 64)]
        return table.at[pl.ds(start + half * 32, 32)]

    def make(ref, number, device, group=table_out):
        return remote(ref, ref, send_sem.at[group], recv_sem.at[number], device)

    def pass_on(ref, number, device, group=table_out):
        make(ref, number, device, group).start()

    pass_on(rows(y, xh, 1), 6, to_before)
    pass_on(rows(y, xh, 1), 5, to_after)
    pass_on(rows(y, xh, 0), 0, to_cross)
    pass_on(rows(y, xh, 0), 8, to_before)
    pass_on(rows(y, xh, 0), 7, to_after)
    for k in range(1, 8):
        remote(own_ids, id_all.at[slot], send_sem.at[id_out], recv_sem.at[39], peer_of(k)).start()

    own_mix = mix.at[:, slot]
    pass_on(own_mix, 35, to_sibling, mix_out)

    def pieces(direction, first, end, at):
        if direction == "z":
            return [make(mix.at[p, at], 40 + p // 2, to_z, mix_out) for p in range(first, end)]
        return [make(mix.at[p, at], 31 if at is slot else 33, to_x, mix_out) for p in range(first, end)]

    def feed(direction, first, end):
        for copy in pieces(direction, first, end, slot):
            copy.start()

    mix_x, mix_z, mix_xz = slot_of(2), slot_of(4), slot_of(6)

    def feed_corner(group):
        arrived(mix.at[pl.ds(2 * group, 2), mix_z], recv_sem.at[40 + group])
        for copy in pieces("x", 2 * group, 2 * group + 2, mix_z):
            copy.start()

    feed("z", 0, 3)
    bulk = [make(rows(y, xh, 1), 1, to_cross)] + pieces("x", 0, 3, slot)

    @pl.when(s != last)
    def _():
        for copy in bulk:
            copy.start()

    def piece(k):
        at = pl.ds(k * share, share)
        direct = k % 2 == 1 or k in (2, last - 1)
        target_device = {"section": k if direct else k + 1, "dp": r}
        return (
            remote(
                normed_all.at[at],
                hid if direct else hid_pass,
                spread_send.at[k],
                spread_recv.at[0 if direct else 2],
                target_device,
            ),
            remote(
                inv_all.at[at],
                inv_in if direct else inv_pass,
                spread_send.at[8 + k],
                spread_recv.at[1 if direct else 3],
                target_device,
            ),
        )

    def passed():
        return (
            remote(hid_pass, hid, spread_send.at[0], spread_recv.at[0], to_far),
            remote(inv_pass, inv_in, spread_send.at[8], spread_recv.at[1], to_far),
        )

    passes = jnp.logical_or(s == 1, s == 5)

    @pl.when(s == last)
    def _():
        for k in range(8):
            weight_load[k].wait()
        block_load.wait()

        @pl.loop(0, 8)
        def _(k):
            at = pl.ds(pl.multiple_of(k * 256, 256), 256)
            final[:, at] = block_own[:, at].astype(jnp.float32) + times_transposed(
                mix[:, slot].reshape(256, 2048), w_all[at, :]
            )

        for k in (0, 4, 2, 6, 3, 1, 5, 7):
            at = pl.ds(k * share, share)
            value = final[at, :]
            inverse = lax.rsqrt(jnp.mean(value * value, axis=-1, keepdims=True) + norm_eps)
            normed = (value * inverse * gain[...]).astype(jnp.bfloat16)
            wide_inverse = jnp.broadcast_to(inverse, (share, 128))
            if k < last:
                normed_all[at, :] = normed
                inv_all[at, :] = wide_inverse
                for copy in piece(k):
                    copy.start()
            else:
                hid[...] = normed
                inv_in[...] = wide_inverse
        for copy in bulk:
            copy.start()

    def swap_columns(array, spread, base):
        for k in range(1, 8):
            for b in range(2):
                remote(
                    array.at[:, columns_of(k, b)],
                    spread.at[b, s, slot],
                    send_sem.at[swap_out],
                    recv_sem.at[base],
                    peer_of(k),
                ).start()
        for b in range(2):
            spread[b, s, slot] = array[:, columns_of(0, b)]

    def wait_columns(spread, base):
        arrived(spread.at[:, 0, pl.ds(0, 7)], recv_sem.at[base])

    cot_base, hid_base, lc_base = 46, 55, 64

    def gather_start(spread, base):
        own = spread.at[:, s]
        pass_on(own, base, to_far, cot_out if base == cot_base else hid_out)
        pass_on(own, base + 2, to_before, cot_out if base == cot_base else hid_out)
        pass_on(own, base + 1, to_after, cot_out if base == cot_base else hid_out)

    def gather_near(spread, base):
        arrived(spread.at[:, section_of(before, xh)], recv_sem.at[base + 1])
        pass_on(spread.at[0, section_of(before, xh)], base + 5, to_after, cot_out if base == cot_base else hid_out)
        arrived(spread.at[:, section_of(after, xh)], recv_sem.at[base + 2])
        pass_on(spread.at[1, section_of(after, xh)], base + 6, to_before, cot_out if base == cot_base else hid_out)

    def gather_far(spread, base):
        other = spread.at[:, section_of(y, far)]
        arrived(other, recv_sem.at[base])
        pass_on(other, base + 4, to_before, cot_out if base == cot_base else hid_out)
        pass_on(other, base + 3, to_after, cot_out if base == cot_base else hid_out)

    def gather_far_near(spread, base):
        arrived(spread.at[:, section_of(before, far)], recv_sem.at[base + 3])
        pass_on(spread.at[0, section_of(before, far)], base + 7, to_after, cot_out if base == cot_base else hid_out)
        arrived(spread.at[:, section_of(after, far)], recv_sem.at[base + 4])
        pass_on(spread.at[1, section_of(after, far)], base + 8, to_before, cot_out if base == cot_base else hid_out)

    def gather_end(spread, base):
        arrived(spread.at[0, section_of(opposite, xh)], recv_sem.at[base + 5])
        arrived(spread.at[1, section_of(opposite, xh)], recv_sem.at[base + 6])
        arrived(spread.at[0, section_of(opposite, far)], recv_sem.at[base + 7])
        arrived(spread.at[1, section_of(opposite, far)], recv_sem.at[base + 8])

    shared = []

    def share_chunk(yy, hh, p):
        shared.append((yy, hh, p))
        pass_on(rows(yy, hh, p), 17 if len(shared) <= 7 else 45, to_sibling)

    def chunk_arrived(yy, hh, p, number, half=None):
        arrived(rows(yy, hh, p, half), recv_sem.at[number])

    chunk_arrived(before, xh, 1, 5)
    pass_on(rows(before, xh, 1, 0), 11, to_after)
    pass_on(rows(before, xh, 1), 2, to_cross)
    share_chunk(before, xh, 1)
    chunk_arrived(after, xh, 1, 6)
    pass_on(rows(after, xh, 1, 1), 12, to_before)
    pass_on(rows(after, xh, 1), 3, to_cross)
    share_chunk(after, xh, 1)
    feed("x", 3, 5)
    chunk_arrived(y, far, 0, 0)
    pass_on(rows(y, far, 0), 9, to_after)
    pass_on(rows(y, far, 0), 10, to_before)
    share_chunk(y, far, 0)
    chunk_arrived(before, xh, 0, 7)
    pass_on(rows(before, xh, 0, 0), 13, to_after)
    share_chunk(before, xh, 0)
    chunk_arrived(after, xh, 0, 8)
    pass_on(rows(after, xh, 0, 1), 14, to_before)
    share_chunk(after, xh, 0)
    feed("z", 3, 4)
    feed("x", 5, 8)
    chunk_arrived(opposite, xh, 1, 11, 0)
    chunk_arrived(opposite, xh, 1, 12, 1)
    pass_on(rows(opposite, xh, 1), 4, to_cross)
    share_chunk(opposite, xh, 1)
    chunk_arrived(y, far, 1, 1)
    share_chunk(y, far, 1)
    feed("z", 4, 5)
    feed_corner(0)
    @pl.when(passes)
    def _():
        for copy in piece(0):
            copy.wait_recv()
        for copy in passed():
            copy.start()

    chunk_arrived(before, far, 0, 9)
    pass_on(rows(before, far, 0, 0), 15, to_after)
    share_chunk(before, far, 0)
    chunk_arrived(after, far, 0, 10)
    pass_on(rows(after, far, 0, 1), 16, to_before)
    share_chunk(after, far, 0)

    feed("z", 5, 6)
    chunk_arrived(before, far, 1, 2)
    share_chunk(before, far, 1)
    chunk_arrived(after, far, 1, 3)
    share_chunk(after, far, 1)
    chunk_arrived(opposite, xh, 0, 13, 0)
    chunk_arrived(opposite, xh, 0, 14, 1)
    share_chunk(opposite, xh, 0)
    chunk_arrived(opposite, far, 0, 15, 0)
    chunk_arrived(opposite, far, 0, 16, 1)
    share_chunk(opposite, far, 0)
    @pl.when(s != last)
    def _():
        for copy in passed():
            copy.wait_recv()

    swap_columns(hid, hid_all, 36)
    feed("z", 6, 7)
    feed_corner(1)
    chunk_arrived(opposite, far, 1, 4)
    share_chunk(opposite, far, 1)
    def score(sections):
        for section in sections:
            at = pl.ds(pl.multiple_of(section * 256, 256), 256)
            logits[:, at] = times_transposed(hid[...], table[at, :])

    arrived(table.at[pl.ds(0, 7 * 64)], recv_sem.at[17])
    score([s, section_of(before, xh), section_of(after, xh), section_of(y, far)])
    arrived(table.at[pl.ds(0, 7 * 64)], recv_sem.at[45])

    score([section_of(opposite, xh), section_of(before, far), section_of(after, far), section_of(opposite, far)])

    value = logits[...]
    weights = jnp.exp(value - jnp.max(value, axis=-1, keepdims=True))
    predicted = weights / jnp.sum(weights, axis=-1, keepdims=True)
    columns = lax.broadcasted_iota(jnp.int32, value.shape, 1)
    target_row = jnp.zeros((1, 64), jnp.float32)
    for m in range(4):
        target_row = jnp.where(s // 2 == m, small[16 + m : 17 + m, 64:128], target_row)
    here = lax.broadcasted_iota(jnp.int32, (share, 64), 1) == share * (s % 2) + lax.broadcasted_iota(
        jnp.int32, (share, 64), 0
    )
    own_target = jnp.sum(jnp.where(here, target_row, 0.0), axis=1, keepdims=True)
    hit = columns == own_target.astype(jnp.int32)
    logit_cot[...] = jnp.where(hit, predicted - 1.0, predicted).astype(jnp.bfloat16)

    for step in range(1, 8):
        other = lax.rem(s + step, 8)
        at = pl.ds(pl.multiple_of(other * 256, 256), 256)
        remote(
            logit_cot.at[:, at],
            lc_all.at[s, slot],
            send_sem.at[lc_swap_out],
            recv_sem.at[38],
            {"section": other, "dp": r},
        ).start()
    lc_all[s, slot] = logit_cot[:, pl.ds(pl.multiple_of(s * 256, 256), 256)]

    @pl.loop(0, 8)
    def _(k):
        at = pl.ds(pl.multiple_of(k * 256, 256), 256)
        logits[:, at] = plain_times(logit_cot[...], table[:, at]) * gain[:, at]

    scaled = logits[...]
    unit = hid[...].astype(jnp.float32) / gain[...]
    cot[...] = (
        inv_in[:, :1] * (scaled - unit * jnp.mean(scaled * unit, axis=-1, keepdims=True))
    ).astype(jnp.bfloat16)
    swap_columns(cot, cot_all, 37)

    feed("z", 7, 8)
    wait_columns(hid_all, 36)
    gather_start(hid_all, hid_base)
    wait_columns(cot_all, 37)
    gather_start(cot_all, cot_base)
    feed_corner(2)
    gather_near(hid_all, hid_base)
    arrived(lc_all.at[0, pl.ds(0, 7)], recv_sem.at[38])
    for k in (2, 4, 6, 1):
        pass_on(lc_all.at[:, slot], lc_base + k, peer_of(k), lc_out)
    gather_near(cot_all, cot_base)
    gather_far(cot_all, cot_base)
    gather_far(hid_all, hid_base)
    arrived(mix.at[:, mix_x], recv_sem.at[31])
    pass_on(mix.at[:, mix_x], 32, to_sibling, mix_out)
    feed_corner(3)
    pass_on(mix.at[:, mix_z], 34, to_sibling, mix_out)
    gather_far_near(cot_all, cot_base)
    gather_far_near(hid_all, hid_base)
    def row_copy(send, recv, send_at, recv_at, target_dp):
        return remote(
            send.at[target_dp], recv.at[pair, slot], send_at, recv_at, {"section": s, "dp": target_dp}
        )

    head_rows = (head_send, head_recv, send_sem.at[8], recv_sem.at[18])
    embed_rows = (embed_send, embed_recv, send_sem.at[9], recv_sem.at[19])

    def rows_start(refs):
        @pl.loop(1, 32)
        def _(step):
            row_copy(*refs, lax.rem(r + step, 32)).start()

        refs[1][pair, slot] = refs[0][r]

    def rows_wait(refs):
        arrived(refs[0].at[pl.ds(0, 31)], refs[3])

    def rows_end(refs):
        everything = refs[0].at[pl.ds(0, 31)]
        remote(everything, everything, refs[2], refs[3], to_sibling).wait_send()

    def rows_sum(recv, grad):
        sources = {}
        for w in range(4):
            for j in range(8):
                sender_z = (2 * w + 3 * (j // 4)) % 8
                for b in range(2):
                    delta = j % 2 if b == 0 else 2 - 3 * (j % 2)
                    owner_of = (sender_z + 8 + (2 * (sender_z % 2) - 1) * delta) % 8
                    sources.setdefault(owner_of * 2 + (j // 2) % 2, []).append((w, j, b))
        for column, senders in sources.items():
            total = 0.0
            for w, j, b in senders:
                total = total + recv[w, j, 8 * b : 8 * b + 8, :]
            grad[:, column * 128 : column * 128 + 128] = total

    gather_end(cot_all, cot_base)

    arrived(id_all.at[pl.ds(0, 7)], recv_sem.at[39])
    vocabulary = s * 256 + lax.broadcasted_iota(jnp.int32, (256, 256), 0)
    totals = [jnp.zeros((256, 128), jnp.float32)] * 2
    for k in range(8):
        marks = jnp.where(vocabulary == id_all[k], 1.0, 0.0).astype(jnp.bfloat16)
        for b in range(2):
            totals[b] = totals[b] + plain_times(marks, cot_all[b, :, k].reshape(256, 128))
    embed_send[...] = jnp.concatenate([total.reshape(32, 8, 128) for total in totals], axis=1)
    rows_start(embed_rows)
    for k in (2, 4, 6):
        other = lc_all.at[:, slot_of(k)]
        arrived(other, recv_sem.at[lc_base + k])
        pass_on(other, lc_base + k + 1, to_sibling, lc_out)
    gather_end(hid_all, hid_base)
    for k in (1, 3, 5, 7):
        arrived(lc_all.at[:, slot_of(k)], recv_sem.at[lc_base + k])
    products = [
        transposed_times(lc_all[...].reshape(2048, 256), hid_all[b].reshape(2048, 128)).reshape(32, 8, 128)
        for b in range(2)
    ]
    head_send[...] = jnp.concatenate(products, axis=1)
    rows_start(head_rows)
    arrived(mix.at[:, mix_xz], recv_sem.at[33])
    pass_on(mix.at[:, mix_xz], 44, to_sibling, mix_out)
    for number, k in ((35, 1), (32, 3), (34, 5), (44, 7)):
        arrived(mix.at[:, slot_of(k)], recv_sem.at[number])

    for b in range(2):
        cot_t[pl.ds(b * 128, 128), :] = cot_all[b].reshape(2048, 128).T

    sign = 2 * zin - 1

    def owner(delta, core):
        return {"section": s, "dp": lax.rem(z + 8 + sign * delta, 8) * 4 + xl * 2 + core}

    deltas = (0, 1, -1, 2)

    def far_rows(half, number, b, core, place):
        at = pl.ds(half * 1024, 1024)
        return remote(
            out_send.at[2 * b + core, :, at],
            out_recv.at[place - 1, :, at],
            far_send.at[half * 4 + number],
            far_recv.at[half * 4 + place],
            owner(deltas[place], core),
        )

    def sibling_rows(half):
        at = pl.ds(half * 1024, 1024)
        return remote(
            part.at[pl.ds(64, 64), at], out_own.at[:, at], far_send.at[half * 4], far_recv.at[half * 4], owner(0, 1)
        )

    def even_core(half):
        return [far_rows(half, 1, 1, 0, 3), far_rows(half, 2, 1, 1, 3), sibling_rows(half)]

    def odd_core(half):
        return [far_rows(half, 2 * b + core, b, core, 1 + b) for b in (1, 0) for core in range(2)]

    for half in range(2):

        @pl.loop(half * 4, half * 4 + 4)
        def _(k):
            at = pl.ds(pl.multiple_of(k * 256, 256), 256)
            product = plain_times(cot_t[...], mix[:, :, :, at].reshape(2048, 256))
            part[:, at] = product[:128]
            out_send[:, :, at] = product.reshape(4, 64, 256).astype(jnp.bfloat16)

        @pl.when(c == 0)
        def _():
            for copy in even_core(half):
                copy.start()

        @pl.when(c == 1)
        def _():
            for copy in odd_core(half):
                copy.start()

    for half in range(2):
        at = pl.ds(half * 1024, 1024)

        @pl.when(c == 1)
        def _():
            arrived(out_own.at[:, at], far_recv.at[half * 4])

        @pl.when(c == 0)
        def _():
            out_own[:, at] = part[:64, at]

        for place in (1, 2, 3):
            arrived(out_recv.at[place - 1, :, at], far_recv.at[half * 4 + place])
        total = out_own[:, at]
        for place in (1, 2, 3):
            total = total + out_recv[place - 1, :, at].astype(jnp.float32)
        out_grad[:, at] = total

    rows_wait(embed_rows)
    rows_sum(embed_recv, embed_grad)

    rows_wait(head_rows)
    rows_sum(head_recv, head_grad)
    rows_end(head_rows)
    rows_end(embed_rows)

    @pl.when(s == last)
    def _():
        for k in range(last):
            for copy in piece(k):
                copy.wait_send()

    @pl.when(passes)
    def _():
        for copy in passed():
            copy.wait_send()

    for half in range(2):

        @pl.when(c == 0)
        def _():
            for copy in even_core(half):
                copy.wait_send()

        @pl.when(c == 1)
        def _():
            for copy in odd_core(half):
                copy.wait_send()

    sent(table.at[pl.ds(0, 1792)], table_out)
    sent(mix.at[pl.ds(0, 7)], mix_out)
    sent(cot_all.at[0, pl.ds(0, 7), pl.ds(0, 4)], swap_out)
    sent(cot_all.at[:, pl.ds(0, 7)], cot_out)
    sent(hid_all.at[:, pl.ds(0, 7)], hid_out)
    sent(lc_all.at[pl.ds(0, 7)], lc_out)
    sent(lc_all.at[0, pl.ds(0, 7)], lc_swap_out)
    sent(id_all.at[pl.ds(0, 7)], id_out)


def gradients(mixed, block, weight, head, small):
    sections, share, width = mixed.shape
    tokens = sections * share
    vmem = pl.BlockSpec(memory_space=pltpu.VMEM)
    anywhere = pl.BlockSpec(memory_space=pl.ANY)
    bf16, f32 = jnp.bfloat16, jnp.float32
    dma = pltpu.SemaphoreType.DMA
    return pl.pallas_call(
        step_kernel,
        out_shape=[
            jax.ShapeDtypeStruct((64, width), f32),
            jax.ShapeDtypeStruct((8, width), f32),
            jax.ShapeDtypeStruct((8, width), f32),
        ],
        in_specs=[anywhere, anywhere, anywhere, anywhere, vmem],
        out_specs=[vmem, vmem, vmem],
        scratch_shapes=[
            pltpu.VMEM((2048, width), bf16),
            pltpu.VMEM((width, width), bf16),
            pltpu.VMEM((tokens, width), bf16),
            pltpu.VMEM((tokens, width), f32),
            pltpu.VMEM((tokens, width), bf16),
            pltpu.VMEM((tokens, 128), f32),
            pltpu.VMEM((share, 128), f32),
            pltpu.VMEM((share, width), bf16),
            pltpu.VMEM((share, 128), f32),
            pltpu.VMEM((share, 2048), f32),
            pltpu.VMEM((share, width), bf16),
            pltpu.VMEM((share, 2048), bf16),
            pltpu.VMEM((share, width), bf16),
            pltpu.VMEM((1, width), f32),
            pltpu.VMEM((1, tokens), jnp.int32),
            pltpu.VMEM((8, 1, tokens), jnp.int32),
            pltpu.VMEM((8, 8, share, width), bf16),
            pltpu.VMEM((2, 8, 8, share, 128), bf16),
            pltpu.VMEM((2, 8, 8, share, 128), bf16),
            pltpu.VMEM((8, 8, share, 256), bf16),
            pltpu.VMEM((256, 2048), bf16),
            pltpu.VMEM((128, width), f32),
            pltpu.VMEM((4, 64, width), bf16),
            pltpu.VMEM((64, width), f32),
            pltpu.VMEM((3, 64, width), bf16),
            pltpu.VMEM((32, 16, 128), f32),
            pltpu.VMEM((32, 16, 128), f32),
            pltpu.VMEM((4, 8, 16, 128), f32),
            pltpu.VMEM((4, 8, 16, 128), f32),
            dma((10,)),
            dma((72,)),
            dma((16,)),
            dma((4,)),
            dma((8,)),
            dma((8,)),
            dma((11,)),
        ],
        compiler_params=pltpu.CompilerParams(collective_id=0, has_side_effects=True, vmem_limit_bytes=53 * 2**20),
        name="gradients",
    )(mixed, block, weight, head, small)


def local(
    block_inputs,
    mixed_inputs,
    token_ids,
    target_ids,
    final_gain,
    out_weight,
    head_weight,
    out_master,
    out_first,
    out_second,
    head_master,
    head_first,
    head_second,
    embed_master,
    embed_first,
    embed_second,
):
    sections = lax.axis_size("section")
    batches, rows, width = mixed_inputs[0].shape
    tokens = batches * rows
    id_rows = jnp.concatenate([token_ids, target_ids], axis=1).astype(jnp.float32)
    small = jnp.concatenate([final_gain.reshape(width // 128, 128), id_rows])
    out_gradient, head_gradient, embed_gradient = gradients(
        mixed_inputs[0].reshape(sections, tokens // sections, width),
        block_inputs[0].reshape(tokens, width),
        out_weight[0],
        head_weight,
        small,
    )
    out_out = adam_update(out_master, out_first, out_second, out_gradient.reshape(out_master.shape))
    head_out = adam_update(head_master, head_first, head_second, head_gradient)
    embed_out = adam_update(embed_master, embed_first, embed_second, embed_gradient)
    return out_out + head_out + embed_out


def solution(mesh):
    step = jax.shard_map(
        local,
        mesh=mesh,
        in_specs=(
            P("section", None, "dp", None),
            P("section", None, "dp", None),
            P(None, "dp"),
            P(None, "dp"),
            P(),
            P("section", None, None),
            P("section", None),
            P("section", "dp", None),
            P("section", "dp", None),
            P("section", "dp", None),
            P(("section", "dp"), None),
            P(("section", "dp"), None),
            P(("section", "dp"), None),
            P(("section", "dp"), None),
            P(("section", "dp"), None),
            P(("section", "dp"), None),
        ),
        out_specs=(
            P("section", "dp", None),
            P("section", "dp", None),
            P("section", "dp", None),
            P(("section", "dp"), None),
            P(("section", "dp"), None),
            P(("section", "dp"), None),
            P(("section", "dp"), None),
            P(("section", "dp"), None),
            P(("section", "dp"), None),
        ),
        check_vma=False,
    )
    return step
```
